32 devices in a mesh: wave: 4 (over x, core), band: 8 (over z, y).
Axes of the slice: x: 2, y: 2, z: 4, core: 2. Of those that a mesh axis runs over, the one named last changes fastest.
Arguments:
- control: float32 [256, 224, 192], P('band', 'wave'), may hold values from -6 to 6
- spectral_scale: float32 [256, 224, 192], P('band', 'wave'), may hold values from 0.3 to 3
- vertical_root: float32 [96, 96], replicated, may hold values from -0.625 to 0.625
- legendre: float32 [224, 448, 256], P('wave'), may hold values from -0.375 to 0.375
- zonal_number: int32 [224], replicated, may hold values from 0 to 223, each once
- courant: float32 [448, 96, 1024], P('band', None, 'wave'), may hold values from 0.05 to 0.9
- lidar_coef: float32 [12], replicated, may hold values from 0.2 to 1
- aod_coef: float32 [96], replicated, may hold values from 0.02 to 0.2
- obs_count: int32 [32, 32], P(('wave', 'band')), may hold values from 0 to 128, as said below
- obs_column: int32 [1024, 128], P(('wave', 'band')), may hold values from 0 to 14335
- obs_level: int32 [1024, 128], P(('wave', 'band')), may hold values from 0 to 7
- lidar_obs: float32 [1024, 128], P(('wave', 'band')), may hold values from -6 to 6
- aod_obs: float32 [1024, 128], P(('wave', 'band')), may hold values from -6 to 6
- obs_weight: float32 [1024, 128], P(('wave', 'band')), may hold values from 0.5 to 2
Outputs:
- gradient: float32 [256, 224, 192], P('band', 'wave')
- state_increment: float32 [448, 96, 1024], P('band', None, 'wave')
The draws below stay inside these ranges and needn't reach their ends.
Inputs may be any that keep to these rules, and one draw needn't show every extreme that they name: `obs_count`: live slots from a device to an owner; in every draw one owner receives 128 from every device. `zonal_number`: each number of 0 to 223 once.
All inputs are finite; a program needn't handle non-finite values.
Results may differ from the reference program's by a relative error of at most 0.0003.
Values sent between devices are 32-bit elements; how exact they have to be, the bound alone decides.
A program may use at most 128 MiB of HBM per device.

```python
import math
import jax
import jax.numpy as jnp
from jax import lax

NT = 256
MW = 224
NLAT = 448
NLON = 1024
LEV = 8
BINS = 12
STEPS = 4
SLOT = 128
LB = 96
N_WAVE = 4
N_BAND = 8
DEVICES = 32


def draw_obs_count(key, part):
    count_key, owner_key = jax.random.split(jax.random.fold_in(key, 11))
    counts = jax.random.randint(count_key, (DEVICES, DEVICES), 0, SLOT + 1)
    owner = jax.random.randint(owner_key, (), 0, DEVICES)
    filled = jnp.arange(DEVICES)[None, :] == owner
    return jnp.where(filled, SLOT, counts).astype(jnp.int32)


def with_ends(array, stream_key, low, largest):
    spot = [jax.random.randint(jax.random.fold_in(stream_key, axis), (), 0, length) for axis, length in enumerate(array.shape)]
    longest = array.shape.index(max(array.shape))
    next_to = spot[:longest] + [(spot[longest] + 1) % array.shape[longest]] + spot[longest + 1:]
    return array.at[tuple(spot)].set(low).at[tuple(next_to)].set(largest)


def level_of(stream_key, extent, cuts, smallest, top_value):
    factor_of = 1.0
    for axis_at, blocks in cuts:
        heights = jax.random.uniform(jax.random.fold_in(jax.random.fold_in(stream_key, 6), axis_at), (blocks,), jnp.float32, smallest / len(cuts), top_value / len(cuts))
        factor_of = factor_of * jnp.repeat(jnp.exp(heights), extent[axis_at] // blocks).reshape((-1,) + (1,) * (len(extent) - 1 - axis_at))
    return factor_of


def scatter_about(rng, dims, deviation, reach, pieces=(), kind=jnp.bfloat16):
    entries = deviation * jax.random.normal(rng, dims, jnp.float32)
    if pieces:
        entries = entries * level_of(rng, dims, pieces, -0.22, 0.18)
    return jnp.clip(entries, -reach, reach).astype(kind)


def setup_inputs(seed: int = 0) -> dict:
    keys = jax.random.split(jax.random.key(seed), 15)
    return {
        "control": scatter_about(keys[0], (NT, MW, 2 * LB), 1.0, 6.0, ((0, 8), (1, 4)), jnp.float32),
        "spectral_scale": jnp.clip(jnp.exp(math.log(3.0) - 2.3025851 * jax.random.uniform(keys[1], (NT, MW, 2 * LB), jnp.float32) ** level_of(keys[1], (NT, MW, 2 * LB), ((0, 8), (1, 4)), -0.2, 0.2)), 0.3, 3.0),
        "vertical_root": scatter_about(keys[2], (LB, LB), LB ** -0.5, 0.625, (), jnp.float32),
        "legendre": scatter_about(keys[3], (MW, NLAT, NT), NT ** -0.5, 0.375, ((0, 4),), jnp.float32),
        "zonal_number": jax.random.permutation(keys[4], MW).astype(jnp.int32),
        "courant": jnp.clip(0.05 + 0.84999998 * jax.random.uniform(keys[5], (NLAT, LB, NLON), jnp.float32) ** level_of(keys[5], (NLAT, LB, NLON), ((0, 8), (2, 4)), -0.2, 0.2), 0.05, 0.9),
        "lidar_coef": jnp.clip(jnp.exp(jax.random.uniform(keys[6], (BINS,), jnp.float32, math.log(0.2), math.log(1.0))), 0.2, 1.0),
        "aod_coef": jnp.clip(jnp.exp(jax.random.uniform(keys[7], (LB,), jnp.float32, math.log(0.02), math.log(0.2))), 0.02, 0.2),
        "obs_count": draw_obs_count(jax.random.fold_in(keys[14], 71), 0),
        "obs_column": with_ends(jax.random.randint(keys[9], (DEVICES * DEVICES, SLOT), 0, NLAT * NLON // DEVICES), jax.random.fold_in(keys[9], 1), 0, (NLAT * NLON // DEVICES) - 1).astype(jnp.int32),
        "obs_level": with_ends(jax.random.randint(keys[10], (DEVICES * DEVICES, SLOT), 0, LEV), jax.random.fold_in(keys[10], 1), 0, LEV - 1).astype(jnp.int32),
        "lidar_obs": scatter_about(keys[11], (DEVICES * DEVICES, SLOT), 1.0, 6.0, ((0, 32),), jnp.float32),
        "aod_obs": scatter_about(keys[12], (DEVICES * DEVICES, SLOT), 1.0, 6.0, ((0, 32),), jnp.float32),
        "obs_weight": jnp.clip(jnp.exp(math.log(2.0) - 1.3862944 * jax.random.uniform(keys[13], (DEVICES * DEVICES, SLOT), jnp.float32) ** level_of(keys[13], (DEVICES * DEVICES, SLOT), ((0, 32),), -0.2, 0.2)), 0.5, 2.0),
    }


highest = lax.Precision.HIGHEST


def trig_tables(numbers, lon_first, lon_count, lon_total, factor):
    longitudes = lon_first + jnp.arange(lon_count, dtype=jnp.int32)
    phases = (numbers[:, None] * longitudes[None, :]) % lon_total
    angles = phases.astype(jnp.float32) * (2.0 * math.pi / lon_total)
    return jnp.cos(angles) * factor, jnp.sin(angles) * factor


def settle(tracer, courant):
    outflow = courant * tracer
    inflow = jnp.concatenate([jnp.zeros_like(outflow[:, :BINS]), outflow[:, :-BINS]], axis=1)
    return tracer - outflow + inflow


def settle_adjoint(adjoint, courant):
    below = jnp.concatenate([adjoint[:, BINS:], jnp.zeros_like(adjoint[:, :BINS])], axis=1)
    return adjoint + courant * (below - adjoint)


def departures(profile, levels, active, lidar_vals, aod_vals, weights, lidar_coef, aod_coef):
    chosen = (jnp.arange(LEV, dtype=jnp.int32)[None, :] == levels[:, None]).astype(profile.dtype)
    layered = profile.reshape(-1, LEV, BINS)
    at_level = jnp.sum(chosen[:, :, None] * layered, axis=1)
    lidar_model = jnp.sum(at_level * lidar_coef[None, :], axis=1)
    aod_model = jnp.sum(profile * aod_coef[None, :], axis=1)
    lidar_resid = active * weights * (lidar_model - lidar_vals)
    aod_resid = active * weights * (aod_model - aod_vals)
    spread = lidar_resid[:, None, None] * chosen[:, :, None] * lidar_coef[None, None, :]
    return spread.reshape(-1, LEV * BINS) + aod_resid[:, None] * aod_coef[None, :]


def reference(control, spectral_scale, vertical_root, legendre, zonal_number, courant, lidar_coef, aod_coef, obs_count, obs_column, obs_level, lidar_obs, aod_obs, obs_weight):
    channels = LEV * BINS
    factor = MW ** -0.5
    paired = control.reshape(NT, MW, channels, 2)
    mixed = jnp.einsum('nmcp,cd->nmdp', paired, vertical_root, precision=highest).reshape(NT, MW, 2 * channels)
    scaled = spectral_scale * mixed
    spectral = jnp.einsum('mln,nmc->mlc', legendre, scaled, precision=highest)
    cosine, sine_table = trig_tables(zonal_number, 0, NLON, NLON, factor)
    parts = spectral.reshape(MW, NLAT, channels, 2)
    tracer = jnp.einsum('mo,mtc->tco', cosine, parts[..., 0], precision=highest) - jnp.einsum('mo,mtc->tco', sine_table, parts[..., 1], precision=highest)
    for repeat in range(STEPS):
        tracer = settle(tracer, courant)

    lat_block = NLAT // N_BAND
    lon_block = NLON // N_WAVE
    owners = jnp.arange(DEVICES, dtype=jnp.int32)[:, None]
    slot_index = jnp.arange(SLOT, dtype=jnp.int32)[None, :]

    def one_source(adjoint, source):
        first_row = source * DEVICES
        columns = lax.dynamic_slice_in_dim(obs_column, first_row, DEVICES, 0)
        levels = lax.dynamic_slice_in_dim(obs_level, first_row, DEVICES, 0).reshape(-1)
        lidar_vals = lax.dynamic_slice_in_dim(lidar_obs, first_row, DEVICES, 0).reshape(-1)
        aod_vals = lax.dynamic_slice_in_dim(aod_obs, first_row, DEVICES, 0).reshape(-1)
        weights = lax.dynamic_slice_in_dim(obs_weight, first_row, DEVICES, 0).reshape(-1)
        counts = lax.dynamic_index_in_dim(obs_count, source, 0, keepdims=False)
        active = (slot_index < counts[:, None]).astype(jnp.float32).reshape(-1)
        lat_index = ((owners % N_BAND) * lat_block + columns // lon_block).reshape(-1)
        lon_index = ((owners // N_BAND) * lon_block + columns % lon_block).reshape(-1)
        profile = tracer[lat_index, :, lon_index]
        contrib = departures(profile, levels, active, lidar_vals, aod_vals, weights, lidar_coef, aod_coef)
        return adjoint.at[lat_index, :, lon_index].add(contrib), None

    adjoint, unused = lax.scan(one_source, jnp.zeros_like(tracer), jnp.arange(DEVICES, dtype=jnp.int32))
    for repeat in range(STEPS):
        adjoint = settle_adjoint(adjoint, courant)
    real_adj = jnp.einsum('mo,tco->mtc', cosine, adjoint, precision=highest)
    imag_adj = -jnp.einsum('mo,tco->mtc', sine_table, adjoint, precision=highest)
    spectral_adj = jnp.stack([real_adj, imag_adj], axis=-1).reshape(MW, NLAT, 2 * channels)
    scaled_adj = jnp.einsum('mtn,mtc->nmc', legendre, spectral_adj, precision=highest)
    mixed_adj = (spectral_scale * scaled_adj).reshape(NT, MW, channels, 2)
    control_adj = jnp.einsum('nmdp,cd->nmcp', mixed_adj, vertical_root, precision=highest).reshape(NT, MW, 2 * channels)
    return control + control_adj, tracer
```

```python
import math

import jax
import jax.numpy as jnp
from jax import lax
from jax.experimental import pallas as pl
from jax.experimental.pallas import tpu as pltpu
from jax.sharding import PartitionSpec as P

MW = 224
LEV = 8
BINS = 12
STEPS = 4


highest = lax.Precision.HIGHEST
high = lax.Precision.HIGH


def trig_tables(numbers, lon_first, lon_count, lon_total, factor):
    longitudes = lon_first + jnp.arange(lon_count, dtype=jnp.int32)
    phases = numbers[:, None] * longitudes[None, :] % lon_total
    angles = phases.astype(jnp.float32) * (2.0 * math.pi / lon_total)
    return (jnp.cos(angles) * factor, jnp.sin(angles) * factor)


def settle_kernel(bins, tracer_ref, courant_ref, proj_ref, out_ref, model_ref):
    tracer = tracer_ref[0]
    courant = courant_ref[0]
    row = lax.broadcasted_iota(jnp.int32, tracer.shape, 0)
    for repeat in range(STEPS):
        outflow = courant * tracer
        inflow = jnp.where(row >= bins, pltpu.roll(outflow, bins, 0), 0.0)
        tracer = tracer - outflow + inflow
    out_ref[0] = tracer
    model_ref[0] = jnp.dot(proj_ref[...], tracer, precision=highest, preferred_element_type=jnp.float32)


def settle_adjoint_kernel(bins, resid_ref, courant_ref, proj_ref, out_ref):
    courant = courant_ref[0]
    adjoint = jnp.dot(proj_ref[...], resid_ref[0], precision=highest, preferred_element_type=jnp.float32)
    channels = adjoint.shape[0]
    row = lax.broadcasted_iota(jnp.int32, adjoint.shape, 0)
    for repeat in range(STEPS):
        below = jnp.where(row < channels - bins, pltpu.roll(adjoint, channels - bins, 0), 0.0)
        adjoint = adjoint + courant * (below - adjoint)
    out_ref[0] = adjoint


def per_lat(rows, cols):
    return pl.BlockSpec((1, rows, cols), lambda t: (t, 0, 0))


def whole(rows, cols):
    return pl.BlockSpec((rows, cols), lambda t: (0, 0))


def settle_forward(tracer, courant, proj, bins):
    lats, channels, lons = tracer.shape
    rows = proj.shape[0]
    return pl.pallas_call(
        lambda *refs: settle_kernel(bins, *refs),
        grid=(lats,),
        in_specs=[per_lat(channels, lons), per_lat(channels, lons), whole(rows, channels)],
        out_specs=[per_lat(channels, lons), per_lat(rows, lons)],
        out_shape=[
            jax.ShapeDtypeStruct((lats, channels, lons), jnp.float32),
            jax.ShapeDtypeStruct((lats, rows, lons), jnp.float32),
        ],
        name="settle_forward",
    )(tracer, courant, proj)


def settle_backward(resid, courant, proj_t, bins):
    lats, channels, lons = courant.shape
    rows = proj_t.shape[1]
    return pl.pallas_call(
        lambda *refs: settle_adjoint_kernel(bins, *refs),
        grid=(lats,),
        in_specs=[per_lat(rows, lons), per_lat(channels, lons), whole(channels, rows)],
        out_specs=per_lat(channels, lons),
        out_shape=jax.ShapeDtypeStruct((lats, channels, lons), jnp.float32),
        name="settle_backward",
    )(resid, courant, proj_t)


def synthesis_sum(cosine, sine_table, parts):
    return jnp.einsum("mo,mtc->tco", cosine, parts[..., 0], precision=high) - jnp.einsum(
        "mo,mtc->tco", sine_table, parts[..., 1], precision=high
    )


def analysis(cosine, sine_table, field):
    real_adj = jnp.einsum("mo,tco->mtc", cosine, field, precision=high)
    imag_adj = -jnp.einsum("mo,tco->mtc", sine_table, field, precision=high)
    stacked = jnp.stack([real_adj, imag_adj], axis=-1)
    return stacked.reshape(stacked.shape[0], stacked.shape[1], -1)


def body(
    control,
    spectral_scale,
    vertical_root,
    legendre,
    zonal_number,
    courant,
    lidar_coef,
    aod_coef,
    obs_count,
    obs_column,
    obs_level,
    lidar_obs,
    aod_obs,
    obs_weight,
):
    modes_here, waves_here, width = control.shape
    channels = width // 2
    wave_count = lax.axis_size("wave")
    band_count = lax.axis_size("band")
    lat_here = legendre.shape[1] // band_count
    lon_here = courant.shape[2]
    lon_total = lon_here * wave_count
    lon_first = lax.axis_index("wave") * lon_here
    factor = MW ** (-0.5)
    slot_count = obs_column.shape[1]
    live = jnp.arange(slot_count, dtype=jnp.int32)[None, :] < obs_count.reshape(-1, 1)
    packet = jnp.stack(
        [
            obs_column.astype(jnp.float32),
            obs_level.astype(jnp.float32),
            lidar_obs,
            aod_obs,
            jnp.where(live, obs_weight, 0.0),
        ],
        axis=1,
    )
    arrived = lax.all_to_all(packet, ("wave", "band"), split_axis=0, concat_axis=0, tiled=True)
    columns, levels, lidar_vals, aod_vals, weights = [arrived[:, i].reshape(-1) for i in range(5)]
    columns = columns.astype(jnp.int32)
    levels = levels.astype(jnp.int32)
    paired = control.reshape(modes_here, waves_here, channels, 2)
    mixed = jnp.einsum("nmcp,cd->nmdp", paired, vertical_root, precision=high).reshape(
        modes_here, waves_here, width
    )
    scaled = spectral_scale * mixed
    all_modes = lax.all_to_all(scaled, "band", split_axis=2, concat_axis=0, tiled=True)
    every_lat = jnp.einsum("mln,nmc->mlc", legendre, all_modes, precision=high)
    spectral = lax.all_to_all(every_lat, "band", split_axis=1, concat_axis=2, tiled=True)
    shard_piece = lax.all_gather(spectral, "wave", axis=0, tiled=True)
    numbers = zonal_number
    cosine, sine_table = trig_tables(numbers, lon_first, lon_here, lon_total, factor)
    parts = shard_piece.reshape(shard_piece.shape[0], lat_here, channels, 2)
    tracer = synthesis_sum(cosine, sine_table, parts)
    bins = lidar_coef.shape[0]
    levels_here = channels // bins
    proj_rows = -(-(levels_here + 1) // 8) * 8
    level_of = jnp.arange(channels, dtype=jnp.int32) // bins
    in_level = jnp.arange(levels_here, dtype=jnp.int32)[:, None] == level_of[None, :]
    proj = jnp.concatenate(
        [
            jnp.where(in_level, jnp.tile(lidar_coef, levels_here)[None, :], 0.0),
            aod_coef[None, :],
            jnp.zeros((proj_rows - levels_here - 1, channels), jnp.float32),
        ],
        axis=0,
    )
    tracer, model = settle_forward(tracer, courant, proj, bins)
    lat_index = columns // lon_here
    lon_hot = (columns % lon_here)[:, None] == jnp.arange(lon_here, dtype=jnp.int32)[None, :]
    lat_hot = (lat_index[:, None] == jnp.arange(lat_here, dtype=jnp.int32)[None, :]).astype(jnp.float32)
    cell = lat_index * levels_here + levels
    cell_hot = (
        cell[:, None] == jnp.arange(lat_here * levels_here, dtype=jnp.int32)[None, :]
    ).astype(jnp.float32)
    lidar_field = model[:, :levels_here].reshape(lat_here * levels_here, lon_here)
    aod_field = model[:, levels_here]
    lidar_rows = jnp.dot(cell_hot, lidar_field, precision=highest)
    aod_rows = jnp.dot(lat_hot, aod_field, precision=highest)
    lidar_model = jnp.sum(jnp.where(lon_hot, lidar_rows, 0.0), axis=1)
    aod_model = jnp.sum(jnp.where(lon_hot, aod_rows, 0.0), axis=1)
    lidar_resid = weights * (lidar_model - lidar_vals)
    aod_resid = weights * (aod_model - aod_vals)
    lidar_sum = lax.dot_general(
        cell_hot, jnp.where(lon_hot, lidar_resid[:, None], 0.0), (((0,), (0,)), ((), ())), precision=highest
    )
    aod_sum = lax.dot_general(
        lat_hot, jnp.where(lon_hot, aod_resid[:, None], 0.0), (((0,), (0,)), ((), ())), precision=highest
    )
    resid = jnp.concatenate(
        [
            lidar_sum.reshape(lat_here, levels_here, lon_here),
            aod_sum[:, None, :],
            jnp.zeros((lat_here, proj_rows - levels_here - 1, lon_here), jnp.float32),
        ],
        axis=1,
    )
    adjoint = settle_backward(resid, courant, proj.T, bins)
    numbers = zonal_number
    cosine, sine_table = trig_tables(numbers, lon_first, lon_here, lon_total, factor)
    spectral_adj = lax.psum_scatter(
        analysis(cosine, sine_table, adjoint), "wave", scatter_dimension=0, tiled=True
    )
    all_lats = lax.all_to_all(spectral_adj, "band", split_axis=2, concat_axis=1, tiled=True)
    mode_block = jnp.einsum("mtn,mtc->nmc", legendre, all_lats, precision=high)
    scaled_adj = lax.all_to_all(mode_block, "band", split_axis=0, concat_axis=2, tiled=True)
    mixed_adj = (spectral_scale * scaled_adj).reshape(modes_here, waves_here, channels, 2)
    control_adj = jnp.einsum("nmdp,cd->nmcp", mixed_adj, vertical_root, precision=high).reshape(
        modes_here, waves_here, width
    )
    return (control + control_adj, tracer)


LANES = 128
MESH_ID = pl.DeviceIdType.MESH
bf16 = jnp.bfloat16
f32 = jnp.float32
VMEM_LIMIT = 63 * 1024 * 1024


def split2(x):
    hi = x.astype(bf16)
    return hi, (x - hi.astype(f32)).astype(bf16)


def split3(x):
    hi, lo = split2(x)
    rest = x - hi.astype(f32)
    return hi, lo, (rest - lo.astype(f32)).astype(bf16)


def product(a, b, dims=((1,), (0,))):
    def one(x, y):
        return lax.dot_general(x, y, (dims, ((), ())), preferred_element_type=f32)

    return one(a[1], b[0]) + one(a[0], b[1]) + one(a[0], b[0])


def lane_of(shape):
    return lax.broadcasted_iota(jnp.int32, shape, len(shape) - 1)


def packed_order(channels, transposed):
    half = LANES // 2
    width = 2 * channels
    shape = (2 * LANES, width) if transposed else (width, 2 * LANES)
    source = lax.broadcasted_iota(jnp.int32, shape, 1 if transposed else 0)
    target = lax.broadcasted_iota(jnp.int32, shape, 0 if transposed else 1)
    channel = source // 2
    place = jnp.where(channel < half, channel, channel + half) + (source % 2) * half
    return jnp.where(place == target, 1.0, 0.0).astype(bf16)


def select_product(x, matrix):
    return sum(
        lax.dot_general(piece, matrix, (((1,), (0,)), ((), ())), preferred_element_type=f32)
        for piece in reversed(split3(x))
    )


class Sizes:
    def __init__(self, modes, waves, width, lats, bands, wave_count):
        self.modes, self.waves, self.width, self.lats = modes, waves, width, lats
        self.bands, self.wave_count = bands, wave_count
        self.own = waves // bands
        self.pairs = lats // 2
        self.rows = -(-(3 * self.pairs) // 8) * 8
        self.in_rows = modes + modes // 2
        self.slots = waves * wave_count


def first_kernel(z, control_ref, scale_ref, root_ref, leg_ref, out_ref, s_a, s_b, send_u, recv_v, leg, y_a, y_b, send_y,
                 leg_sem, a1_send, a1_recv, a2_send, a2_recv, x_send, x_recv, c_send, c_recv):
    w, b = lax.axis_index("wave"), lax.axis_index("band")
    partner = w + 1 - 2 * (w % 2)
    across = (w + 2) % z.wave_count
    relay = (partner + 2) % z.wave_count
    half = LANES // 2
    quarter = LANES // 4

    def peer(d):
        return (b + d) % z.bands

    leg_copy = pltpu.make_async_copy(leg_ref.at[pl.ds(b * z.own, z.own)], leg, leg_sem)
    leg_copy.start()
    barrier = pltpu.get_barrier_semaphore()
    for d in range(1, z.bands):
        pl.semaphore_signal(barrier, inc=1, device_id={"wave": w, "band": peer(d)}, device_id_type=MESH_ID)
    for other in (partner, across):
        pl.semaphore_signal(barrier, inc=1, device_id={"wave": other, "band": b}, device_id_type=MESH_ID)

    root = split2(root_ref[...])
    order = packed_order(z.width // 2, False)
    group = 8

    def vertical(i, carry):
        x = control_ref[pl.ds(i * group, group)].reshape(group * z.waves, z.width)
        scale = scale_ref[pl.ds(i * group, group)].reshape(group * z.waves, z.width)
        placed = select_product(scale * product(split2(x), root), order)
        at = pl.ds(pl.multiple_of(i * group * z.waves, 8), group * z.waves)
        s_a[at, :] = placed[:, :LANES]
        s_b[at, :] = placed[:, LANES:]
        return carry

    lax.fori_loop(0, z.modes // group, vertical, 0)

    def pack(m, carry):
        tall = s_b[pl.ds(m, z.modes, stride=z.waves), :]
        low = z.modes // 2
        send_u[m, : z.modes] = s_a[pl.ds(m, z.modes, stride=z.waves), :]
        send_u[m, z.modes :] = tall[:low] + pltpu.roll(tall[low:], quarter, 1)
        return carry

    lax.fori_loop(0, z.waves, pack, 0)
    pl.semaphore_wait(barrier, z.bands + 1)

    def first_copy(d):
        return pltpu.make_async_remote_copy(
            send_u.at[pl.ds(peer(d) * z.own, z.own)], recv_v.at[b], a1_send.at[d], a1_recv.at[d],
            device_id={"wave": w, "band": peer(d)}, device_id_type=MESH_ID)

    first_own = pltpu.make_async_copy(send_u.at[pl.ds(b * z.own, z.own)], recv_v.at[b], a1_send.at[0])
    for d in range(1, z.bands):
        first_copy(d).start()
    first_own.start()
    leg_copy.wait()
    first_own.wait()
    for d in range(1, z.bands):
        first_copy(d).wait_recv()

    def second_copy(p, d):
        return pltpu.make_async_remote_copy(
            send_y.at[p, peer(d)], out_ref.at[w, b, p], a2_send.at[p, d], a2_recv.at[p, d],
            device_id={"wave": w, "band": peer(d)}, device_id_type=MESH_ID)

    def second_own(p):
        return pltpu.make_async_copy(send_y.at[p, b], out_ref.at[w, b, p], a2_send.at[p, 0])

    def across_copy(p):
        return pltpu.make_async_remote_copy(
            out_ref.at[w, :, p], out_ref.at[w, :, p], x_send.at[p], x_recv.at[p],
            device_id={"wave": across, "band": b}, device_id_type=MESH_ID)

    def core_copy(p, which):
        block = w if which == 0 else across
        return pltpu.make_async_remote_copy(
            out_ref.at[block, :, p], out_ref.at[block, :, p], c_send.at[p, which], c_recv.at[p, which],
            device_id={"wave": partner, "band": b}, device_id_type=MESH_ID)

    def transform(p):
        tops, tails = [], []
        for s in range(z.bands):
            tail = recv_v[s, p, z.modes :]
            keep = lane_of(tail.shape) % half < quarter
            tops.append(recv_v[s, p, : z.modes])
            tails.append(jnp.where(keep, tail, 0.0))
            tails.append(jnp.where(keep, pltpu.roll(tail, LANES - quarter, 1), 0.0))
        x = jnp.concatenate([jnp.concatenate(tops, 0), jnp.concatenate(tails, 0)], 1)
        y = product(split2(leg[p]), split2(x))
        y_a[...] = y[:, :LANES]
        y_b[...] = y[:, LANES:]
        for s in range(z.bands):
            at = s * z.lats
            one = y_a[at : at + z.pairs]
            two = y_a[at + z.pairs : at + z.lats]
            left = lane_of(one.shape) < half
            send_y[p, s, z.rows - 8 :] = jnp.zeros((8, LANES), f32)
            send_y[p, s, : z.pairs] = jnp.where(left, one, pltpu.roll(two, half, 1))
            send_y[p, s, z.pairs : 2 * z.pairs] = jnp.where(left, pltpu.roll(one, half, 1), two)
            send_y[p, s, 2 * z.pairs : 3 * z.pairs] = y_b[at : at + z.pairs] + pltpu.roll(
                y_b[at + z.pairs : at + z.lats], quarter, 1)

    def phase(p, carry):
        @pl.when(p < z.own)
        def _():
            transform(p)
            for d in range(1, z.bands):
                second_copy(p, d).start()
            second_own(p).start()

        @pl.when((p >= 1) & (p <= z.own))
        def _():
            for d in range(1, z.bands):
                second_copy(p - 1, d).wait_recv()
            second_own(p - 1).wait()
            across_copy(p - 1).start()
            core_copy(p - 1, 0).start()

        @pl.when(p >= 2)
        def _():
            across_copy(p - 2).wait_recv()
            core_copy(p - 2, 1).start()

        return carry

    lax.fori_loop(0, z.own + 2, phase, 0)
    for d in range(1, z.bands):
        first_copy(d).wait_send()

    def drain(p, carry):
        for d in range(1, z.bands):
            second_copy(p, d).wait_send()
        across_copy(p).wait_send()
        for which in range(2):
            core_copy(p, which).wait()
        return carry

    lax.fori_loop(0, z.own, drain, 0)


def transform_forward(z, control, scale, root, legendre):
    whole_in = pl.BlockSpec(memory_space=pltpu.VMEM)
    anywhere = pl.BlockSpec(memory_space=pl.ANY)
    dma = pltpu.SemaphoreType.DMA
    lats_all = z.lats * z.bands
    return pl.pallas_call(
        lambda *refs: first_kernel(z, *refs),
        in_specs=[whole_in, whole_in, whole_in, anywhere],
        out_specs=anywhere,
        out_shape=jax.ShapeDtypeStruct((z.wave_count, z.bands, z.own, z.rows, LANES), f32),
        scratch_shapes=[
            pltpu.VMEM((z.modes * z.waves, LANES), f32),
            pltpu.VMEM((z.modes * z.waves, LANES), f32),
            pltpu.VMEM((z.waves, z.in_rows, LANES), f32),
            pltpu.VMEM((z.bands, z.own, z.in_rows, LANES), f32),
            pltpu.VMEM((z.own, lats_all, z.modes * z.bands), f32),
            pltpu.VMEM((lats_all, LANES), f32),
            pltpu.VMEM((lats_all, LANES), f32),
            pltpu.VMEM((z.own, z.bands, z.rows, LANES), f32),
            dma(()), dma((z.bands,)), dma((z.bands,)), dma((z.own, z.bands)), dma((z.own, z.bands)),
            dma((z.own,)), dma((z.own,)), dma((z.own, 2)), dma((z.own, 2)),
        ],
        compiler_params=pltpu.CompilerParams(collective_id=0, has_side_effects=True, vmem_limit_bytes=VMEM_LIMIT),
        name="transform_forward",
    )(control, scale, root, legendre)


def synthesis_kernel(z, bins, slabs_ref, cos_ref, sin_ref, courant_ref, proj_ref, out_ref, model_ref, c_hi, c_lo, n_hi, n_lo):
    i = pl.program_id(0)
    half = LANES // 2

    @pl.when(i == 0)
    def _():
        c_hi[...], c_lo[...] = split2(cos_ref[...])
        n_hi[...], n_lo[...] = split2(-sin_ref[...])

    def slab(row):
        return slabs_ref[pl.ds(row, z.slots, stride=z.rows), :]

    tail = slab(2 * z.pairs + i)
    real = jnp.concatenate([slab(i), tail], 1)
    imag = jnp.concatenate([slab(z.pairs + i), pltpu.roll(tail, half, 1)], 1)
    over_waves = ((0,), (0,))
    field = product(split2(real), (c_hi[...], c_lo[...]), over_waves) + product(
        split2(imag), (n_hi[...], n_lo[...]), over_waves)
    channels = z.width // 2
    rest = channels - half
    proj = split2(proj_ref[...])
    for which in range(2):
        tracer = jnp.concatenate(
            [field[which * half : (which + 1) * half],
             field[LANES + which * (half // 2) : LANES + which * (half // 2) + rest]], 0)
        courant = courant_ref[which, 0]
        row = lax.broadcasted_iota(jnp.int32, tracer.shape, 0)
        for repeat in range(STEPS):
            outflow = courant * tracer
            inflow = jnp.where(row >= bins, pltpu.roll(outflow, bins, 0), 0.0)
            tracer = tracer - outflow + inflow
        out_ref[which, 0] = tracer
        model_ref[which, 0] = product(proj, split2(tracer))


def paired(rows, cols):
    return pl.BlockSpec((2, 1, rows, cols), lambda i: (0, i, 0, 0))


def synthesis_settle(z, slabs, cosine, sine, courant, proj, bins):
    lats, channels, lons = courant.shape
    rows = proj.shape[0]
    tracer, model = pl.pallas_call(
        lambda *refs: synthesis_kernel(z, bins, *refs),
        grid=(z.pairs,),
        in_specs=[whole(z.slots * z.rows, LANES), whole(z.slots, lons), whole(z.slots, lons), paired(channels, lons),
                  whole(rows, channels)],
        out_specs=[paired(channels, lons), paired(rows, lons)],
        out_shape=[
            jax.ShapeDtypeStruct((2, z.pairs, channels, lons), f32),
            jax.ShapeDtypeStruct((2, z.pairs, rows, lons), f32),
        ],
        scratch_shapes=[pltpu.VMEM((z.slots, lons), bf16)] * 4,
        compiler_params=pltpu.CompilerParams(vmem_limit_bytes=VMEM_LIMIT),
        name="synthesis_settle",
    )(slabs.reshape(z.slots * z.rows, LANES), cosine, sine, courant.reshape(2, z.pairs, channels, lons), proj)
    return tracer.reshape(lats, channels, lons), model.reshape(lats, rows, lons)


def analysis_kernel(z, bins, resid_ref, courant_ref, proj_ref, cos_ref, sin_ref, out_ref, c_hi, c_lo, n_hi, n_lo):
    i = pl.program_id(0)
    half = LANES // 2

    @pl.when(i == 0)
    def _():
        c_hi[...], c_lo[...] = split2(cos_ref[...])
        n_hi[...], n_lo[...] = split2(-sin_ref[...])

    proj = split2(proj_ref[...])
    fields = []
    for which in range(2):
        courant = courant_ref[which, 0]
        adjoint = product(proj, split2(resid_ref[which, 0]))
        channels = adjoint.shape[0]
        row = lax.broadcasted_iota(jnp.int32, adjoint.shape, 0)
        for repeat in range(STEPS):
            below = jnp.where(row < channels - bins, pltpu.roll(adjoint, channels - bins, 0), 0.0)
            adjoint = adjoint + courant * (below - adjoint)
        fields.append(adjoint)
    gap = jnp.zeros((half // 2 - (channels - half), fields[0].shape[1]), f32)
    pieces = [field[:half] for field in fields]
    for field in fields:
        pieces.append(field[half:])
        if gap.shape[0]:
            pieces.append(gap)
    pieces.append(jnp.zeros((half, fields[0].shape[1]), f32))
    both = split2(jnp.concatenate(pieces, 0))
    over_lons = ((1,), (1,))
    real = product((c_hi[...], c_lo[...]), both, over_lons)
    imag = product((n_hi[...], n_lo[...]), both, over_lons)

    @pl.when(i == 0)
    def _():
        for spare in range(3 * z.pairs, z.rows):
            out_ref[pl.ds(spare, z.slots, stride=z.rows), :] = jnp.zeros((z.slots, LANES), f32)

    out_ref[pl.ds(i, z.slots, stride=z.rows), :] = real[:, :LANES]
    out_ref[pl.ds(z.pairs + i, z.slots, stride=z.rows), :] = imag[:, :LANES]
    out_ref[pl.ds(2 * z.pairs + i, z.slots, stride=z.rows), :] = real[:, LANES:] + pltpu.roll(imag[:, LANES:], half, 1)


def settle_analysis(z, resid, courant, proj_t, cosine, sine, bins):
    lats, channels, lons = courant.shape
    rows = proj_t.shape[1]
    out = pl.pallas_call(
        lambda *refs: analysis_kernel(z, bins, *refs),
        grid=(z.pairs,),
        in_specs=[paired(rows, lons), paired(channels, lons), whole(channels, rows), whole(z.slots, lons),
                  whole(z.slots, lons)],
        out_specs=whole(z.slots * z.rows, LANES),
        out_shape=jax.ShapeDtypeStruct((z.slots * z.rows, LANES), f32),
        scratch_shapes=[pltpu.VMEM((z.slots, lons), bf16)] * 4,
        compiler_params=pltpu.CompilerParams(vmem_limit_bytes=VMEM_LIMIT),
        name="settle_analysis",
    )(resid.reshape(2, z.pairs, rows, lons), courant.reshape(2, z.pairs, channels, lons), proj_t, cosine, sine)
    return out.reshape(z.wave_count, z.bands, z.own, z.rows, LANES)


def second_kernel(z, part_ref, leg_ref, out_ref, part, r1, r2, v3, leg, z_all, send_u,
                  leg_sem, q_sem, c_send, c_recv, x_send, x_recv, a3_send, a3_recv, a4_send, a4_recv):
    w, b = lax.axis_index("wave"), lax.axis_index("band")
    partner = w + 1 - 2 * (w % 2)
    across = (w + 2) % z.wave_count
    relay = (partner + 2) % z.wave_count
    half = LANES // 2
    quarter = LANES // 4

    def peer(d):
        return (b + d) % z.bands

    def target(q):
        return (b + 1 + q) % z.bands

    leg_copy = pltpu.make_async_copy(leg_ref.at[pl.ds(b * z.own, z.own)], leg, leg_sem)
    barrier = pltpu.get_barrier_semaphore()
    for d in range(1, z.bands):
        pl.semaphore_signal(barrier, inc=1, device_id={"wave": w, "band": peer(d)}, device_id_type=MESH_ID)
    for other in (partner, across):
        pl.semaphore_signal(barrier, inc=1, device_id={"wave": other, "band": b}, device_id_type=MESH_ID)

    def local_copy(q, which):
        block = w if which == 0 else across
        return pltpu.make_async_copy(part_ref.at[block, target(q)], part.at[q, which], q_sem.at[q, which])

    def core_copy(q, which):
        block = partner if which == 0 else relay
        return pltpu.make_async_remote_copy(
            part_ref.at[block, target(q)], r1.at[q, which], c_send.at[q, which], c_recv.at[q, which],
            device_id={"wave": partner, "band": b}, device_id_type=MESH_ID)

    def across_copy(q):
        return pltpu.make_async_remote_copy(
            part.at[q, 1], r2.at[q], x_send.at[q], x_recv.at[q],
            device_id={"wave": across, "band": b}, device_id_type=MESH_ID)

    def third_copy(q):
        return pltpu.make_async_remote_copy(
            part.at[q, 0], v3.at[b], a3_send.at[q], a3_recv.at[q],
            device_id={"wave": w, "band": target(q)}, device_id_type=MESH_ID)

    pl.semaphore_wait(barrier, z.bands + 1)

    def begin(q, carry):
        for which in (1, 0):
            core_copy(q, which).start()
            local_copy(q, which).start()
        return carry

    lax.fori_loop(0, z.bands, begin, 0)
    leg_copy.start()

    def stage(q, carry):
        @pl.when(q < z.bands)
        def _():
            local_copy(q, 1).wait()
            core_copy(q, 1).wait_recv()

            def add(p, inner):
                part[q, 1, p] = part[q, 1, p] + r1[q, 1, p]
                return inner

            lax.fori_loop(0, z.own, add, 0)
            across_copy(q).start()

        @pl.when(q >= 1)
        def _():
            k = q - 1
            local_copy(k, 0).wait()
            core_copy(k, 0).wait_recv()
            across_copy(k).wait_recv()

            def add(p, inner):
                part[k, 0, p] = part[k, 0, p] + r1[k, 0, p] + r2[k, p]
                return inner

            lax.fori_loop(0, z.own, add, 0)

            @pl.when(k < z.bands - 1)
            def _():
                third_copy(k).start()

        return carry

    lax.fori_loop(0, z.bands + 1, stage, 0)
    own_copy = pltpu.make_async_copy(part.at[z.bands - 1, 0], v3.at[b], a3_send.at[z.bands - 1])
    own_copy.start()
    leg_copy.wait()
    own_copy.wait()
    for q in range(z.bands - 1):
        third_copy(q).wait_recv()

    def fourth_copy(p, d):
        return pltpu.make_async_remote_copy(
            send_u.at[p, peer(d)], out_ref.at[b, p], a4_send.at[p, d], a4_recv.at[p, d],
            device_id={"wave": w, "band": peer(d)}, device_id_type=MESH_ID)

    def fourth_own(p):
        return pltpu.make_async_copy(send_u.at[p, b], out_ref.at[b, p], a4_send.at[p, 0])

    def transform(p, carry):
        for s in range(z.bands):
            at = s * z.lats
            real = v3[s, p, : z.pairs]
            imag = v3[s, p, z.pairs : 2 * z.pairs]
            tail = v3[s, p, 2 * z.pairs : 3 * z.pairs]
            lane = lane_of(real.shape)
            keep = lane % half < quarter
            z_all[at : at + z.pairs, :LANES] = jnp.where(lane < half, real, pltpu.roll(imag, half, 1))
            z_all[at + z.pairs : at + z.lats, :LANES] = jnp.where(lane < half, pltpu.roll(real, half, 1), imag)
            z_all[at : at + z.pairs, LANES:] = jnp.where(keep, tail, 0.0)
            z_all[at + z.pairs : at + z.lats, LANES:] = jnp.where(keep, pltpu.roll(tail, LANES - quarter, 1), 0.0)
        y = product(split2(leg[p]), split2(z_all[...]), ((0,), (0,)))
        for s in range(z.bands):
            rows = y[s * z.modes : (s + 1) * z.modes]
            low = z.modes // 2
            send_u[p, s, : z.modes] = rows[:, :LANES]
            send_u[p, s, z.modes :] = rows[:low, LANES:] + pltpu.roll(rows[low:, LANES:], quarter, 1)
        for d in range(1, z.bands):
            fourth_copy(p, d).start()
        fourth_own(p).start()
        return carry

    lax.fori_loop(0, z.own, transform, 0)

    def drain_sums(q, carry):
        across_copy(q).wait_send()
        for which in range(2):
            core_copy(q, which).wait_send()
        return carry

    lax.fori_loop(0, z.bands, drain_sums, 0)
    for q in range(z.bands - 1):
        third_copy(q).wait_send()

    def drain(p, carry):
        for d in range(1, z.bands):
            fourth_copy(p, d).wait()
        fourth_own(p).wait()
        return carry

    lax.fori_loop(0, z.own, drain, 0)


def transform_backward(z, part, legendre):
    anywhere = pl.BlockSpec(memory_space=pl.ANY)
    dma = pltpu.SemaphoreType.DMA
    lats_all = z.lats * z.bands
    slab = (z.own, z.rows, LANES)
    return pl.pallas_call(
        lambda *refs: second_kernel(z, *refs),
        in_specs=[anywhere, anywhere],
        out_specs=anywhere,
        out_shape=jax.ShapeDtypeStruct((z.bands, z.own, z.in_rows, LANES), f32),
        scratch_shapes=[
            pltpu.VMEM((z.bands, 2) + slab, f32),
            pltpu.VMEM((z.bands, 2) + slab, f32),
            pltpu.VMEM((z.bands,) + slab, f32),
            pltpu.VMEM((z.bands,) + slab, f32),
            pltpu.VMEM((z.own, lats_all, z.modes * z.bands), f32),
            pltpu.VMEM((lats_all, 2 * LANES), f32),
            pltpu.VMEM((z.own, z.bands, z.in_rows, LANES), f32),
            dma(()), dma((z.bands, 2)), dma((z.bands, 2)), dma((z.bands, 2)), dma((z.bands,)), dma((z.bands,)),
            dma((z.bands,)), dma((z.bands,)), dma((z.own, z.bands)), dma((z.own, z.bands)),
        ],
        compiler_params=pltpu.CompilerParams(collective_id=1, has_side_effects=True, vmem_limit_bytes=VMEM_LIMIT),
        name="transform_backward",
    )(part, legendre)


def last_kernel(z, slabs_ref, control_ref, scale_ref, root_ref, out_ref, s_a, s_b):
    half = LANES // 2
    quarter = LANES // 4

    def unpack(m, carry):
        tail = slabs_ref[m, z.modes :]
        keep = lane_of(tail.shape) % half < quarter
        both = jnp.concatenate(
            [jnp.where(keep, tail, 0.0), jnp.where(keep, pltpu.roll(tail, LANES - quarter, 1), 0.0)], 0)
        s_a[pl.ds(m, z.modes, stride=z.waves), :] = slabs_ref[m, : z.modes]
        s_b[pl.ds(m, z.modes, stride=z.waves), :] = both
        return carry

    lax.fori_loop(0, z.waves, unpack, 0)
    root = split2(root_ref[...])
    order = packed_order(z.width // 2, True)
    group = 8

    def vertical(i, carry):
        at = pl.ds(pl.multiple_of(i * group * z.waves, 8), group * z.waves)
        placed = jnp.concatenate([s_a[at, :], s_b[at, :]], 1)
        scale = scale_ref[pl.ds(i * group, group)].reshape(group * z.waves, z.width)
        mixed = product(split2(scale * select_product(placed, order)), root)
        out_ref[pl.ds(i * group, group)] = control_ref[pl.ds(i * group, group)] + mixed.reshape(
            group, z.waves, z.width)
        return carry

    lax.fori_loop(0, z.modes // group, vertical, 0)


def finish(z, slabs, control, scale, root_t):
    whole_in = pl.BlockSpec(memory_space=pltpu.VMEM)
    return pl.pallas_call(
        lambda *refs: last_kernel(z, *refs),
        in_specs=[whole_in] * 4,
        out_specs=whole_in,
        out_shape=jax.ShapeDtypeStruct(control.shape, f32),
        scratch_shapes=[pltpu.VMEM((z.modes * z.waves, LANES), f32)] * 2,
        compiler_params=pltpu.CompilerParams(vmem_limit_bytes=VMEM_LIMIT),
        name="finish",
    )(slabs.reshape(z.waves, z.in_rows, LANES), control, scale, root_t)


def observation_sums(z, tracer_shape, model, arrived, lidar_coef, levels_here, proj_rows):
    lat_here, lon_here = tracer_shape
    columns, levels, lidar_vals, aod_vals, weights = [arrived[:, i].reshape(-1) for i in range(5)]
    columns = columns.astype(jnp.int32)
    levels = levels.astype(jnp.int32)
    lat_index = columns // lon_here
    lon_hot = (columns % lon_here)[:, None] == jnp.arange(lon_here, dtype=jnp.int32)[None, :]
    lat_hot = (lat_index[:, None] == jnp.arange(lat_here, dtype=jnp.int32)[None, :]).astype(jnp.float32)
    cell = lat_index * levels_here + levels
    cell_hot = (
        cell[:, None] == jnp.arange(lat_here * levels_here, dtype=jnp.int32)[None, :]
    ).astype(jnp.float32)
    lidar_field = model[:, :levels_here].reshape(lat_here * levels_here, lon_here)
    aod_field = model[:, levels_here]
    lidar_rows = jnp.dot(cell_hot, lidar_field, precision=highest)
    aod_rows = jnp.dot(lat_hot, aod_field, precision=highest)
    lidar_model = jnp.sum(jnp.where(lon_hot, lidar_rows, 0.0), axis=1)
    aod_model = jnp.sum(jnp.where(lon_hot, aod_rows, 0.0), axis=1)
    lidar_resid = weights * (lidar_model - lidar_vals)
    aod_resid = weights * (aod_model - aod_vals)
    lidar_sum = lax.dot_general(
        cell_hot, jnp.where(lon_hot, lidar_resid[:, None], 0.0), (((0,), (0,)), ((), ())), precision=highest
    )
    aod_sum = lax.dot_general(
        lat_hot, jnp.where(lon_hot, aod_resid[:, None], 0.0), (((0,), (0,)), ((), ())), precision=highest
    )
    return jnp.concatenate(
        [
            lidar_sum.reshape(lat_here, levels_here, lon_here),
            aod_sum[:, None, :],
            jnp.zeros((lat_here, proj_rows - levels_here - 1, lon_here), jnp.float32),
        ],
        axis=1,
    )


def observation_packet(obs_count, obs_column, obs_level, lidar_obs, aod_obs, obs_weight):
    slot_count = obs_column.shape[1]
    live = jnp.arange(slot_count, dtype=jnp.int32)[None, :] < obs_count.reshape(-1, 1)
    packet = jnp.stack(
        [
            obs_column.astype(jnp.float32),
            obs_level.astype(jnp.float32),
            lidar_obs,
            aod_obs,
            jnp.where(live, obs_weight, 0.0),
        ],
        axis=1,
    )
    return lax.all_to_all(packet, ("wave", "band"), split_axis=0, concat_axis=0, tiled=True)


def projection(lidar_coef, aod_coef):
    bins = lidar_coef.shape[0]
    channels = aod_coef.shape[0]
    levels_here = channels // bins
    proj_rows = -(-(levels_here + 1) // 8) * 8
    level_of = jnp.arange(channels, dtype=jnp.int32) // bins
    in_level = jnp.arange(levels_here, dtype=jnp.int32)[:, None] == level_of[None, :]
    return jnp.concatenate(
        [
            jnp.where(in_level, jnp.tile(lidar_coef, levels_here)[None, :], 0.0),
            aod_coef[None, :],
            jnp.zeros((proj_rows - levels_here - 1, channels), jnp.float32),
        ],
        axis=0,
    )


def interleaved(root):
    channels = root.shape[0]
    wide = root[:, None, :, None] * jnp.eye(2, dtype=jnp.float32)[None, :, None, :]
    return wide.reshape(2 * channels, 2 * channels)


def fast_body(
    control,
    spectral_scale,
    vertical_root,
    legendre,
    zonal_number,
    courant,
    lidar_coef,
    aod_coef,
    obs_count,
    obs_column,
    obs_level,
    lidar_obs,
    aod_obs,
    obs_weight,
):
    modes_here, waves_here, width = control.shape
    wave_count = lax.axis_size("wave")
    lats_here, channels, lon_here = courant.shape
    z = Sizes(modes_here, waves_here, width, lats_here, lax.axis_size("band"), wave_count)
    lon_first = lax.axis_index("wave") * lon_here
    factor = zonal_number.shape[0] ** (-0.5)
    bins = lidar_coef.shape[0]
    levels_here = channels // bins
    arrived = observation_packet(obs_count, obs_column, obs_level, lidar_obs, aod_obs, obs_weight)
    cosine, sine = trig_tables(zonal_number, lon_first, lon_here, lon_here * wave_count, factor)
    proj = projection(lidar_coef, aod_coef)
    slabs = transform_forward(z, control, spectral_scale, interleaved(vertical_root), legendre)
    tracer, model = synthesis_settle(z, slabs, cosine, sine, courant, proj, bins)
    resid = observation_sums(z, (lats_here, lon_here), model, arrived, lidar_coef, levels_here, proj.shape[0])
    part = settle_analysis(z, resid, courant, proj.T, cosine, sine, bins)
    back = transform_backward(z, part, legendre)
    return finish(z, back, control, spectral_scale, interleaved(vertical_root.T)), tracer


def fits(mesh, control, courant):
    bands, waves = mesh.shape["band"], mesh.shape["wave"]
    modes_here, waves_here = control[0] // bands, control[1] // waves
    lats_here, channels = courant[0] // bands, courant[1]
    return (
        waves == 4
        and waves_here % bands == 0
        and waves_here % 8 == 0
        and modes_here % 16 == 0
        and lats_here % 8 == 0
        and LANES // 2 < channels <= LANES * 3 // 4
        and (channels - LANES // 2) % 8 == 0
        and courant[2] // waves % LANES == 0
    )


SPECS = (
    P("band", "wave", None),
    P("band", "wave", None),
    P(),
    P("wave", None, None),
    P(),
    P("band", None, "wave"),
    P(),
    P(),
    P(("wave", "band"), None),
    P(("wave", "band"), None),
    P(("wave", "band"), None),
    P(("wave", "band"), None),
    P(("wave", "band"), None),
    P(("wave", "band"), None),
)


def solution(mesh):
    def program(*args):
        chosen = fast_body if fits(mesh, args[0].shape, args[5].shape) else body
        return jax.shard_map(
            chosen,
            mesh=mesh,
            in_specs=SPECS,
            out_specs=(P("band", "wave", None), P("band", None, "wave")),
            check_vma=False,
        )(*args)

    return program
```

```python
import math

import jax
import jax.numpy as jnp
from jax import lax
from jax.experimental import pallas as pl
from jax.experimental.pallas import tpu as pltpu
from jax.sharding import PartitionSpec as P

MW = 224
LEV = 8
BINS = 12
STEPS = 4


highest = lax.Precision.HIGHEST
high = lax.Precision.HIGH


def trig_tables(numbers, lon_first, lon_count, lon_total, factor):
    longitudes = lon_first + jnp.arange(lon_count, dtype=jnp.int32)
    phases = numbers[:, None] * longitudes[None, :] % lon_total
    angles = phases.astype(jnp.float32) * (2.0 * math.pi / lon_total)
    return (jnp.cos(angles) * factor, jnp.sin(angles) * factor)


def settle_kernel(bins, tracer_ref, courant_ref, proj_ref, out_ref, model_ref):
    tracer = tracer_ref[0]
    courant = courant_ref[0]
    row = lax.broadcasted_iota(jnp.int32, tracer.shape, 0)
    for repeat in range(STEPS):
        outflow = courant * tracer
        inflow = jnp.where(row >= bins, pltpu.roll(outflow, bins, 0), 0.0)
        tracer = tracer - outflow + inflow
    out_ref[0] = tracer
    model_ref[0] = jnp.dot(proj_ref[...], tracer, precision=highest, preferred_element_type=jnp.float32)


def settle_adjoint_kernel(bins, resid_ref, courant_ref, proj_ref, out_ref):
    courant = courant_ref[0]
    adjoint = jnp.dot(proj_ref[...], resid_ref[0], precision=highest, preferred_element_type=jnp.float32)
    channels = adjoint.shape[0]
    row = lax.broadcasted_iota(jnp.int32, adjoint.shape, 0)
    for repeat in range(STEPS):
        below = jnp.where(row < channels - bins, pltpu.roll(adjoint, channels - bins, 0), 0.0)
        adjoint = adjoint + courant * (below - adjoint)
    out_ref[0] = adjoint


def per_lat(rows, cols):
    return pl.BlockSpec((1, rows, cols), lambda t: (t, 0, 0))


def whole(rows, cols):
    return pl.BlockSpec((rows, cols), lambda t: (0, 0))


def settle_forward(tracer, courant, proj, bins):
    lats, channels, lons = tracer.shape
    rows = proj.shape[0]
    return pl.pallas_call(
        lambda *refs: settle_kernel(bins, *refs),
        grid=(lats,),
        in_specs=[per_lat(channels, lons), per_lat(channels, lons), whole(rows, channels)],
        out_specs=[per_lat(channels, lons), per_lat(rows, lons)],
        out_shape=[
            jax.ShapeDtypeStruct((lats, channels, lons), jnp.float32),
            jax.ShapeDtypeStruct((lats, rows, lons), jnp.float32),
        ],
        name="settle_forward",
    )(tracer, courant, proj)


def settle_backward(resid, courant, proj_t, bins):
    lats, channels, lons = courant.shape
    rows = proj_t.shape[1]
    return pl.pallas_call(
        lambda *refs: settle_adjoint_kernel(bins, *refs),
        grid=(lats,),
        in_specs=[per_lat(rows, lons), per_lat(channels, lons), whole(channels, rows)],
        out_specs=per_lat(channels, lons),
        out_shape=jax.ShapeDtypeStruct((lats, channels, lons), jnp.float32),
        name="settle_backward",
    )(resid, courant, proj_t)


def synthesis_sum(cosine, sine_table, parts):
    return jnp.einsum("mo,mtc->tco", cosine, parts[..., 0], precision=high) - jnp.einsum(
        "mo,mtc->tco", sine_table, parts[..., 1], precision=high
    )


def analysis(cosine, sine_table, field):
    real_adj = jnp.einsum("mo,tco->mtc", cosine, field, precision=high)
    imag_adj = -jnp.einsum("mo,tco->mtc", sine_table, field, precision=high)
    stacked = jnp.stack([real_adj, imag_adj], axis=-1)
    return stacked.reshape(stacked.shape[0], stacked.shape[1], -1)


def body(
    control,
    spectral_scale,
    vertical_root,
    legendre,
    zonal_number,
    courant,
    lidar_coef,
    aod_coef,
    obs_count,
    obs_column,
    obs_level,
    lidar_obs,
    aod_obs,
    obs_weight,
):
    modes_here, waves_here, width = control.shape
    channels = width // 2
    wave_count = lax.axis_size("wave")
    band_count = lax.axis_size("band")
    lat_here = legendre.shape[1] // band_count
    lon_here = courant.shape[2]
    lon_total = lon_here * wave_count
    lon_first = lax.axis_index("wave") * lon_here
    factor = MW ** (-0.5)
    slot_count = obs_column.shape[1]
    live = jnp.arange(slot_count, dtype=jnp.int32)[None, :] < obs_count.reshape(-1, 1)
    packet = jnp.stack(
        [
            obs_column.astype(jnp.float32),
            obs_level.astype(jnp.float32),
            lidar_obs,
            aod_obs,
            jnp.where(live, obs_weight, 0.0),
        ],
        axis=1,
    )
    arrived = lax.all_to_all(packet, ("wave", "band"), split_axis=0, concat_axis=0, tiled=True)
    columns, levels, lidar_vals, aod_vals, weights = [arrived[:, i].reshape(-1) for i in range(5)]
    columns = columns.astype(jnp.int32)
    levels = levels.astype(jnp.int32)
    paired = control.reshape(modes_here, waves_here, channels, 2)
    mixed = jnp.einsum("nmcp,cd->nmdp", paired, vertical_root, precision=high).reshape(
        modes_here, waves_here, width
    )
    scaled = spectral_scale * mixed
    all_modes = lax.all_to_all(scaled, "band", split_axis=2, concat_axis=0, tiled=True)
    every_lat = jnp.einsum("mln,nmc->mlc", legendre, all_modes, precision=high)
    spectral = lax.all_to_all(every_lat, "band", split_axis=1, concat_axis=2, tiled=True)
    shard_piece = lax.all_gather(spectral, "wave", axis=0, tiled=True)
    numbers = zonal_number
    cosine, sine_table = trig_tables(numbers, lon_first, lon_here, lon_total, factor)
    parts = shard_piece.reshape(shard_piece.shape[0], lat_here, channels, 2)
    tracer = synthesis_sum(cosine, sine_table, parts)
    bins = lidar_coef.shape[0]
    levels_here = channels // bins
    proj_rows = -(-(levels_here + 1) // 8) * 8
    level_of = jnp.arange(channels, dtype=jnp.int32) // bins
    in_level = jnp.arange(levels_here, dtype=jnp.int32)[:, None] == level_of[None, :]
    proj = jnp.concatenate(
        [
            jnp.where(in_level, jnp.tile(lidar_coef, levels_here)[None, :], 0.0),
            aod_coef[None, :],
            jnp.zeros((proj_rows - levels_here - 1, channels), jnp.float32),
        ],
        axis=0,
    )
    tracer, model = settle_forward(tracer, courant, proj, bins)
    lat_index = columns // lon_here
    lon_hot = (columns % lon_here)[:, None] == jnp.arange(lon_here, dtype=jnp.int32)[None, :]
    lat_hot = (lat_index[:, None] == jnp.arange(lat_here, dtype=jnp.int32)[None, :]).astype(jnp.float32)
    cell = lat_index * levels_here + levels
    cell_hot = (
        cell[:, None] == jnp.arange(lat_here * levels_here, dtype=jnp.int32)[None, :]
    ).astype(jnp.float32)
    lidar_field = model[:, :levels_here].reshape(lat_here * levels_here, lon_here)
    aod_field = model[:, levels_here]
    lidar_rows = jnp.dot(cell_hot, lidar_field, precision=highest)
    aod_rows = jnp.dot(lat_hot, aod_field, precision=highest)
    lidar_model = jnp.sum(jnp.where(lon_hot, lidar_rows, 0.0), axis=1)
    aod_model = jnp.sum(jnp.where(lon_hot, aod_rows, 0.0), axis=1)
    lidar_resid = weights * (lidar_model - lidar_vals)
    aod_resid = weights * (aod_model - aod_vals)
    lidar_sum = lax.dot_general(
        cell_hot, jnp.where(lon_hot, lidar_resid[:, None], 0.0), (((0,), (0,)), ((), ())), precision=highest
    )
    aod_sum = lax.dot_general(
        lat_hot, jnp.where(lon_hot, aod_resid[:, None], 0.0), (((0,), (0,)), ((), ())), precision=highest
    )
    resid = jnp.concatenate(
        [
            lidar_sum.reshape(lat_here, levels_here, lon_here),
            aod_sum[:, None, :],
            jnp.zeros((lat_here, proj_rows - levels_here - 1, lon_here), jnp.float32),
        ],
        axis=1,
    )
    adjoint = settle_backward(resid, courant, proj.T, bins)
    numbers = zonal_number
    cosine, sine_table = trig_tables(numbers, lon_first, lon_here, lon_total, factor)
    spectral_adj = lax.psum_scatter(
        analysis(cosine, sine_table, adjoint), "wave", scatter_dimension=0, tiled=True
    )
    all_lats = lax.all_to_all(spectral_adj, "band", split_axis=2, concat_axis=1, tiled=True)
    mode_block = jnp.einsum("mtn,mtc->nmc", legendre, all_lats, precision=high)
    scaled_adj = lax.all_to_all(mode_block, "band", split_axis=0, concat_axis=2, tiled=True)
    mixed_adj = (spectral_scale * scaled_adj).reshape(modes_here, waves_here, channels, 2)
    control_adj = jnp.einsum("nmdp,cd->nmcp", mixed_adj, vertical_root, precision=high).reshape(
        modes_here, waves_here, width
    )
    return (control + control_adj, tracer)


LANES = 128
MESH_ID = pl.DeviceIdType.MESH
bf16 = jnp.bfloat16
f32 = jnp.float32
VMEM_LIMIT = 63 * 1024 * 1024


def split2(x):
    hi = x.astype(bf16)
    return hi, (x - hi.astype(f32)).astype(bf16)


def split3(x):
    hi, lo = split2(x)
    rest = x - hi.astype(f32)
    return hi, lo, (rest - lo.astype(f32)).astype(bf16)


def product(a, b, dims=((1,), (0,))):
    def one(x, y):
        return lax.dot_general(x, y, (dims, ((), ())), preferred_element_type=f32)

    return one(a[1], b[0]) + one(a[0], b[1]) + one(a[0], b[0])


def lane_of(shape):
    return lax.broadcasted_iota(jnp.int32, shape, len(shape) - 1)


def packed_order(channels, transposed):
    half = LANES // 2
    width = 2 * channels
    shape = (2 * LANES, width) if transposed else (width, 2 * LANES)
    source = lax.broadcasted_iota(jnp.int32, shape, 1 if transposed else 0)
    target = lax.broadcasted_iota(jnp.int32, shape, 0 if transposed else 1)
    channel = source // 2
    place = jnp.where(channel < half, channel, channel + half) + (source % 2) * half
    return jnp.where(place == target, 1.0, 0.0).astype(bf16)


def select_product(x, matrix):
    return sum(
        lax.dot_general(piece, matrix, (((1,), (0,)), ((), ())), preferred_element_type=f32)
        for piece in reversed(split3(x))
    )


def interleaved(root):
    channels = root.shape[0]
    wide = 2 * channels
    spread = (lax.broadcasted_iota(jnp.int32, (wide, channels), 0) // 2
              == lax.broadcasted_iota(jnp.int32, (wide, channels), 1))
    gather = (lax.broadcasted_iota(jnp.int32, (channels, wide), 1) // 2
              == lax.broadcasted_iota(jnp.int32, (channels, wide), 0))
    spread = jnp.where(spread, 1.0, 0.0).astype(bf16)
    gather = jnp.where(gather, 1.0, 0.0).astype(bf16)
    both = select_product(root, gather)
    both = sum(jnp.dot(spread, piece, preferred_element_type=f32) for piece in reversed(split3(both)))
    same = (lax.broadcasted_iota(jnp.int32, both.shape, 0) % 2) == (lax.broadcasted_iota(jnp.int32, both.shape, 1) % 2)
    return jnp.where(same, both, 0.0)


class Sizes:
    def __init__(self, modes, waves, width, lats, bands, wave_count):
        self.modes, self.waves, self.width, self.lats = modes, waves, width, lats
        self.bands, self.wave_count = bands, wave_count
        self.group = bands // 2
        self.own = waves // self.group
        self.half_lats = lats * self.group
        self.pairs = lats // 2
        self.rows = -(-(3 * self.pairs) // 8) * 8
        self.in_rows = modes + modes // 2
        self.slots = waves * wave_count


class Place:
    def __init__(self, z):
        self.w, self.b = lax.axis_index("wave"), lax.axis_index("band")
        self.partner = self.w + 1 - 2 * (self.w % 2)
        self.across = (self.w + 2) % z.wave_count
        self.relay = (self.partner + 2) % z.wave_count
        self.half, self.spot = self.b // z.group, self.b % z.group
        self.z = z

    def peer(self, d):
        return (self.b + d) % self.z.bands

    def near_spot(self, e):
        return (self.spot + e) % self.z.group

    def near(self, e):
        return self.half * self.z.group + self.near_spot(e)

    def greet(self):
        barrier = pltpu.get_barrier_semaphore()
        others = [(self.w, self.peer(d)) for d in range(1, self.z.bands)]
        for wave, band in others + [(self.partner, self.b), (self.across, self.b)]:
            pl.semaphore_signal(barrier, inc=1, device_id={"wave": wave, "band": band}, device_id_type=MESH_ID)
        return barrier


def remote(src, dst, send, recv, wave, band):
    return pltpu.make_async_remote_copy(
        src, dst, send, recv, device_id={"wave": wave, "band": band}, device_id_type=MESH_ID)


AHEAD = 3


def first_kernel(z, control_ref, scale_ref, root_ref, leg_ref, out_ref, s_a, s_b, send_u, recv_v, leg, y_a, y_b, send_y,
                 leg_sem, a1_send, a1_recv, a2_send, a2_recv, x_send, x_recv, c_send, c_recv):
    at_me = Place(z)
    w, b = at_me.w, at_me.b
    half = LANES // 2
    quarter = LANES // 4
    leg_copy = pltpu.make_async_copy(
        leg_ref.at[pl.ds(at_me.spot * z.own, z.own), pl.ds(at_me.half * z.half_lats, z.half_lats)], leg, leg_sem)
    leg_copy.start()
    barrier = at_me.greet()

    root = split2(interleaved(root_ref[...]))
    order = packed_order(z.width // 2, False)
    group = 8

    def vertical(i, carry):
        x = control_ref[pl.ds(i * group, group)].reshape(group * z.waves, z.width)
        scale = scale_ref[pl.ds(i * group, group)].reshape(group * z.waves, z.width)
        placed = select_product(scale * product(split2(x), root), order)
        at = pl.ds(pl.multiple_of(i * group * z.waves, 8), group * z.waves)
        s_a[at, :] = placed[:, :LANES]
        s_b[at, :] = placed[:, LANES:]
        return carry

    lax.fori_loop(0, z.modes // group, vertical, 0)

    def first_copy(c, d):
        to = at_me.peer(d)
        return remote(send_u.at[(to % z.group) * z.own + c], recv_v.at[b, c], a1_send.at[c, d], a1_recv.at[c, d], w, to)

    def first_own(c):
        return pltpu.make_async_copy(send_u.at[at_me.spot * z.own + c], recv_v.at[b, c], a1_send.at[c, 0])

    def launch(c):
        low = z.modes // 2
        for spot in range(z.group):
            m = spot * z.own + c
            tall = s_b[pl.ds(m, z.modes, stride=z.waves), :]
            send_u[m, : z.modes] = s_a[pl.ds(m, z.modes, stride=z.waves), :]
            send_u[m, z.modes :] = tall[:low] + pltpu.roll(tall[low:], quarter, 1)
        for d in range(1, z.bands):
            first_copy(c, d).start()
        first_own(c).start()

    def second_copy(c, e):
        return remote(send_y.at[c, at_me.near_spot(e)], out_ref.at[w, at_me.spot, c], a2_send.at[c, e], a2_recv.at[c, e],
                      w, at_me.near(e))

    def second_own(c):
        return pltpu.make_async_copy(send_y.at[c, at_me.spot], out_ref.at[w, at_me.spot, c], a2_send.at[c, 0])

    def across_copy(c):
        return remote(out_ref.at[w, :, c], out_ref.at[w, :, c], x_send.at[c], x_recv.at[c], at_me.across, b)

    def core_copy(c, which):
        block = w if which == 0 else at_me.across
        return remote(out_ref.at[block, :, c], out_ref.at[block, :, c], c_send.at[c, which], c_recv.at[c, which],
                      at_me.partner, b)

    def transform(c):
        tops, tails = [], []
        for s in range(z.bands):
            tail = recv_v[s, c, z.modes :]
            keep = lane_of(tail.shape) % half < quarter
            tops.append(recv_v[s, c, : z.modes])
            tails.append(jnp.where(keep, tail, 0.0))
            tails.append(jnp.where(keep, pltpu.roll(tail, LANES - quarter, 1), 0.0))
        x = jnp.concatenate([jnp.concatenate(tops, 0), jnp.concatenate(tails, 0)], 1)
        y = product(split2(leg[c]), split2(x))
        y_a[...] = y[:, :LANES]
        y_b[...] = y[:, LANES:]
        for s in range(z.group):
            at = s * z.lats
            one = y_a[at : at + z.pairs]
            two = y_a[at + z.pairs : at + z.lats]
            left = lane_of(one.shape) < half
            send_y[c, s, z.rows - 8 :] = jnp.zeros((8, LANES), f32)
            send_y[c, s, : z.pairs] = jnp.where(left, one, pltpu.roll(two, half, 1))
            send_y[c, s, z.pairs : 2 * z.pairs] = jnp.where(left, pltpu.roll(one, half, 1), two)
            send_y[c, s, 2 * z.pairs : 3 * z.pairs] = y_b[at : at + z.pairs] + pltpu.roll(
                y_b[at + z.pairs : at + z.lats], quarter, 1)

    pl.semaphore_wait(barrier, z.bands + 1)
    for c in range(min(AHEAD, z.own)):
        launch(c)
    leg_copy.wait()

    def phase(p, carry):
        @pl.when(p + AHEAD < z.own)
        def _():
            launch(p + AHEAD)

        @pl.when(p < z.own)
        def _():
            first_own(p).wait()
            for d in range(1, z.bands):
                first_copy(p, d).wait_recv()
            transform(p)
            for e in range(1, z.group):
                second_copy(p, e).start()
            second_own(p).start()

        @pl.when((p >= 1) & (p <= z.own))
        def _():
            for e in range(1, z.group):
                second_copy(p - 1, e).wait_recv()
            second_own(p - 1).wait()
            across_copy(p - 1).start()
            core_copy(p - 1, 0).start()

        @pl.when(p >= 2)
        def _():
            across_copy(p - 2).wait_recv()
            core_copy(p - 2, 1).start()

        return carry

    lax.fori_loop(0, z.own + 2, phase, 0)

    def drain(c, carry):
        for d in range(1, z.bands):
            first_copy(c, d).wait_send()
        for e in range(1, z.group):
            second_copy(c, e).wait_send()
        across_copy(c).wait_send()
        for which in range(2):
            core_copy(c, which).wait()
        return carry

    lax.fori_loop(0, z.own, drain, 0)


def transform_forward(z, control, scale, root, legendre):
    whole_in = pl.BlockSpec(memory_space=pltpu.VMEM)
    anywhere = pl.BlockSpec(memory_space=pl.ANY)
    dma = pltpu.SemaphoreType.DMA
    return pl.pallas_call(
        lambda *refs: first_kernel(z, *refs),
        in_specs=[whole_in, whole_in, whole_in, anywhere],
        out_specs=anywhere,
        out_shape=jax.ShapeDtypeStruct((z.wave_count, z.group, z.own, z.rows, LANES), f32),
        scratch_shapes=[
            pltpu.VMEM((z.modes * z.waves, LANES), f32),
            pltpu.VMEM((z.modes * z.waves, LANES), f32),
            pltpu.VMEM((z.waves, z.in_rows, LANES), f32),
            pltpu.VMEM((z.bands, z.own, z.in_rows, LANES), f32),
            pltpu.VMEM((z.own, z.half_lats, z.modes * z.bands), f32),
            pltpu.VMEM((z.half_lats, LANES), f32),
            pltpu.VMEM((z.half_lats, LANES), f32),
            pltpu.VMEM((z.own, z.group, z.rows, LANES), f32),
            dma(()), dma((z.own, z.bands)), dma((z.own, z.bands)), dma((z.own, z.group)), dma((z.own, z.group)),
            dma((z.own,)), dma((z.own,)), dma((z.own, 2)), dma((z.own, 2)),
        ],
        compiler_params=pltpu.CompilerParams(collective_id=0, has_side_effects=True, vmem_limit_bytes=VMEM_LIMIT),
        name="transform_forward",
    )(control, scale, root, legendre)


def synthesis_kernel(z, bins, slabs_ref, cos_ref, sin_ref, courant_ref, proj_ref, out_ref, model_ref, c_hi, c_lo, n_hi, n_lo):
    i = pl.program_id(0)
    half = LANES // 2

    @pl.when(i == 0)
    def _():
        c_hi[...], c_lo[...] = split2(cos_ref[...])
        n_hi[...], n_lo[...] = split2(-sin_ref[...])

    def slab(row):
        return slabs_ref[pl.ds(row, z.slots, stride=z.rows), :]

    tail = slab(2 * z.pairs + i)
    real = jnp.concatenate([slab(i), tail], 1)
    imag = jnp.concatenate([slab(z.pairs + i), pltpu.roll(tail, half, 1)], 1)
    over_waves = ((0,), (0,))
    field = product(split2(real), (c_hi[...], c_lo[...]), over_waves) + product(
        split2(imag), (n_hi[...], n_lo[...]), over_waves)
    channels = z.width // 2
    rest = channels - half
    proj = split2(proj_ref[...])
    for which in range(2):
        tracer = jnp.concatenate(
            [field[which * half : (which + 1) * half],
             field[LANES + which * (half // 2) : LANES + which * (half // 2) + rest]], 0)
        courant = courant_ref[which, 0]
        row = lax.broadcasted_iota(jnp.int32, tracer.shape, 0)
        for repeat in range(STEPS):
            outflow = courant * tracer
            inflow = jnp.where(row >= bins, pltpu.roll(outflow, bins, 0), 0.0)
            tracer = tracer - outflow + inflow
        out_ref[which, 0] = tracer
        model_ref[which, 0] = product(proj, split2(tracer))


def paired(rows, cols):
    return pl.BlockSpec((2, 1, rows, cols), lambda i: (0, i, 0, 0))


def synthesis_settle(z, slabs, cosine, sine, courant, proj, bins):
    lats, channels, lons = courant.shape
    rows = proj.shape[0]
    tracer, model = pl.pallas_call(
        lambda *refs: synthesis_kernel(z, bins, *refs),
        grid=(z.pairs,),
        in_specs=[whole(z.slots * z.rows, LANES), whole(z.slots, lons), whole(z.slots, lons), paired(channels, lons),
                  whole(rows, channels)],
        out_specs=[paired(channels, lons), paired(rows, lons)],
        out_shape=[
            jax.ShapeDtypeStruct((2, z.pairs, channels, lons), f32),
            jax.ShapeDtypeStruct((2, z.pairs, rows, lons), f32),
        ],
        scratch_shapes=[pltpu.VMEM((z.slots, lons), bf16)] * 4,
        compiler_params=pltpu.CompilerParams(vmem_limit_bytes=VMEM_LIMIT),
        name="synthesis_settle",
    )(slabs.reshape(z.slots * z.rows, LANES), cosine, sine, courant.reshape(2, z.pairs, channels, lons), proj)
    return tracer.reshape(lats, channels, lons), model.reshape(lats, rows, lons)


def analysis_kernel(z, bins, resid_ref, courant_ref, proj_ref, cos_ref, sin_ref, out_ref, c_hi, c_lo, n_hi, n_lo):
    i = pl.program_id(0)
    half = LANES // 2

    @pl.when(i == 0)
    def _():
        c_hi[...], c_lo[...] = split2(cos_ref[...])
        n_hi[...], n_lo[...] = split2(-sin_ref[...])

    proj = split2(proj_ref[...])
    fields = []
    for which in range(2):
        courant = courant_ref[which, 0]
        adjoint = product(proj, split2(resid_ref[which, 0]))
        channels = adjoint.shape[0]
        row = lax.broadcasted_iota(jnp.int32, adjoint.shape, 0)
        for repeat in range(STEPS):
            below = jnp.where(row < channels - bins, pltpu.roll(adjoint, channels - bins, 0), 0.0)
            adjoint = adjoint + courant * (below - adjoint)
        fields.append(adjoint)
    gap = jnp.zeros((half // 2 - (channels - half), fields[0].shape[1]), f32)
    pieces = [field[:half] for field in fields]
    for field in fields:
        pieces.append(field[half:])
        if gap.shape[0]:
            pieces.append(gap)
    pieces.append(jnp.zeros((half, fields[0].shape[1]), f32))
    both = split2(jnp.concatenate(pieces, 0))
    over_lons = ((1,), (1,))
    real = product((c_hi[...], c_lo[...]), both, over_lons)
    imag = product((n_hi[...], n_lo[...]), both, over_lons)

    @pl.when(i == 0)
    def _():
        for spare in range(3 * z.pairs, z.rows):
            out_ref[pl.ds(spare, z.slots, stride=z.rows), :] = jnp.zeros((z.slots, LANES), f32)

    out_ref[pl.ds(i, z.slots, stride=z.rows), :] = real[:, :LANES]
    out_ref[pl.ds(z.pairs + i, z.slots, stride=z.rows), :] = imag[:, :LANES]
    out_ref[pl.ds(2 * z.pairs + i, z.slots, stride=z.rows), :] = real[:, LANES:] + pltpu.roll(imag[:, LANES:], half, 1)


def settle_analysis(z, resid, courant, proj_t, cosine, sine, bins):
    lats, channels, lons = courant.shape
    rows = proj_t.shape[1]
    out = pl.pallas_call(
        lambda *refs: analysis_kernel(z, bins, *refs),
        grid=(z.pairs,),
        in_specs=[paired(rows, lons), paired(channels, lons), whole(channels, rows), whole(z.slots, lons),
                  whole(z.slots, lons)],
        out_specs=whole(z.slots * z.rows, LANES),
        out_shape=jax.ShapeDtypeStruct((z.slots * z.rows, LANES), f32),
        scratch_shapes=[pltpu.VMEM((z.slots, lons), bf16)] * 4,
        compiler_params=pltpu.CompilerParams(vmem_limit_bytes=VMEM_LIMIT),
        name="settle_analysis",
    )(resid.reshape(2, z.pairs, rows, lons), courant.reshape(2, z.pairs, channels, lons), proj_t, cosine, sine)
    return out.reshape(z.wave_count, z.group, z.own, z.rows, LANES)


def second_kernel(z, part_ref, leg_ref, out_ref, part, r1, r2, v3, leg, z_all, send_u,
                  leg_sem, q_sem, c_send, c_recv, x_send, x_recv, a3_send, a3_recv, a4_send, a4_recv):
    at_me = Place(z)
    w, b = at_me.w, at_me.b
    half = LANES // 2
    quarter = LANES // 4
    leg_copy = pltpu.make_async_copy(
        leg_ref.at[pl.ds(at_me.spot * z.own, z.own), pl.ds(at_me.half * z.half_lats, z.half_lats)], leg, leg_sem)
    barrier = at_me.greet()

    def local_copy(c, which):
        block = w if which == 0 else at_me.across
        return pltpu.make_async_copy(part_ref.at[block, :, c], part.at[c, which], q_sem.at[c, which])

    def core_copy(c, which):
        block = at_me.partner if which == 0 else at_me.relay
        return remote(part_ref.at[block, :, c], r1.at[c, which], c_send.at[c, which], c_recv.at[c, which], at_me.partner, b)

    def across_copy(c):
        return remote(part.at[c, 1], r2.at[c], x_send.at[c], x_recv.at[c], at_me.across, b)

    def third_copy(c, e):
        return remote(part.at[c, 0, at_me.near_spot(e)], v3.at[at_me.spot, c], a3_send.at[c, e], a3_recv.at[c, e],
                      w, at_me.near(e))

    def third_own(c):
        return pltpu.make_async_copy(part.at[c, 0, at_me.spot], v3.at[at_me.spot, c], a3_send.at[c, 0])

    def fourth_copy(c, d):
        return remote(send_u.at[c, at_me.peer(d)], out_ref.at[at_me.half, at_me.spot, c], a4_send.at[c, d],
                      a4_recv.at[c, d], w, at_me.peer(d))

    def fourth_own(c):
        return pltpu.make_async_copy(send_u.at[c, b], out_ref.at[at_me.half, at_me.spot, c], a4_send.at[c, 0])

    def transform(c):
        for s in range(z.group):
            at = s * z.lats
            real = v3[s, c, : z.pairs]
            imag = v3[s, c, z.pairs : 2 * z.pairs]
            tail = v3[s, c, 2 * z.pairs : 3 * z.pairs]
            lane = lane_of(real.shape)
            keep = lane % half < quarter
            z_all[at : at + z.pairs, :LANES] = jnp.where(lane < half, real, pltpu.roll(imag, half, 1))
            z_all[at + z.pairs : at + z.lats, :LANES] = jnp.where(lane < half, pltpu.roll(real, half, 1), imag)
            z_all[at : at + z.pairs, LANES:] = jnp.where(keep, tail, 0.0)
            z_all[at + z.pairs : at + z.lats, LANES:] = jnp.where(keep, pltpu.roll(tail, LANES - quarter, 1), 0.0)
        y = product(split2(leg[c]), split2(z_all[...]), ((0,), (0,)))
        low = z.modes // 2
        for s in range(z.bands):
            rows = y[s * z.modes : (s + 1) * z.modes]
            send_u[c, s, : z.modes] = rows[:, :LANES]
            send_u[c, s, z.modes :] = rows[:low, LANES:] + pltpu.roll(rows[low:, LANES:], quarter, 1)

    pl.semaphore_wait(barrier, z.bands + 1)

    def begin(c, carry):
        for which in (1, 0):
            core_copy(c, which).start()
            local_copy(c, which).start()
        return carry

    lax.fori_loop(0, z.own, begin, 0)
    leg_copy.start()

    def phase(p, carry):
        @pl.when(p < z.own)
        def _():
            local_copy(p, 1).wait()
            core_copy(p, 1).wait_recv()
            part[p, 1] = part[p, 1] + r1[p, 1]
            across_copy(p).start()

        @pl.when((p >= 1) & (p <= z.own))
        def _():
            c = p - 1
            local_copy(c, 0).wait()
            core_copy(c, 0).wait_recv()
            part[c, 0] = part[c, 0] + r1[c, 0]
            across_copy(c).wait_recv()
            part[c, 0] = part[c, 0] + r2[c]
            for e in range(1, z.group):
                third_copy(c, e).start()
            third_own(c).start()

        @pl.when(p == 2)
        def _():
            leg_copy.wait()

        @pl.when(p >= 2)
        def _():
            c = p - 2
            third_own(c).wait()
            for e in range(1, z.group):
                third_copy(c, e).wait_recv()
            transform(c)
            for d in range(1, z.bands):
                fourth_copy(c, d).start()
            fourth_own(c).start()

        return carry

    lax.fori_loop(0, z.own + 2, phase, 0)

    def drain(c, carry):
        across_copy(c).wait_send()
        for which in range(2):
            core_copy(c, which).wait_send()
        for e in range(1, z.group):
            third_copy(c, e).wait_send()
        for d in range(1, z.bands):
            fourth_copy(c, d).wait()
        fourth_own(c).wait()
        return carry

    lax.fori_loop(0, z.own, drain, 0)


def transform_backward(z, part, legendre):
    anywhere = pl.BlockSpec(memory_space=pl.ANY)
    dma = pltpu.SemaphoreType.DMA
    slab = (z.rows, LANES)
    return pl.pallas_call(
        lambda *refs: second_kernel(z, *refs),
        in_specs=[anywhere, anywhere],
        out_specs=anywhere,
        out_shape=jax.ShapeDtypeStruct((2, z.group, z.own, z.in_rows, LANES), f32),
        scratch_shapes=[
            pltpu.VMEM((z.own, 2, z.group) + slab, f32),
            pltpu.VMEM((z.own, 2, z.group) + slab, f32),
            pltpu.VMEM((z.own, z.group) + slab, f32),
            pltpu.VMEM((z.group, z.own) + slab, f32),
            pltpu.VMEM((z.own, z.half_lats, z.modes * z.bands), f32),
            pltpu.VMEM((z.half_lats, 2 * LANES), f32),
            pltpu.VMEM((z.own, z.bands, z.in_rows, LANES), f32),
            dma(()), dma((z.own, 2)), dma((z.own, 2)), dma((z.own, 2)), dma((z.own,)), dma((z.own,)),
            dma((z.own, z.group)), dma((z.own, z.group)), dma((z.own, z.bands)), dma((z.own, z.bands)),
        ],
        compiler_params=pltpu.CompilerParams(collective_id=1, has_side_effects=True, vmem_limit_bytes=VMEM_LIMIT),
        name="transform_backward",
    )(part, legendre)


def last_kernel(z, slabs_ref, control_ref, scale_ref, root_ref, out_ref, s_a, s_b):
    half = LANES // 2
    quarter = LANES // 4

    def unpack(m, carry):
        slab = slabs_ref[0, m] + slabs_ref[1, m]
        tail = slab[z.modes :]
        keep = lane_of(tail.shape) % half < quarter
        both = jnp.concatenate(
            [jnp.where(keep, tail, 0.0), jnp.where(keep, pltpu.roll(tail, LANES - quarter, 1), 0.0)], 0)
        s_a[pl.ds(m, z.modes, stride=z.waves), :] = slab[: z.modes]
        s_b[pl.ds(m, z.modes, stride=z.waves), :] = both
        return carry

    lax.fori_loop(0, z.waves, unpack, 0)
    root = split2(interleaved(root_ref[...]))
    order = packed_order(z.width // 2, True)
    group = 8

    def vertical(i, carry):
        at = pl.ds(pl.multiple_of(i * group * z.waves, 8), group * z.waves)
        placed = jnp.concatenate([s_a[at, :], s_b[at, :]], 1)
        scale = scale_ref[pl.ds(i * group, group)].reshape(group * z.waves, z.width)
        mixed = product(split2(scale * select_product(placed, order)), root, ((1,), (1,)))
        out_ref[pl.ds(i * group, group)] = control_ref[pl.ds(i * group, group)] + mixed.reshape(
            group, z.waves, z.width)
        return carry

    lax.fori_loop(0, z.modes // group, vertical, 0)


def finish(z, slabs, control, scale, root):
    whole_in = pl.BlockSpec(memory_space=pltpu.VMEM)
    return pl.pallas_call(
        lambda *refs: last_kernel(z, *refs),
        in_specs=[whole_in] * 4,
        out_specs=whole_in,
        out_shape=jax.ShapeDtypeStruct(control.shape, f32),
        scratch_shapes=[pltpu.VMEM((z.modes * z.waves, LANES), f32)] * 2,
        compiler_params=pltpu.CompilerParams(vmem_limit_bytes=VMEM_LIMIT),
        name="finish",
    )(slabs.reshape(2, z.waves, z.in_rows, LANES), control, scale, root)


def observation_sums(z, tracer_shape, model, arrived, lidar_coef, levels_here, proj_rows):
    lat_here, lon_here = tracer_shape
    columns, levels, lidar_vals, aod_vals, weights = [arrived[:, i].reshape(-1) for i in range(5)]
    columns = columns.astype(jnp.int32)
    levels = levels.astype(jnp.int32)
    lat_index = columns // lon_here
    lon_hot = (columns % lon_here)[:, None] == jnp.arange(lon_here, dtype=jnp.int32)[None, :]
    lat_hot = (lat_index[:, None] == jnp.arange(lat_here, dtype=jnp.int32)[None, :]).astype(jnp.float32)
    cell = lat_index * levels_here + levels
    cell_hot = (
        cell[:, None] == jnp.arange(lat_here * levels_here, dtype=jnp.int32)[None, :]
    ).astype(jnp.float32)
    lidar_field = model[:, :levels_here].reshape(lat_here * levels_here, lon_here)
    aod_field = model[:, levels_here]
    lidar_rows = jnp.dot(cell_hot, lidar_field, precision=highest)
    aod_rows = jnp.dot(lat_hot, aod_field, precision=highest)
    lidar_model = jnp.sum(jnp.where(lon_hot, lidar_rows, 0.0), axis=1)
    aod_model = jnp.sum(jnp.where(lon_hot, aod_rows, 0.0), axis=1)
    lidar_resid = weights * (lidar_model - lidar_vals)
    aod_resid = weights * (aod_model - aod_vals)
    lidar_sum = lax.dot_general(
        cell_hot, jnp.where(lon_hot, lidar_resid[:, None], 0.0), (((0,), (0,)), ((), ())), precision=highest
    )
    aod_sum = lax.dot_general(
        lat_hot, jnp.where(lon_hot, aod_resid[:, None], 0.0), (((0,), (0,)), ((), ())), precision=highest
    )
    return jnp.concatenate(
        [
            lidar_sum.reshape(lat_here, levels_here, lon_here),
            aod_sum[:, None, :],
            jnp.zeros((lat_here, proj_rows - levels_here - 1, lon_here), jnp.float32),
        ],
        axis=1,
    )


def observation_packet(obs_count, obs_column, obs_level, lidar_obs, aod_obs, obs_weight):
    slot_count = obs_column.shape[1]
    live = jnp.arange(slot_count, dtype=jnp.int32)[None, :] < obs_count.reshape(-1, 1)
    packet = jnp.stack(
        [
            obs_column.astype(jnp.float32),
            obs_level.astype(jnp.float32),
            lidar_obs,
            aod_obs,
            jnp.where(live, obs_weight, 0.0),
        ],
        axis=1,
    )
    return lax.all_to_all(packet, ("wave", "band"), split_axis=0, concat_axis=0, tiled=True)


def projection(lidar_coef, aod_coef):
    bins = lidar_coef.shape[0]
    channels = aod_coef.shape[0]
    levels_here = channels // bins
    proj_rows = -(-(levels_here + 1) // 8) * 8
    level_of = jnp.arange(channels, dtype=jnp.int32) // bins
    in_level = jnp.arange(levels_here, dtype=jnp.int32)[:, None] == level_of[None, :]
    return jnp.concatenate(
        [
            jnp.where(in_level, jnp.tile(lidar_coef, levels_here)[None, :], 0.0),
            aod_coef[None, :],
            jnp.zeros((proj_rows - levels_here - 1, channels), jnp.float32),
        ],
        axis=0,
    )


def fast_body(
    control,
    spectral_scale,
    vertical_root,
    legendre,
    zonal_number,
    courant,
    lidar_coef,
    aod_coef,
    obs_count,
    obs_column,
    obs_level,
    lidar_obs,
    aod_obs,
    obs_weight,
):
    modes_here, waves_here, width = control.shape
    wave_count = lax.axis_size("wave")
    lats_here, channels, lon_here = courant.shape
    z = Sizes(modes_here, waves_here, width, lats_here, lax.axis_size("band"), wave_count)
    lon_first = lax.axis_index("wave") * lon_here
    factor = zonal_number.shape[0] ** (-0.5)
    bins = lidar_coef.shape[0]
    levels_here = channels // bins
    arrived = observation_packet(obs_count, obs_column, obs_level, lidar_obs, aod_obs, obs_weight)
    cosine, sine = trig_tables(zonal_number, lon_first, lon_here, lon_here * wave_count, factor)
    proj = projection(lidar_coef, aod_coef)
    slabs = transform_forward(z, control, spectral_scale, vertical_root, legendre)
    tracer, model = synthesis_settle(z, slabs, cosine, sine, courant, proj, bins)
    resid = observation_sums(z, (lats_here, lon_here), model, arrived, lidar_coef, levels_here, proj.shape[0])
    part = settle_analysis(z, resid, courant, proj.T, cosine, sine, bins)
    back = transform_backward(z, part, legendre)
    return finish(z, back, control, spectral_scale, vertical_root), tracer


def fits(mesh, control, courant):
    bands, waves = mesh.shape["band"], mesh.shape["wave"]
    modes_here, waves_here = control[0] // bands, control[1] // waves
    lats_here, channels = courant[0] // bands, courant[1]
    return (
        waves == 4
        and bands % 2 == 0
        and waves_here % (bands // 2) == 0
        and waves_here % 8 == 0
        and modes_here % 16 == 0
        and lats_here % 8 == 0
        and LANES // 2 < channels <= LANES * 3 // 4
        and (channels - LANES // 2) % 8 == 0
        and courant[2] // waves % LANES == 0
    )


SPECS = (
    P("band", "wave", None),
    P("band", "wave", None),
    P(),
    P("wave", None, None),
    P(),
    P("band", None, "wave"),
    P(),
    P(),
    P(("wave", "band"), None),
    P(("wave", "band"), None),
    P(("wave", "band"), None),
    P(("wave", "band"), None),
    P(("wave", "band"), None),
    P(("wave", "band"), None),
)


def solution(mesh):
    def program(*args):
        chosen = fast_body if fits(mesh, args[0].shape, args[5].shape) else body
        return jax.shard_map(
            chosen,
            mesh=mesh,
            in_specs=SPECS,
            out_specs=(P("band", "wave", None), P("band", None, "wave")),
            check_vma=False,
        )(*args)

    return program
```

```python
import math

import jax
import jax.numpy as jnp
from jax import lax
from jax.experimental import pallas as pl
from jax.experimental.pallas import tpu as pltpu
from jax.sharding import PartitionSpec as P

MW = 224
LEV = 8
BINS = 12
STEPS = 4


highest = lax.Precision.HIGHEST
high = lax.Precision.HIGH


def trig_tables(numbers, lon_first, lon_count, lon_total, factor):
    longitudes = lon_first + jnp.arange(lon_count, dtype=jnp.int32)
    phases = numbers[:, None] * longitudes[None, :] % lon_total
    angles = phases.astype(jnp.float32) * (2.0 * math.pi / lon_total)
    return (jnp.cos(angles) * factor, jnp.sin(angles) * factor)


def settle_kernel(bins, tracer_ref, courant_ref, proj_ref, out_ref, model_ref):
    tracer = tracer_ref[0]
    courant = courant_ref[0]
    row = lax.broadcasted_iota(jnp.int32, tracer.shape, 0)
    for repeat in range(STEPS):
        outflow = courant * tracer
        inflow = jnp.where(row >= bins, pltpu.roll(outflow, bins, 0), 0.0)
        tracer = tracer - outflow + inflow
    out_ref[0] = tracer
    model_ref[0] = jnp.dot(proj_ref[...], tracer, precision=highest, preferred_element_type=jnp.float32)


def settle_adjoint_kernel(bins, resid_ref, courant_ref, proj_ref, out_ref):
    courant = courant_ref[0]
    adjoint = jnp.dot(proj_ref[...], resid_ref[0], precision=highest, preferred_element_type=jnp.float32)
    channels = adjoint.shape[0]
    row = lax.broadcasted_iota(jnp.int32, adjoint.shape, 0)
    for repeat in range(STEPS):
        below = jnp.where(row < channels - bins, pltpu.roll(adjoint, channels - bins, 0), 0.0)
        adjoint = adjoint + courant * (below - adjoint)
    out_ref[0] = adjoint


def per_lat(rows, cols):
    return pl.BlockSpec((1, rows, cols), lambda t: (t, 0, 0))


def whole(rows, cols):
    return pl.BlockSpec((rows, cols), lambda t: (0, 0))


def settle_forward(tracer, courant, proj, bins):
    lats, channels, lons = tracer.shape
    rows = proj.shape[0]
    return pl.pallas_call(
        lambda *refs: settle_kernel(bins, *refs),
        grid=(lats,),
        in_specs=[per_lat(channels, lons), per_lat(channels, lons), whole(rows, channels)],
        out_specs=[per_lat(channels, lons), per_lat(rows, lons)],
        out_shape=[
            jax.ShapeDtypeStruct((lats, channels, lons), jnp.float32),
            jax.ShapeDtypeStruct((lats, rows, lons), jnp.float32),
        ],
        name="settle_forward",
    )(tracer, courant, proj)


def settle_backward(resid, courant, proj_t, bins):
    lats, channels, lons = courant.shape
    rows = proj_t.shape[1]
    return pl.pallas_call(
        lambda *refs: settle_adjoint_kernel(bins, *refs),
        grid=(lats,),
        in_specs=[per_lat(rows, lons), per_lat(channels, lons), whole(channels, rows)],
        out_specs=per_lat(channels, lons),
        out_shape=jax.ShapeDtypeStruct((lats, channels, lons), jnp.float32),
        name="settle_backward",
    )(resid, courant, proj_t)


def synthesis_sum(cosine, sine_table, parts):
    return jnp.einsum("mo,mtc->tco", cosine, parts[..., 0], precision=high) - jnp.einsum(
        "mo,mtc->tco", sine_table, parts[..., 1], precision=high
    )


def analysis(cosine, sine_table, field):
    real_adj = jnp.einsum("mo,tco->mtc", cosine, field, precision=high)
    imag_adj = -jnp.einsum("mo,tco->mtc", sine_table, field, precision=high)
    stacked = jnp.stack([real_adj, imag_adj], axis=-1)
    return stacked.reshape(stacked.shape[0], stacked.shape[1], -1)


def body(
    control,
    spectral_scale,
    vertical_root,
    legendre,
    zonal_number,
    courant,
    lidar_coef,
    aod_coef,
    obs_count,
    obs_column,
    obs_level,
    lidar_obs,
    aod_obs,
    obs_weight,
):
    modes_here, waves_here, width = control.shape
    channels = width // 2
    wave_count = lax.axis_size("wave")
    band_count = lax.axis_size("band")
    lat_here = legendre.shape[1] // band_count
    lon_here = courant.shape[2]
    lon_total = lon_here * wave_count
    lon_first = lax.axis_index("wave") * lon_here
    factor = MW ** (-0.5)
    slot_count = obs_column.shape[1]
    live = jnp.arange(slot_count, dtype=jnp.int32)[None, :] < obs_count.reshape(-1, 1)
    packet = jnp.stack(
        [
            obs_column.astype(jnp.float32),
            obs_level.astype(jnp.float32),
            lidar_obs,
            aod_obs,
            jnp.where(live, obs_weight, 0.0),
        ],
        axis=1,
    )
    arrived = lax.all_to_all(packet, ("wave", "band"), split_axis=0, concat_axis=0, tiled=True)
    columns, levels, lidar_vals, aod_vals, weights = [arrived[:, i].reshape(-1) for i in range(5)]
    columns = columns.astype(jnp.int32)
    levels = levels.astype(jnp.int32)
    paired = control.reshape(modes_here, waves_here, channels, 2)
    mixed = jnp.einsum("nmcp,cd->nmdp", paired, vertical_root, precision=high).reshape(
        modes_here, waves_here, width
    )
    scaled = spectral_scale * mixed
    all_modes = lax.all_to_all(scaled, "band", split_axis=2, concat_axis=0, tiled=True)
    every_lat = jnp.einsum("mln,nmc->mlc", legendre, all_modes, precision=high)
    spectral = lax.all_to_all(every_lat, "band", split_axis=1, concat_axis=2, tiled=True)
    shard_piece = lax.all_gather(spectral, "wave", axis=0, tiled=True)
    numbers = zonal_number
    cosine, sine_table = trig_tables(numbers, lon_first, lon_here, lon_total, factor)
    parts = shard_piece.reshape(shard_piece.shape[0], lat_here, channels, 2)
    tracer = synthesis_sum(cosine, sine_table, parts)
    bins = lidar_coef.shape[0]
    levels_here = channels // bins
    proj_rows = -(-(levels_here + 1) // 8) * 8
    level_of = jnp.arange(channels, dtype=jnp.int32) // bins
    in_level = jnp.arange(levels_here, dtype=jnp.int32)[:, None] == level_of[None, :]
    proj = jnp.concatenate(
        [
            jnp.where(in_level, jnp.tile(lidar_coef, levels_here)[None, :], 0.0),
            aod_coef[None, :],
            jnp.zeros((proj_rows - levels_here - 1, channels), jnp.float32),
        ],
        axis=0,
    )
    tracer, model = settle_forward(tracer, courant, proj, bins)
    lat_index = columns // lon_here
    lon_hot = (columns % lon_here)[:, None] == jnp.arange(lon_here, dtype=jnp.int32)[None, :]
    lat_hot = (lat_index[:, None] == jnp.arange(lat_here, dtype=jnp.int32)[None, :]).astype(jnp.float32)
    cell = lat_index * levels_here + levels
    cell_hot = (
        cell[:, None] == jnp.arange(lat_here * levels_here, dtype=jnp.int32)[None, :]
    ).astype(jnp.float32)
    lidar_field = model[:, :levels_here].reshape(lat_here * levels_here, lon_here)
    aod_field = model[:, levels_here]
    lidar_rows = jnp.dot(cell_hot, lidar_field, precision=highest)
    aod_rows = jnp.dot(lat_hot, aod_field, precision=highest)
    lidar_model = jnp.sum(jnp.where(lon_hot, lidar_rows, 0.0), axis=1)
    aod_model = jnp.sum(jnp.where(lon_hot, aod_rows, 0.0), axis=1)
    lidar_resid = weights * (lidar_model - lidar_vals)
    aod_resid = weights * (aod_model - aod_vals)
    lidar_sum = lax.dot_general(
        cell_hot, jnp.where(lon_hot, lidar_resid[:, None], 0.0), (((0,), (0,)), ((), ())), precision=highest
    )
    aod_sum = lax.dot_general(
        lat_hot, jnp.where(lon_hot, aod_resid[:, None], 0.0), (((0,), (0,)), ((), ())), precision=highest
    )
    resid = jnp.concatenate(
        [
            lidar_sum.reshape(lat_here, levels_here, lon_here),
            aod_sum[:, None, :],
            jnp.zeros((lat_here, proj_rows - levels_here - 1, lon_here), jnp.float32),
        ],
        axis=1,
    )
    adjoint = settle_backward(resid, courant, proj.T, bins)
    numbers = zonal_number
    cosine, sine_table = trig_tables(numbers, lon_first, lon_here, lon_total, factor)
    spectral_adj = lax.psum_scatter(
        analysis(cosine, sine_table, adjoint), "wave", scatter_dimension=0, tiled=True
    )
    all_lats = lax.all_to_all(spectral_adj, "band", split_axis=2, concat_axis=1, tiled=True)
    mode_block = jnp.einsum("mtn,mtc->nmc", legendre, all_lats, precision=high)
    scaled_adj = lax.all_to_all(mode_block, "band", split_axis=0, concat_axis=2, tiled=True)
    mixed_adj = (spectral_scale * scaled_adj).reshape(modes_here, waves_here, channels, 2)
    control_adj = jnp.einsum("nmdp,cd->nmcp", mixed_adj, vertical_root, precision=high).reshape(
        modes_here, waves_here, width
    )
    return (control + control_adj, tracer)


LANES = 128
MESH_ID = pl.DeviceIdType.MESH
bf16 = jnp.bfloat16
f32 = jnp.float32
VMEM_LIMIT = 63 * 1024 * 1024


def split2(x):
    hi = x.astype(bf16)
    return hi, (x - hi.astype(f32)).astype(bf16)


def split3(x):
    hi, lo = split2(x)
    rest = x - hi.astype(f32)
    return hi, lo, (rest - lo.astype(f32)).astype(bf16)


def product(a, b, dims=((1,), (0,))):
    def one(x, y):
        return lax.dot_general(x, y, (dims, ((), ())), preferred_element_type=f32)

    return one(a[1], b[0]) + one(a[0], b[1]) + one(a[0], b[0])


def lane_of(shape):
    return lax.broadcasted_iota(jnp.int32, shape, len(shape) - 1)


def packed_order(channels, transposed):
    half = LANES // 2
    width = 2 * channels
    shape = (2 * LANES, width) if transposed else (width, 2 * LANES)
    source = lax.broadcasted_iota(jnp.int32, shape, 1 if transposed else 0)
    target = lax.broadcasted_iota(jnp.int32, shape, 0 if transposed else 1)
    channel = source // 2
    place = jnp.where(channel < half, channel, channel + half) + (source % 2) * half
    return jnp.where(place == target, 1.0, 0.0).astype(bf16)


def select_product(x, matrix):
    return sum(
        lax.dot_general(piece, matrix, (((1,), (0,)), ((), ())), preferred_element_type=f32)
        for piece in reversed(split3(x))
    )


def interleaved(root):
    channels = root.shape[0]
    wide = 2 * channels
    spread = (lax.broadcasted_iota(jnp.int32, (wide, channels), 0) // 2
              == lax.broadcasted_iota(jnp.int32, (wide, channels), 1))
    gather = (lax.broadcasted_iota(jnp.int32, (channels, wide), 1) // 2
              == lax.broadcasted_iota(jnp.int32, (channels, wide), 0))
    spread = jnp.where(spread, 1.0, 0.0).astype(bf16)
    gather = jnp.where(gather, 1.0, 0.0).astype(bf16)
    both = select_product(root, gather)
    both = sum(jnp.dot(spread, piece, preferred_element_type=f32) for piece in reversed(split3(both)))
    same = (lax.broadcasted_iota(jnp.int32, both.shape, 0) % 2) == (lax.broadcasted_iota(jnp.int32, both.shape, 1) % 2)
    return jnp.where(same, both, 0.0)


class Sizes:
    def __init__(self, modes, waves, width, lats, bands, wave_count):
        self.modes, self.waves, self.width, self.lats = modes, waves, width, lats
        self.bands, self.wave_count = bands, wave_count
        self.group = bands // 2
        self.own = waves // self.group
        self.half_lats = lats * self.group
        self.pairs = lats // 2
        self.rows = -(-(3 * self.pairs) // 8) * 8
        self.in_rows = modes + modes // 2
        self.slots = waves * wave_count


class Place:
    def __init__(self, z):
        self.w, self.b = lax.axis_index("wave"), lax.axis_index("band")
        self.partner = self.w + 1 - 2 * (self.w % 2)
        self.across = (self.w + 2) % z.wave_count
        self.relay = (self.partner + 2) % z.wave_count
        self.half, self.spot = self.b // z.group, self.b % z.group
        self.z = z

    def peer(self, d):
        return (self.b + d) % self.z.bands

    def near_spot(self, e):
        return (self.spot + e) % self.z.group

    def near(self, e):
        return self.half * self.z.group + self.near_spot(e)

    def greet(self):
        barrier = pltpu.get_barrier_semaphore()
        others = [(self.w, self.peer(d)) for d in range(1, self.z.bands)]
        for wave, band in others + [(self.partner, self.b), (self.across, self.b)]:
            pl.semaphore_signal(barrier, inc=1, device_id={"wave": wave, "band": band}, device_id_type=MESH_ID)
        return barrier


def remote(src, dst, send, recv, wave, band):
    return pltpu.make_async_remote_copy(
        src, dst, send, recv, device_id={"wave": wave, "band": band}, device_id_type=MESH_ID)


AHEAD = 2
LAG_SPREAD = 2
LAG_ACROSS = 2
GROUP_ROWS = 8


def first_kernel(z, control_ref, scale_ref, root_ref, leg_ref, count_ref, column_ref, level_ref, lidar_ref, aod_ref,
                 weight_ref, out_ref, seen_ref, control, scale, s_a, s_b, send_u, recv_v, leg, y_a, y_b, send_y, packet,
                 leg_sem, in_sem, o_send, o_recv, a1_send, a1_recv, a2_send, a2_recv, x_send, x_recv, c_send, c_recv):
    at_me = Place(z)
    w, b = at_me.w, at_me.b
    half = LANES // 2
    quarter = LANES // 4
    phases = GROUP_ROWS // z.group
    groups = z.waves // GROUP_ROWS
    devices = z.wave_count * z.bands
    me = w * z.bands + b

    def input_copy(i, which):
        source, target = ((control_ref, control), (scale_ref, scale))[which]
        return pltpu.make_async_copy(
            source.at[:, pl.ds(i * GROUP_ROWS, GROUP_ROWS), :], target.at[i], in_sem.at[i, which])

    for i in range(groups):
        for which in range(2):
            input_copy(i, which).start()
    leg_copy = pltpu.make_async_copy(
        leg_ref.at[:, at_me.spot, pl.ds(at_me.half * z.half_lats, z.half_lats)], leg, leg_sem)
    leg_copy.start()
    barrier = pltpu.get_barrier_semaphore()

    def greet(e, carry):
        to = (me + e) % devices
        pl.semaphore_signal(barrier, inc=1, device_id={"wave": to // z.bands, "band": to % z.bands},
                            device_id_type=MESH_ID)
        return carry

    lax.fori_loop(1, devices, greet, 0)

    counts = jnp.broadcast_to(count_ref[...], (devices, devices))
    diagonal = lax.broadcasted_iota(jnp.int32, counts.shape, 0) == lax.broadcasted_iota(jnp.int32, counts.shape, 1)
    counts = jnp.sum(jnp.where(diagonal, counts, 0).astype(f32), axis=1, keepdims=True)
    weights = weight_ref[...]
    live = lax.broadcasted_iota(jnp.int32, weights.shape, 1).astype(f32) < counts
    fields = (column_ref[...].astype(f32), level_ref[...].astype(f32), lidar_ref[...], aod_ref[...],
              jnp.where(live, weights, 0.0))
    for k in range(GROUP_ROWS):
        value = fields[k] if k < len(fields) else jnp.zeros_like(weights)
        packet[pl.ds(k, devices, stride=GROUP_ROWS), :] = value

    def packet_copy(e):
        to = (me + e) % devices
        return remote(packet.at[pl.ds(to * GROUP_ROWS, GROUP_ROWS)], seen_ref.at[pl.ds(me * GROUP_ROWS, GROUP_ROWS)],
                      o_send.at[e], o_recv.at[e], to // z.bands, to % z.bands)

    packet_own = pltpu.make_async_copy(
        packet.at[pl.ds(me * GROUP_ROWS, GROUP_ROWS)], seen_ref.at[pl.ds(me * GROUP_ROWS, GROUP_ROWS)], o_send.at[0])

    root = split2(interleaved(root_ref[...]))
    order = packed_order(z.width // 2, False)

    def vertical(i):
        for which in range(2):
            input_copy(i, which).wait()
        x = control[i].reshape(z.modes * GROUP_ROWS, z.width)
        y = scale[i].reshape(z.modes * GROUP_ROWS, z.width)
        placed = select_product(y * product(split2(x), root), order)
        s_a[...] = placed[:, :LANES]
        s_b[...] = placed[:, LANES:]

    def first_copy(c, d):
        to = at_me.peer(d)
        return remote(send_u.at[c, to % z.group], recv_v.at[b, c], a1_send.at[c, d], a1_recv.at[c, d], w, to)

    def first_own(c):
        return pltpu.make_async_copy(send_u.at[c, at_me.spot], recv_v.at[b, c], a1_send.at[c, 0])

    def launch(c):
        @pl.when(c % phases == 0)
        def _():
            vertical(c // phases)

        low = z.modes // 2
        for spot in range(z.group):
            at = pl.ds(c % phases * z.group + spot, z.modes, stride=GROUP_ROWS)
            tall = s_b[at, :]
            send_u[c, spot, : z.modes] = s_a[at, :]
            send_u[c, spot, z.modes :] = tall[:low] + pltpu.roll(tall[low:], quarter, 1)
        for d in range(1, z.bands):
            first_copy(c, d).start()
        first_own(c).start()

    def second_copy(c, e):
        return remote(send_y.at[c, at_me.near_spot(e)], out_ref.at[w, c, at_me.spot], a2_send.at[c, e], a2_recv.at[c, e],
                      w, at_me.near(e))

    def second_own(c):
        return pltpu.make_async_copy(send_y.at[c, at_me.spot], out_ref.at[w, c, at_me.spot], a2_send.at[c, 0])

    def across_copy(c):
        return remote(out_ref.at[w, c], out_ref.at[w, c], x_send.at[c], x_recv.at[c], at_me.across, b)

    def core_copy(c, which):
        block = w if which == 0 else at_me.across
        return remote(out_ref.at[block, c], out_ref.at[block, c], c_send.at[c, which], c_recv.at[c, which],
                      at_me.partner, b)

    def transform(c):
        tops, tails = [], []
        for s in range(z.bands):
            tail = recv_v[s, c, z.modes :]
            keep = lane_of(tail.shape) % half < quarter
            tops.append(recv_v[s, c, : z.modes])
            tails.append(jnp.where(keep, tail, 0.0))
            tails.append(jnp.where(keep, pltpu.roll(tail, LANES - quarter, 1), 0.0))
        x = jnp.concatenate([jnp.concatenate(tops, 0), jnp.concatenate(tails, 0)], 1)
        y = product(split2(leg[c]), split2(x))
        y_a[...] = y[:, :LANES]
        y_b[...] = y[:, LANES:]
        for s in range(z.group):
            at = s * z.lats
            one = y_a[at : at + z.pairs]
            two = y_a[at + z.pairs : at + z.lats]
            left = lane_of(one.shape) < half
            send_y[c, s, z.rows - 8 :] = jnp.zeros((8, LANES), f32)
            send_y[c, s, : z.pairs] = jnp.where(left, one, pltpu.roll(two, half, 1))
            send_y[c, s, z.pairs : 2 * z.pairs] = jnp.where(left, pltpu.roll(one, half, 1), two)
            send_y[c, s, 2 * z.pairs : 3 * z.pairs] = y_b[at : at + z.pairs] + pltpu.roll(
                y_b[at + z.pairs : at + z.lats], quarter, 1)

    pl.semaphore_wait(barrier, devices - 1)
    for c in range(min(AHEAD, z.own)):
        launch(c)

    def send_packet(e, carry):
        packet_copy(e).start()
        return carry

    lax.fori_loop(1, devices, send_packet, 0)
    packet_own.start()
    leg_copy.wait()

    def phase(p, carry):
        @pl.when(p + AHEAD < z.own)
        def _():
            launch(p + AHEAD)

        @pl.when(p < z.own)
        def _():
            first_own(p).wait()
            for d in range(1, z.bands):
                first_copy(p, d).wait_recv()
            transform(p)
            for e in range(1, z.group):
                second_copy(p, e).start()
            second_own(p).start()

        @pl.when((p >= LAG_SPREAD) & (p < z.own + LAG_SPREAD))
        def _():
            c = p - LAG_SPREAD
            for e in range(1, z.group):
                second_copy(c, e).wait_recv()
            second_own(c).wait()
            across_copy(c).start()
            core_copy(c, 0).start()

        @pl.when(p >= LAG_SPREAD + LAG_ACROSS)
        def _():
            c = p - LAG_SPREAD - LAG_ACROSS
            across_copy(c).wait_recv()
            core_copy(c, 1).start()

        return carry

    lax.fori_loop(0, z.own + LAG_SPREAD + LAG_ACROSS, phase, 0)

    def drain(c, carry):
        for d in range(1, z.bands):
            first_copy(c, d).wait_send()
        for e in range(1, z.group):
            second_copy(c, e).wait_send()
        across_copy(c).wait_send()
        for which in range(2):
            core_copy(c, which).wait()
        return carry

    lax.fori_loop(0, z.own, drain, 0)

    def drain_packet(e, carry):
        packet_copy(e).wait()
        return carry

    lax.fori_loop(1, devices, drain_packet, 0)
    packet_own.wait()


def transform_forward(z, control, scale, root, legendre, observed):
    in_vmem = pl.BlockSpec(memory_space=pltpu.VMEM)
    anywhere = pl.BlockSpec(memory_space=pl.ANY)
    dma = pltpu.SemaphoreType.DMA
    devices = z.wave_count * z.bands
    groups = z.waves // GROUP_ROWS
    block = (groups, z.modes, GROUP_ROWS, z.width)
    return pl.pallas_call(
        lambda *refs: first_kernel(z, *refs),
        in_specs=[anywhere, anywhere, in_vmem, anywhere] + [in_vmem] * 6,
        out_specs=[anywhere, anywhere],
        out_shape=[
            jax.ShapeDtypeStruct((z.wave_count, z.own, z.group, z.rows, LANES), f32),
            jax.ShapeDtypeStruct((devices * GROUP_ROWS, LANES), f32),
        ],
        scratch_shapes=[
            pltpu.VMEM(block, f32),
            pltpu.VMEM(block, f32),
            pltpu.VMEM((z.modes * GROUP_ROWS, LANES), f32),
            pltpu.VMEM((z.modes * GROUP_ROWS, LANES), f32),
            pltpu.VMEM((z.own, z.group, z.in_rows, LANES), f32),
            pltpu.VMEM((z.bands, z.own, z.in_rows, LANES), f32),
            pltpu.VMEM((z.own, z.half_lats, z.modes * z.bands), f32),
            pltpu.VMEM((z.half_lats, LANES), f32),
            pltpu.VMEM((z.half_lats, LANES), f32),
            pltpu.VMEM((z.own, z.group, z.rows, LANES), f32),
            pltpu.VMEM((devices * GROUP_ROWS, LANES), f32),
            dma(()), dma((groups, 2)), dma((devices,)), dma((devices,)),
            dma((z.own, z.bands)), dma((z.own, z.bands)), dma((z.own, z.group)), dma((z.own, z.group)),
            dma((z.own,)), dma((z.own,)), dma((z.own, 2)), dma((z.own, 2)),
        ],
        compiler_params=pltpu.CompilerParams(collective_id=0, has_side_effects=True, vmem_limit_bytes=VMEM_LIMIT),
        name="transform_forward",
    )(control, scale, root, legendre.reshape(z.own, z.group, *legendre.shape[1:]), *observed)


def synthesis_kernel(z, bins, slabs_ref, cos_ref, sin_ref, courant_ref, proj_ref, out_ref, model_ref, c_hi, c_lo, n_hi, n_lo):
    i = pl.program_id(0)
    half = LANES // 2

    @pl.when(i == 0)
    def _():
        c_hi[...], c_lo[...] = split2(cos_ref[...])
        n_hi[...], n_lo[...] = split2(-sin_ref[...])

    def slab(row):
        return slabs_ref[pl.ds(row, z.slots, stride=z.rows), :]

    tail = slab(2 * z.pairs + i)
    real = jnp.concatenate([slab(i), tail], 1)
    imag = jnp.concatenate([slab(z.pairs + i), pltpu.roll(tail, half, 1)], 1)
    over_waves = ((0,), (0,))
    field = product(split2(real), (c_hi[...], c_lo[...]), over_waves) + product(
        split2(imag), (n_hi[...], n_lo[...]), over_waves)
    channels = z.width // 2
    rest = channels - half
    proj = split2(proj_ref[...])
    for which in range(2):
        tracer = jnp.concatenate(
            [field[which * half : (which + 1) * half],
             field[LANES + which * (half // 2) : LANES + which * (half // 2) + rest]], 0)
        courant = courant_ref[which, 0]
        row = lax.broadcasted_iota(jnp.int32, tracer.shape, 0)
        for repeat in range(STEPS):
            outflow = courant * tracer
            inflow = jnp.where(row >= bins, pltpu.roll(outflow, bins, 0), 0.0)
            tracer = tracer - outflow + inflow
        out_ref[which, 0] = tracer
        model_ref[which, 0] = product(proj, split2(tracer))


def paired(rows, cols):
    return pl.BlockSpec((2, 1, rows, cols), lambda i: (0, i, 0, 0))


def synthesis_settle(z, slabs, cosine, sine, courant, proj, bins):
    lats, channels, lons = courant.shape
    rows = proj.shape[0]
    tracer, model = pl.pallas_call(
        lambda *refs: synthesis_kernel(z, bins, *refs),
        grid=(z.pairs,),
        in_specs=[whole(z.slots * z.rows, LANES), whole(z.slots, lons), whole(z.slots, lons), paired(channels, lons),
                  whole(rows, channels)],
        out_specs=[paired(channels, lons), paired(rows, lons)],
        out_shape=[
            jax.ShapeDtypeStruct((2, z.pairs, channels, lons), f32),
            jax.ShapeDtypeStruct((2, z.pairs, rows, lons), f32),
        ],
        scratch_shapes=[pltpu.VMEM((z.slots, lons), bf16)] * 4,
        compiler_params=pltpu.CompilerParams(vmem_limit_bytes=VMEM_LIMIT),
        name="synthesis_settle",
    )(slabs.reshape(z.slots * z.rows, LANES), cosine, sine, courant.reshape(2, z.pairs, channels, lons), proj)
    return tracer.reshape(lats, channels, lons), model.reshape(lats, rows, lons)


def analysis_kernel(z, bins, resid_ref, courant_ref, proj_ref, cos_ref, sin_ref, out_ref, c_hi, c_lo, n_hi, n_lo):
    i = pl.program_id(0)
    half = LANES // 2

    @pl.when(i == 0)
    def _():
        c_hi[...], c_lo[...] = split2(cos_ref[...])
        n_hi[...], n_lo[...] = split2(-sin_ref[...])

    proj = split2(proj_ref[...])
    fields = []
    for which in range(2):
        courant = courant_ref[which, 0]
        adjoint = product(proj, split2(resid_ref[which, 0]))
        channels = adjoint.shape[0]
        row = lax.broadcasted_iota(jnp.int32, adjoint.shape, 0)
        for repeat in range(STEPS):
            below = jnp.where(row < channels - bins, pltpu.roll(adjoint, channels - bins, 0), 0.0)
            adjoint = adjoint + courant * (below - adjoint)
        fields.append(adjoint)
    gap = jnp.zeros((half // 2 - (channels - half), fields[0].shape[1]), f32)
    pieces = [field[:half] for field in fields]
    for field in fields:
        pieces.append(field[half:])
        if gap.shape[0]:
            pieces.append(gap)
    pieces.append(jnp.zeros((half, fields[0].shape[1]), f32))
    both = split2(jnp.concatenate(pieces, 0))
    over_lons = ((1,), (1,))
    real = product((c_hi[...], c_lo[...]), both, over_lons)
    imag = product((n_hi[...], n_lo[...]), both, over_lons)

    @pl.when(i == 0)
    def _():
        for spare in range(3 * z.pairs, z.rows):
            out_ref[pl.ds(spare, z.slots, stride=z.rows), :] = jnp.zeros((z.slots, LANES), f32)

    out_ref[pl.ds(i, z.slots, stride=z.rows), :] = real[:, :LANES]
    out_ref[pl.ds(z.pairs + i, z.slots, stride=z.rows), :] = imag[:, :LANES]
    out_ref[pl.ds(2 * z.pairs + i, z.slots, stride=z.rows), :] = real[:, LANES:] + pltpu.roll(imag[:, LANES:], half, 1)


def settle_analysis(z, resid, courant, proj_t, cosine, sine, bins):
    lats, channels, lons = courant.shape
    rows = proj_t.shape[1]
    out = pl.pallas_call(
        lambda *refs: analysis_kernel(z, bins, *refs),
        grid=(z.pairs,),
        in_specs=[paired(rows, lons), paired(channels, lons), whole(channels, rows), whole(z.slots, lons),
                  whole(z.slots, lons)],
        out_specs=whole(z.slots * z.rows, LANES),
        out_shape=jax.ShapeDtypeStruct((z.slots * z.rows, LANES), f32),
        scratch_shapes=[pltpu.VMEM((z.slots, lons), bf16)] * 4,
        compiler_params=pltpu.CompilerParams(vmem_limit_bytes=VMEM_LIMIT),
        name="settle_analysis",
    )(resid.reshape(2, z.pairs, rows, lons), courant.reshape(2, z.pairs, channels, lons), proj_t, cosine, sine)
    return out.reshape(z.wave_count, z.own, z.group, z.rows, LANES)


def second_kernel(z, part_ref, leg_ref, out_ref, part, r1, r2, v3, leg, z_all, send_u,
                  leg_sem, q_sem, c_send, c_recv, x_send, x_recv, a3_send, a3_recv, a4_send, a4_recv):
    at_me = Place(z)
    w, b = at_me.w, at_me.b
    half = LANES // 2
    quarter = LANES // 4
    leg_copy = pltpu.make_async_copy(
        leg_ref.at[:, at_me.spot, pl.ds(at_me.half * z.half_lats, z.half_lats)], leg, leg_sem)
    barrier = at_me.greet()

    def local_copy(c, which):
        block = w if which == 0 else at_me.across
        return pltpu.make_async_copy(part_ref.at[block, c], part.at[c, which], q_sem.at[c, which])

    def core_copy(c, which):
        block = at_me.partner if which == 0 else at_me.relay
        return remote(part_ref.at[block, c], r1.at[c, which], c_send.at[c, which], c_recv.at[c, which], at_me.partner, b)

    def across_copy(c):
        return remote(part.at[c, 1], r2.at[c], x_send.at[c], x_recv.at[c], at_me.across, b)

    def third_copy(c, e):
        return remote(part.at[c, 0, at_me.near_spot(e)], v3.at[at_me.spot, c], a3_send.at[c, e], a3_recv.at[c, e],
                      w, at_me.near(e))

    def third_own(c):
        return pltpu.make_async_copy(part.at[c, 0, at_me.spot], v3.at[at_me.spot, c], a3_send.at[c, 0])

    def fourth_copy(c, d):
        return remote(send_u.at[c, at_me.peer(d)], out_ref.at[at_me.half, c, at_me.spot], a4_send.at[c, d],
                      a4_recv.at[c, d], w, at_me.peer(d))

    def fourth_own(c):
        return pltpu.make_async_copy(send_u.at[c, b], out_ref.at[at_me.half, c, at_me.spot], a4_send.at[c, 0])

    def transform(c):
        for s in range(z.group):
            at = s * z.lats
            real = v3[s, c, : z.pairs]
            imag = v3[s, c, z.pairs : 2 * z.pairs]
            tail = v3[s, c, 2 * z.pairs : 3 * z.pairs]
            lane = lane_of(real.shape)
            keep = lane % half < quarter
            z_all[at : at + z.pairs, :LANES] = jnp.where(lane < half, real, pltpu.roll(imag, half, 1))
            z_all[at + z.pairs : at + z.lats, :LANES] = jnp.where(lane < half, pltpu.roll(real, half, 1), imag)
            z_all[at : at + z.pairs, LANES:] = jnp.where(keep, tail, 0.0)
            z_all[at + z.pairs : at + z.lats, LANES:] = jnp.where(keep, pltpu.roll(tail, LANES - quarter, 1), 0.0)
        y = product(split2(leg[c]), split2(z_all[...]), ((0,), (0,)))
        low = z.modes // 2
        for s in range(z.bands):
            rows = y[s * z.modes : (s + 1) * z.modes]
            send_u[c, s, : z.modes] = rows[:, :LANES]
            send_u[c, s, z.modes :] = rows[:low, LANES:] + pltpu.roll(rows[low:, LANES:], quarter, 1)

    pl.semaphore_wait(barrier, z.bands + 1)

    def begin(c, carry):
        for which in (1, 0):
            core_copy(c, which).start()
            local_copy(c, which).start()
        return carry

    lax.fori_loop(0, z.own, begin, 0)
    leg_copy.start()

    def phase(p, carry):
        @pl.when(p < z.own)
        def _():
            local_copy(p, 1).wait()
            core_copy(p, 1).wait_recv()
            part[p, 1] = part[p, 1] + r1[p, 1]
            across_copy(p).start()

        @pl.when((p >= LAG_ACROSS) & (p < z.own + LAG_ACROSS))
        def _():
            c = p - LAG_ACROSS
            local_copy(c, 0).wait()
            core_copy(c, 0).wait_recv()
            part[c, 0] = part[c, 0] + r1[c, 0]
            across_copy(c).wait_recv()
            part[c, 0] = part[c, 0] + r2[c]
            for e in range(1, z.group):
                third_copy(c, e).start()
            third_own(c).start()

        @pl.when(p == LAG_ACROSS + LAG_SPREAD)
        def _():
            leg_copy.wait()

        @pl.when(p >= LAG_ACROSS + LAG_SPREAD)
        def _():
            c = p - LAG_ACROSS - LAG_SPREAD
            third_own(c).wait()
            for e in range(1, z.group):
                third_copy(c, e).wait_recv()
            transform(c)
            for d in range(1, z.bands):
                fourth_copy(c, d).start()
            fourth_own(c).start()

        return carry

    lax.fori_loop(0, z.own + LAG_ACROSS + LAG_SPREAD, phase, 0)

    def drain(c, carry):
        across_copy(c).wait_send()
        for which in range(2):
            core_copy(c, which).wait_send()
        for e in range(1, z.group):
            third_copy(c, e).wait_send()
        for d in range(1, z.bands):
            fourth_copy(c, d).wait()
        fourth_own(c).wait()
        return carry

    lax.fori_loop(0, z.own, drain, 0)


def transform_backward(z, part, legendre):
    anywhere = pl.BlockSpec(memory_space=pl.ANY)
    dma = pltpu.SemaphoreType.DMA
    slab = (z.rows, LANES)
    return pl.pallas_call(
        lambda *refs: second_kernel(z, *refs),
        in_specs=[anywhere, anywhere],
        out_specs=anywhere,
        out_shape=jax.ShapeDtypeStruct((2, z.own, z.group, z.in_rows, LANES), f32),
        scratch_shapes=[
            pltpu.VMEM((z.own, 2, z.group) + slab, f32),
            pltpu.VMEM((z.own, 2, z.group) + slab, f32),
            pltpu.VMEM((z.own, z.group) + slab, f32),
            pltpu.VMEM((z.group, z.own) + slab, f32),
            pltpu.VMEM((z.own, z.half_lats, z.modes * z.bands), f32),
            pltpu.VMEM((z.half_lats, 2 * LANES), f32),
            pltpu.VMEM((z.own, z.bands, z.in_rows, LANES), f32),
            dma(()), dma((z.own, 2)), dma((z.own, 2)), dma((z.own, 2)), dma((z.own,)), dma((z.own,)),
            dma((z.own, z.group)), dma((z.own, z.group)), dma((z.own, z.bands)), dma((z.own, z.bands)),
        ],
        compiler_params=pltpu.CompilerParams(collective_id=1, has_side_effects=True, vmem_limit_bytes=VMEM_LIMIT),
        name="transform_backward",
    )(part, legendre.reshape(z.own, z.group, *legendre.shape[1:]))


def last_kernel(z, slabs_ref, control_ref, scale_ref, root_ref, out_ref, s_a, s_b, r_hi, r_lo):
    half = LANES // 2
    quarter = LANES // 4

    @pl.when(pl.program_id(0) == 0)
    def _():
        r_hi[...], r_lo[...] = split2(interleaved(root_ref[...]))

    for m in range(GROUP_ROWS):
        slab = slabs_ref[0, m] + slabs_ref[1, m]
        tail = slab[z.modes :]
        keep = lane_of(tail.shape) % half < quarter
        both = jnp.concatenate(
            [jnp.where(keep, tail, 0.0), jnp.where(keep, pltpu.roll(tail, LANES - quarter, 1), 0.0)], 0)
        s_a[pl.ds(m, z.modes, stride=GROUP_ROWS), :] = slab[: z.modes]
        s_b[pl.ds(m, z.modes, stride=GROUP_ROWS), :] = both
    order = packed_order(z.width // 2, True)
    placed = jnp.concatenate([s_a[...], s_b[...]], 1)
    scale = scale_ref[...].reshape(z.modes * GROUP_ROWS, z.width)
    mixed = product(split2(scale * select_product(placed, order)), (r_hi[...], r_lo[...]), ((1,), (1,)))
    out_ref[...] = control_ref[...] + mixed.reshape(z.modes, GROUP_ROWS, z.width)


def finish(z, slabs, control, scale, root):
    by_waves = pl.BlockSpec((z.modes, GROUP_ROWS, z.width), lambda i: (0, i, 0))
    return pl.pallas_call(
        lambda *refs: last_kernel(z, *refs),
        grid=(z.waves // GROUP_ROWS,),
        in_specs=[
            pl.BlockSpec((2, GROUP_ROWS, z.in_rows, LANES), lambda i: (0, i, 0, 0)),
            by_waves, by_waves, whole(*root.shape),
        ],
        out_specs=by_waves,
        out_shape=jax.ShapeDtypeStruct(control.shape, f32),
        scratch_shapes=[pltpu.VMEM((z.modes * GROUP_ROWS, LANES), f32)] * 2 + [pltpu.VMEM((z.width, z.width), bf16)] * 2,
        compiler_params=pltpu.CompilerParams(vmem_limit_bytes=VMEM_LIMIT),
        name="finish",
    )(slabs.reshape(2, z.waves, z.in_rows, LANES), control, scale, root)


OBS_ROWS = 4


def observation_kernel(levels, model_ref, seen_ref, out_ref, lidar_acc, aod_acc):
    lats, rows, lons = model_ref.shape
    cells = lats * levels
    devices = seen_ref.shape[0] // GROUP_ROWS
    slots = OBS_ROWS * seen_ref.shape[1]

    def halves(x):
        return jnp.concatenate(split2(x.T), 0)

    lidar_field = halves(model_ref[:, :levels, :].reshape(cells, lons))
    aod_field = halves(jnp.sum(model_ref[:, levels:, :], axis=1))
    lidar_acc[...] = jnp.zeros_like(lidar_acc)
    aod_acc[...] = jnp.zeros_like(aod_acc)
    over_slots = ((1,), (1,))

    def step(i, carry):
        def row(k):
            first = i * OBS_ROWS * GROUP_ROWS + k
            return jnp.concatenate([seen_ref[pl.ds(first + r * GROUP_ROWS, 1), :] for r in range(OBS_ROWS)], 1)

        column = row(0).astype(jnp.int32)
        lat = column // lons
        lon_hot = lax.broadcasted_iota(jnp.int32, (lons, slots), 0) == column - lat * lons
        cell = lat * levels + row(1).astype(jnp.int32)
        cell_hot = jnp.where(lax.broadcasted_iota(jnp.int32, (cells, slots), 0) == cell, 1.0, 0.0).astype(bf16)
        lat_hot = jnp.where(lax.broadcasted_iota(jnp.int32, (lats, slots), 0) == lat, 1.0, 0.0).astype(bf16)
        weight = row(4)

        def one(field, hot, observed, acc):
            picked = jnp.dot(field, hot, preferred_element_type=f32)
            picked = picked[:lons] + picked[lons:]
            resid = weight * (jnp.sum(jnp.where(lon_hot, picked, 0.0), axis=0, keepdims=True) - observed)
            hi, lo = (jnp.where(lon_hot, part.astype(f32), 0.0).astype(bf16) for part in split2(resid))
            acc[...] += lax.dot_general(hot, hi, (over_slots, ((), ())), preferred_element_type=f32) + lax.dot_general(
                hot, lo, (over_slots, ((), ())), preferred_element_type=f32)

        one(lidar_field, cell_hot, row(2), lidar_acc)
        one(aod_field, lat_hot, row(3), aod_acc)
        return carry

    lax.fori_loop(0, devices // OBS_ROWS, step, 0)
    out_ref[:, :levels, :] = lidar_acc[...].reshape(lats, levels, lons)
    spread = jnp.broadcast_to(aod_acc[...][:, None, :], (lats, rows - levels, lons))
    first = lax.broadcasted_iota(jnp.int32, spread.shape, 1) == 0
    out_ref[:, levels:, :] = jnp.where(first, spread, 0.0)


def observation_sums(model, seen, levels):
    in_vmem = pl.BlockSpec(memory_space=pltpu.VMEM)
    lats, rows, lons = model.shape
    return pl.pallas_call(
        lambda *refs: observation_kernel(levels, *refs),
        in_specs=[in_vmem, in_vmem],
        out_specs=in_vmem,
        out_shape=jax.ShapeDtypeStruct(model.shape, f32),
        scratch_shapes=[pltpu.VMEM((lats * levels, lons), f32), pltpu.VMEM((lats, lons), f32)],
        compiler_params=pltpu.CompilerParams(vmem_limit_bytes=VMEM_LIMIT),
        name="observation_sums",
    )(model, seen)


def projection(lidar_coef, aod_coef):
    bins = lidar_coef.shape[0]
    channels = aod_coef.shape[0]
    levels_here = channels // bins
    proj_rows = -(-(levels_here + 1) // 8) * 8
    level_of = jnp.arange(channels, dtype=jnp.int32) // bins
    in_level = jnp.arange(levels_here, dtype=jnp.int32)[:, None] == level_of[None, :]
    return jnp.concatenate(
        [
            jnp.where(in_level, jnp.tile(lidar_coef, levels_here)[None, :], 0.0),
            aod_coef[None, :],
            jnp.zeros((proj_rows - levels_here - 1, channels), jnp.float32),
        ],
        axis=0,
    )


def fast_body(
    control,
    spectral_scale,
    vertical_root,
    legendre,
    zonal_number,
    courant,
    lidar_coef,
    aod_coef,
    obs_count,
    obs_column,
    obs_level,
    lidar_obs,
    aod_obs,
    obs_weight,
):
    modes_here, waves_here, width = control.shape
    wave_count = lax.axis_size("wave")
    lats_here, channels, lon_here = courant.shape
    z = Sizes(modes_here, waves_here, width, lats_here, lax.axis_size("band"), wave_count)
    lon_first = lax.axis_index("wave") * lon_here
    factor = zonal_number.shape[0] ** (-0.5)
    bins = lidar_coef.shape[0]
    levels_here = channels // bins
    cosine, sine = trig_tables(zonal_number, lon_first, lon_here, lon_here * wave_count, factor)
    proj = projection(lidar_coef, aod_coef)
    observed = (obs_count, obs_column, obs_level, lidar_obs, aod_obs, obs_weight)
    slabs, seen = transform_forward(z, control, spectral_scale, vertical_root, legendre, observed)
    tracer, model = synthesis_settle(z, slabs, cosine, sine, courant, proj, bins)
    resid = observation_sums(model, seen, levels_here)
    part = settle_analysis(z, resid, courant, proj.T, cosine, sine, bins)
    back = transform_backward(z, part, legendre)
    return finish(z, back, control, spectral_scale, vertical_root), tracer


def fits(mesh, control, courant, columns, bins):
    bands, waves = mesh.shape["band"], mesh.shape["wave"]
    modes_here, waves_here = control[0] // bands, control[1] // waves
    lats_here, channels = courant[0] // bands, courant[1]
    return (
        waves == 4
        and bands % 2 == 0
        and waves_here % (bands // 2) == 0
        and waves_here % 8 == 0
        and modes_here % 16 == 0
        and lats_here % 8 == 0
        and LANES // 2 < channels <= LANES * 3 // 4
        and (channels - LANES // 2) % 8 == 0
        and courant[2] // waves % LANES == 0
        and GROUP_ROWS % (bands // 2) == 0
        and columns[1] == LANES
        and channels // bins == GROUP_ROWS
        and bands * waves % OBS_ROWS == 0
    )


SPECS = (
    P("band", "wave", None),
    P("band", "wave", None),
    P(),
    P("wave", None, None),
    P(),
    P("band", None, "wave"),
    P(),
    P(),
    P(("wave", "band"), None),
    P(("wave", "band"), None),
    P(("wave", "band"), None),
    P(("wave", "band"), None),
    P(("wave", "band"), None),
    P(("wave", "band"), None),
)


def solution(mesh):
    def program(*args):
        chosen = fast_body if fits(mesh, args[0].shape, args[5].shape, args[9].shape, args[6].shape[0]) else body
        return jax.shard_map(
            chosen,
            mesh=mesh,
            in_specs=SPECS,
            out_specs=(P("band", "wave", None), P("band", None, "wave")),
            check_vma=False,
        )(*args)

    return program
```

```python
import math

import jax
import jax.numpy as jnp
from jax import lax
from jax.experimental import pallas as pl
from jax.experimental.pallas import tpu as pltpu
from jax.sharding import PartitionSpec as P

MW = 224
LEV = 8
BINS = 12
STEPS = 4


highest = lax.Precision.HIGHEST
high = lax.Precision.HIGH


def trig_tables(numbers, lon_first, lon_count, lon_total, factor):
    longitudes = lon_first + jnp.arange(lon_count, dtype=jnp.int32)
    phases = numbers[:, None] * longitudes[None, :] % lon_total
    angles = phases.astype(jnp.float32) * (2.0 * math.pi / lon_total)
    return (jnp.cos(angles) * factor, jnp.sin(angles) * factor)


def settle_kernel(bins, tracer_ref, courant_ref, proj_ref, out_ref, model_ref):
    tracer = tracer_ref[0]
    courant = courant_ref[0]
    row = lax.broadcasted_iota(jnp.int32, tracer.shape, 0)
    for repeat in range(STEPS):
        outflow = courant * tracer
        inflow = jnp.where(row >= bins, pltpu.roll(outflow, bins, 0), 0.0)
        tracer = tracer - outflow + inflow
    out_ref[0] = tracer
    model_ref[0] = jnp.dot(proj_ref[...], tracer, precision=highest, preferred_element_type=jnp.float32)


def settle_adjoint_kernel(bins, resid_ref, courant_ref, proj_ref, out_ref):
    courant = courant_ref[0]
    adjoint = jnp.dot(proj_ref[...], resid_ref[0], precision=highest, preferred_element_type=jnp.float32)
    channels = adjoint.shape[0]
    row = lax.broadcasted_iota(jnp.int32, adjoint.shape, 0)
    for repeat in range(STEPS):
        below = jnp.where(row < channels - bins, pltpu.roll(adjoint, channels - bins, 0), 0.0)
        adjoint = adjoint + courant * (below - adjoint)
    out_ref[0] = adjoint


def per_lat(rows, cols):
    return pl.BlockSpec((1, rows, cols), lambda t: (t, 0, 0))


def whole(rows, cols):
    return pl.BlockSpec((rows, cols), lambda t: (0, 0))


def settle_forward(tracer, courant, proj, bins):
    lats, channels, lons = tracer.shape
    rows = proj.shape[0]
    return pl.pallas_call(
        lambda *refs: settle_kernel(bins, *refs),
        grid=(lats,),
        in_specs=[per_lat(channels, lons), per_lat(channels, lons), whole(rows, channels)],
        out_specs=[per_lat(channels, lons), per_lat(rows, lons)],
        out_shape=[
            jax.ShapeDtypeStruct((lats, channels, lons), jnp.float32),
            jax.ShapeDtypeStruct((lats, rows, lons), jnp.float32),
        ],
        name="settle_forward",
    )(tracer, courant, proj)


def settle_backward(resid, courant, proj_t, bins):
    lats, channels, lons = courant.shape
    rows = proj_t.shape[1]
    return pl.pallas_call(
        lambda *refs: settle_adjoint_kernel(bins, *refs),
        grid=(lats,),
        in_specs=[per_lat(rows, lons), per_lat(channels, lons), whole(channels, rows)],
        out_specs=per_lat(channels, lons),
        out_shape=jax.ShapeDtypeStruct((lats, channels, lons), jnp.float32),
        name="settle_backward",
    )(resid, courant, proj_t)


def synthesis_sum(cosine, sine_table, parts):
    return jnp.einsum("mo,mtc->tco", cosine, parts[..., 0], precision=high) - jnp.einsum(
        "mo,mtc->tco", sine_table, parts[..., 1], precision=high
    )


def analysis(cosine, sine_table, field):
    real_adj = jnp.einsum("mo,tco->mtc", cosine, field, precision=high)
    imag_adj = -jnp.einsum("mo,tco->mtc", sine_table, field, precision=high)
    stacked = jnp.stack([real_adj, imag_adj], axis=-1)
    return stacked.reshape(stacked.shape[0], stacked.shape[1], -1)


def body(
    control,
    spectral_scale,
    vertical_root,
    legendre,
    zonal_number,
    courant,
    lidar_coef,
    aod_coef,
    obs_count,
    obs_column,
    obs_level,
    lidar_obs,
    aod_obs,
    obs_weight,
):
    modes_here, waves_here, width = control.shape
    channels = width // 2
    wave_count = lax.axis_size("wave")
    band_count = lax.axis_size("band")
    lat_here = legendre.shape[1] // band_count
    lon_here = courant.shape[2]
    lon_total = lon_here * wave_count
    lon_first = lax.axis_index("wave") * lon_here
    factor = MW ** (-0.5)
    slot_count = obs_column.shape[1]
    live = jnp.arange(slot_count, dtype=jnp.int32)[None, :] < obs_count.reshape(-1, 1)
    packet = jnp.stack(
        [
            obs_column.astype(jnp.float32),
            obs_level.astype(jnp.float32),
            lidar_obs,
            aod_obs,
            jnp.where(live, obs_weight, 0.0),
        ],
        axis=1,
    )
    arrived = lax.all_to_all(packet, ("wave", "band"), split_axis=0, concat_axis=0, tiled=True)
    columns, levels, lidar_vals, aod_vals, weights = [arrived[:, i].reshape(-1) for i in range(5)]
    columns = columns.astype(jnp.int32)
    levels = levels.astype(jnp.int32)
    paired = control.reshape(modes_here, waves_here, channels, 2)
    mixed = jnp.einsum("nmcp,cd->nmdp", paired, vertical_root, precision=high).reshape(
        modes_here, waves_here, width
    )
    scaled = spectral_scale * mixed
    all_modes = lax.all_to_all(scaled, "band", split_axis=2, concat_axis=0, tiled=True)
    every_lat = jnp.einsum("mln,nmc->mlc", legendre, all_modes, precision=high)
    spectral = lax.all_to_all(every_lat, "band", split_axis=1, concat_axis=2, tiled=True)
    shard_piece = lax.all_gather(spectral, "wave", axis=0, tiled=True)
    numbers = zonal_number
    cosine, sine_table = trig_tables(numbers, lon_first, lon_here, lon_total, factor)
    parts = shard_piece.reshape(shard_piece.shape[0], lat_here, channels, 2)
    tracer = synthesis_sum(cosine, sine_table, parts)
    bins = lidar_coef.shape[0]
    levels_here = channels // bins
    proj_rows = -(-(levels_here + 1) // 8) * 8
    level_of = jnp.arange(channels, dtype=jnp.int32) // bins
    in_level = jnp.arange(levels_here, dtype=jnp.int32)[:, None] == level_of[None, :]
    proj = jnp.concatenate(
        [
            jnp.where(in_level, jnp.tile(lidar_coef, levels_here)[None, :], 0.0),
            aod_coef[None, :],
            jnp.zeros((proj_rows - levels_here - 1, channels), jnp.float32),
        ],
        axis=0,
    )
    tracer, model = settle_forward(tracer, courant, proj, bins)
    lat_index = columns // lon_here
    lon_hot = (columns % lon_here)[:, None] == jnp.arange(lon_here, dtype=jnp.int32)[None, :]
    lat_hot = (lat_index[:, None] == jnp.arange(lat_here, dtype=jnp.int32)[None, :]).astype(jnp.float32)
    cell = lat_index * levels_here + levels
    cell_hot = (
        cell[:, None] == jnp.arange(lat_here * levels_here, dtype=jnp.int32)[None, :]
    ).astype(jnp.float32)
    lidar_field = model[:, :levels_here].reshape(lat_here * levels_here, lon_here)
    aod_field = model[:, levels_here]
    lidar_rows = jnp.dot(cell_hot, lidar_field, precision=highest)
    aod_rows = jnp.dot(lat_hot, aod_field, precision=highest)
    lidar_model = jnp.sum(jnp.where(lon_hot, lidar_rows, 0.0), axis=1)
    aod_model = jnp.sum(jnp.where(lon_hot, aod_rows, 0.0), axis=1)
    lidar_resid = weights * (lidar_model - lidar_vals)
    aod_resid = weights * (aod_model - aod_vals)
    lidar_sum = lax.dot_general(
        cell_hot, jnp.where(lon_hot, lidar_resid[:, None], 0.0), (((0,), (0,)), ((), ())), precision=highest
    )
    aod_sum = lax.dot_general(
        lat_hot, jnp.where(lon_hot, aod_resid[:, None], 0.0), (((0,), (0,)), ((), ())), precision=highest
    )
    resid = jnp.concatenate(
        [
            lidar_sum.reshape(lat_here, levels_here, lon_here),
            aod_sum[:, None, :],
            jnp.zeros((lat_here, proj_rows - levels_here - 1, lon_here), jnp.float32),
        ],
        axis=1,
    )
    adjoint = settle_backward(resid, courant, proj.T, bins)
    numbers = zonal_number
    cosine, sine_table = trig_tables(numbers, lon_first, lon_here, lon_total, factor)
    spectral_adj = lax.psum_scatter(
        analysis(cosine, sine_table, adjoint), "wave", scatter_dimension=0, tiled=True
    )
    all_lats = lax.all_to_all(spectral_adj, "band", split_axis=2, concat_axis=1, tiled=True)
    mode_block = jnp.einsum("mtn,mtc->nmc", legendre, all_lats, precision=high)
    scaled_adj = lax.all_to_all(mode_block, "band", split_axis=0, concat_axis=2, tiled=True)
    mixed_adj = (spectral_scale * scaled_adj).reshape(modes_here, waves_here, channels, 2)
    control_adj = jnp.einsum("nmdp,cd->nmcp", mixed_adj, vertical_root, precision=high).reshape(
        modes_here, waves_here, width
    )
    return (control + control_adj, tracer)


LANES = 128
MESH_ID = pl.DeviceIdType.MESH
bf16 = jnp.bfloat16
f32 = jnp.float32
VMEM_LIMIT = 63 * 1024 * 1024


def split2(x):
    hi = x.astype(bf16)
    return hi, (x - hi.astype(f32)).astype(bf16)


def split3(x):
    hi, lo = split2(x)
    rest = x - hi.astype(f32)
    return hi, lo, (rest - lo.astype(f32)).astype(bf16)


def product(a, b, dims=((1,), (0,))):
    def one(x, y):
        return lax.dot_general(x, y, (dims, ((), ())), preferred_element_type=f32)

    return one(a[1], b[0]) + one(a[0], b[1]) + one(a[0], b[0])


def lane_of(shape):
    return lax.broadcasted_iota(jnp.int32, shape, len(shape) - 1)


def packed_order(channels, transposed):
    half = LANES // 2
    width = 2 * channels
    shape = (2 * LANES, width) if transposed else (width, 2 * LANES)
    source = lax.broadcasted_iota(jnp.int32, shape, 1 if transposed else 0)
    target = lax.broadcasted_iota(jnp.int32, shape, 0 if transposed else 1)
    channel = source // 2
    place = jnp.where(channel < half, channel, channel + half) + (source % 2) * half
    return jnp.where(place == target, 1.0, 0.0).astype(bf16)


def select_product(x, matrix):
    return sum(
        lax.dot_general(piece, matrix, (((1,), (0,)), ((), ())), preferred_element_type=f32)
        for piece in reversed(split3(x))
    )


def interleaved(root):
    channels = root.shape[0]
    wide = 2 * channels
    spread = (lax.broadcasted_iota(jnp.int32, (wide, channels), 0) // 2
              == lax.broadcasted_iota(jnp.int32, (wide, channels), 1))
    gather = (lax.broadcasted_iota(jnp.int32, (channels, wide), 1) // 2
              == lax.broadcasted_iota(jnp.int32, (channels, wide), 0))
    spread = jnp.where(spread, 1.0, 0.0).astype(bf16)
    gather = jnp.where(gather, 1.0, 0.0).astype(bf16)
    both = select_product(root, gather)
    both = sum(jnp.dot(spread, piece, preferred_element_type=f32) for piece in reversed(split3(both)))
    same = (lax.broadcasted_iota(jnp.int32, both.shape, 0) % 2) == (lax.broadcasted_iota(jnp.int32, both.shape, 1) % 2)
    return jnp.where(same, both, 0.0)


class Sizes:
    def __init__(self, modes, waves, width, lats, bands, wave_count):
        self.modes, self.waves, self.width, self.lats = modes, waves, width, lats
        self.bands, self.wave_count = bands, wave_count
        self.group = bands // 2
        self.own = waves // self.group
        self.half_lats = lats * self.group
        self.pairs = lats // 2
        self.rows = -(-(3 * self.pairs) // 8) * 8
        self.in_rows = modes + modes // 2
        self.slots = waves * wave_count
        self.unroll = max(u for u in range(1, UNROLL + 1) if self.pairs % u == 0)


class Place:
    def __init__(self, z):
        self.w, self.b = lax.axis_index("wave"), lax.axis_index("band")
        self.partner = self.w + 1 - 2 * (self.w % 2)
        self.across = (self.w + 2) % z.wave_count
        self.relay = (self.partner + 2) % z.wave_count
        self.half, self.spot = self.b // z.group, self.b % z.group
        self.z = z

    def peer(self, d):
        return (self.b + d) % self.z.bands

    def near_spot(self, e):
        return (self.spot + e) % self.z.group

    def near(self, e):
        return self.half * self.z.group + self.near_spot(e)

    def greet(self):
        barrier = pltpu.get_barrier_semaphore()
        others = [(self.w, self.peer(d)) for d in range(1, self.z.bands)]
        for wave, band in others + [(self.partner, self.b), (self.across, self.b)]:
            pl.semaphore_signal(barrier, inc=1, device_id={"wave": wave, "band": band}, device_id_type=MESH_ID)
        return barrier


def remote(src, dst, send, recv, wave, band):
    return pltpu.make_async_remote_copy(
        src, dst, send, recv, device_id={"wave": wave, "band": band}, device_id_type=MESH_ID)


AHEAD = 2
LAG_SPREAD = 2
LAG_ACROSS = 2
GROUP_ROWS = 8
UNROLL = 4


def first_kernel(z, control_ref, scale_ref, root_ref, leg_ref, count_ref, column_ref, level_ref, lidar_ref, aod_ref,
                 weight_ref, number_ref, out_ref, seen_ref, cos_ref, sin_ref, control, scale, s_a, s_b, send_u, recv_v, leg, y_a, y_b, send_y, packet,
                 leg_sem, in_sem, o_send, o_recv, a1_send, a1_recv, a2_send, a2_recv, x_send, x_recv, c_send, c_recv):
    at_me = Place(z)
    w, b = at_me.w, at_me.b
    half = LANES // 2
    quarter = LANES // 4
    phases = GROUP_ROWS // z.group
    groups = z.waves // GROUP_ROWS
    devices = z.wave_count * z.bands
    me = w * z.bands + b

    def input_copy(i, which):
        source, target = ((control_ref, control), (scale_ref, scale))[which]
        return pltpu.make_async_copy(
            source.at[:, pl.ds(i * GROUP_ROWS, GROUP_ROWS), :], target.at[i], in_sem.at[i, which])

    for i in range(groups):
        for which in range(2):
            input_copy(i, which).start()
    leg_copy = pltpu.make_async_copy(
        leg_ref.at[:, at_me.spot, pl.ds(at_me.half * z.half_lats, z.half_lats)], leg, leg_sem)
    leg_copy.start()
    barrier = pltpu.get_barrier_semaphore()

    def greet(e, carry):
        to = (me + e) % devices
        pl.semaphore_signal(barrier, inc=1, device_id={"wave": to // z.bands, "band": to % z.bands},
                            device_id_type=MESH_ID)
        return carry

    lax.fori_loop(1, devices, greet, 0)

    counts = jnp.broadcast_to(count_ref[...], (devices, devices))
    diagonal = lax.broadcasted_iota(jnp.int32, counts.shape, 0) == lax.broadcasted_iota(jnp.int32, counts.shape, 1)
    counts = jnp.sum(jnp.where(diagonal, counts, 0).astype(f32), axis=1, keepdims=True)
    weights = weight_ref[...]
    live = lax.broadcasted_iota(jnp.int32, weights.shape, 1).astype(f32) < counts
    fields = (column_ref[...].astype(f32), level_ref[...].astype(f32), lidar_ref[...], aod_ref[...],
              jnp.where(live, weights, 0.0))
    for k in range(GROUP_ROWS):
        value = fields[k] if k < len(fields) else jnp.zeros_like(weights)
        packet[pl.ds(k, devices, stride=GROUP_ROWS), :] = value

    def packet_copy(e):
        to = (me + e) % devices
        return remote(packet.at[pl.ds(to * GROUP_ROWS, GROUP_ROWS)], seen_ref.at[pl.ds(me * GROUP_ROWS, GROUP_ROWS)],
                      o_send.at[e], o_recv.at[e], to // z.bands, to % z.bands)

    packet_own = pltpu.make_async_copy(
        packet.at[pl.ds(me * GROUP_ROWS, GROUP_ROWS)], seen_ref.at[pl.ds(me * GROUP_ROWS, GROUP_ROWS)], o_send.at[0])

    root = split2(interleaved(root_ref[...]))
    order = packed_order(z.width // 2, False)

    def vertical(i):
        for which in range(2):
            input_copy(i, which).wait()
        x = control[i].reshape(z.modes * GROUP_ROWS, z.width)
        y = scale[i].reshape(z.modes * GROUP_ROWS, z.width)
        placed = select_product(y * product(split2(x), root), order)
        s_a[...] = placed[:, :LANES]
        s_b[...] = placed[:, LANES:]

    def first_copy(c, d):
        to = at_me.peer(d)
        return remote(send_u.at[c, to % z.group], recv_v.at[b, c], a1_send.at[c, d], a1_recv.at[c, d], w, to)

    def first_own(c):
        return pltpu.make_async_copy(send_u.at[c, at_me.spot], recv_v.at[b, c], a1_send.at[c, 0])

    def launch(c):
        @pl.when(c % phases == 0)
        def _():
            vertical(c // phases)

        low = z.modes // 2
        for spot in range(z.group):
            at = pl.ds(c % phases * z.group + spot, z.modes, stride=GROUP_ROWS)
            tall = s_b[at, :]
            send_u[c, spot, : z.modes] = s_a[at, :]
            send_u[c, spot, z.modes :] = tall[:low] + pltpu.roll(tall[low:], quarter, 1)
        for d in range(1, z.bands):
            first_copy(c, d).start()
        first_own(c).start()

    def second_copy(c, e):
        return remote(send_y.at[c, at_me.near_spot(e)], out_ref.at[w, c, at_me.spot], a2_send.at[c, e], a2_recv.at[c, e],
                      w, at_me.near(e))

    def second_own(c):
        return pltpu.make_async_copy(send_y.at[c, at_me.spot], out_ref.at[w, c, at_me.spot], a2_send.at[c, 0])

    def across_copy(c):
        return remote(out_ref.at[w, c], out_ref.at[w, c], x_send.at[c], x_recv.at[c], at_me.across, b)

    def core_copy(c, which):
        block = w if which == 0 else at_me.across
        return remote(out_ref.at[block, c], out_ref.at[block, c], c_send.at[c, which], c_recv.at[c, which],
                      at_me.partner, b)

    def transform(c):
        tops, tails = [], []
        for s in range(z.bands):
            tail = recv_v[s, c, z.modes :]
            keep = lane_of(tail.shape) % half < quarter
            tops.append(recv_v[s, c, : z.modes])
            tails.append(jnp.where(keep, tail, 0.0))
            tails.append(jnp.where(keep, pltpu.roll(tail, LANES - quarter, 1), 0.0))
        x = jnp.concatenate([jnp.concatenate(tops, 0), jnp.concatenate(tails, 0)], 1)
        y = product(split2(leg[c]), split2(x))
        y_a[...] = y[:, :LANES]
        y_b[...] = y[:, LANES:]
        for s in range(z.group):
            at = s * z.lats
            one = y_a[at : at + z.pairs]
            two = y_a[at + z.pairs : at + z.lats]
            left = lane_of(one.shape) < half
            send_y[c, s, z.rows - 8 :] = jnp.zeros((8, LANES), f32)
            send_y[c, s, : z.pairs] = jnp.where(left, one, pltpu.roll(two, half, 1))
            send_y[c, s, z.pairs : 2 * z.pairs] = jnp.where(left, pltpu.roll(one, half, 1), two)
            send_y[c, s, 2 * z.pairs : 3 * z.pairs] = y_b[at : at + z.pairs] + pltpu.roll(
                y_b[at + z.pairs : at + z.lats], quarter, 1)

    pl.semaphore_wait(barrier, devices - 1)
    for c in range(min(AHEAD, z.own)):
        launch(c)

    def send_packet(e, carry):
        packet_copy(e).start()
        return carry

    lax.fori_loop(1, devices, send_packet, 0)
    packet_own.start()
    lons = cos_ref.shape[1]
    lon_total = lons * z.wave_count
    longitude = lax.broadcasted_iota(jnp.int32, cos_ref.shape, 1) + w * lons
    angle = (number_ref[...] * longitude % lon_total).astype(f32) * (2.0 * math.pi / lon_total)
    factor = z.slots ** (-0.5)
    cos_ref[...] = jnp.cos(angle) * factor
    sin_ref[...] = jnp.sin(angle) * factor
    leg_copy.wait()

    def phase(p, carry):
        @pl.when(p + AHEAD < z.own)
        def _():
            launch(p + AHEAD)

        @pl.when(p < z.own)
        def _():
            first_own(p).wait()
            for d in range(1, z.bands):
                first_copy(p, d).wait_recv()
            transform(p)
            for e in range(1, z.group):
                second_copy(p, e).start()
            second_own(p).start()

        @pl.when((p >= LAG_SPREAD) & (p < z.own + LAG_SPREAD))
        def _():
            c = p - LAG_SPREAD
            for e in range(1, z.group):
                second_copy(c, e).wait_recv()
            second_own(c).wait()
            across_copy(c).start()
            core_copy(c, 0).start()

        @pl.when(p >= LAG_SPREAD + LAG_ACROSS)
        def _():
            c = p - LAG_SPREAD - LAG_ACROSS
            across_copy(c).wait_recv()
            core_copy(c, 1).start()

        return carry

    lax.fori_loop(0, z.own + LAG_SPREAD + LAG_ACROSS, phase, 0)

    def drain(c, carry):
        for d in range(1, z.bands):
            first_copy(c, d).wait_send()
        for e in range(1, z.group):
            second_copy(c, e).wait_send()
        across_copy(c).wait_send()
        for which in range(2):
            core_copy(c, which).wait()
        return carry

    lax.fori_loop(0, z.own, drain, 0)

    def drain_packet(e, carry):
        packet_copy(e).wait()
        return carry

    lax.fori_loop(1, devices, drain_packet, 0)
    packet_own.wait()


def transform_forward(z, control, scale, root, legendre, numbers, lons, observed):
    in_vmem = pl.BlockSpec(memory_space=pltpu.VMEM)
    anywhere = pl.BlockSpec(memory_space=pl.ANY)
    dma = pltpu.SemaphoreType.DMA
    devices = z.wave_count * z.bands
    groups = z.waves // GROUP_ROWS
    block = (groups, z.modes, GROUP_ROWS, z.width)
    return pl.pallas_call(
        lambda *refs: first_kernel(z, *refs),
        in_specs=[anywhere, anywhere, in_vmem, anywhere] + [in_vmem] * 7,
        out_specs=[anywhere, anywhere, in_vmem, in_vmem],
        out_shape=[
            jax.ShapeDtypeStruct((z.wave_count, z.own, z.group, z.rows, LANES), f32),
            jax.ShapeDtypeStruct((devices * GROUP_ROWS, LANES), f32),
            jax.ShapeDtypeStruct((z.slots, lons), f32),
            jax.ShapeDtypeStruct((z.slots, lons), f32),
        ],
        scratch_shapes=[
            pltpu.VMEM(block, f32),
            pltpu.VMEM(block, f32),
            pltpu.VMEM((z.modes * GROUP_ROWS, LANES), f32),
            pltpu.VMEM((z.modes * GROUP_ROWS, LANES), f32),
            pltpu.VMEM((z.own, z.group, z.in_rows, LANES), f32),
            pltpu.VMEM((z.bands, z.own, z.in_rows, LANES), f32),
            pltpu.VMEM((z.own, z.half_lats, z.modes * z.bands), f32),
            pltpu.VMEM((z.half_lats, LANES), f32),
            pltpu.VMEM((z.half_lats, LANES), f32),
            pltpu.VMEM((z.own, z.group, z.rows, LANES), f32),
            pltpu.VMEM((devices * GROUP_ROWS, LANES), f32),
            dma(()), dma((groups, 2)), dma((devices,)), dma((devices,)),
            dma((z.own, z.bands)), dma((z.own, z.bands)), dma((z.own, z.group)), dma((z.own, z.group)),
            dma((z.own,)), dma((z.own,)), dma((z.own, 2)), dma((z.own, 2)),
        ],
        compiler_params=pltpu.CompilerParams(collective_id=0, has_side_effects=True, vmem_limit_bytes=VMEM_LIMIT),
        name="transform_forward",
    )(control, scale, root, legendre.reshape(z.own, z.group, *legendre.shape[1:]), *observed,
      numbers.reshape(-1, 1))


def synthesis_kernel(z, bins, slabs_ref, cos_ref, sin_ref, courant_ref, lidar_ref, aod_ref, out_ref, model_ref,
                     c_hi, c_lo, n_hi, n_lo, p_hi, p_lo):
    half = LANES // 2

    @pl.when(pl.program_id(0) == 0)
    def _():
        c_hi[...], c_lo[...] = split2(cos_ref[...])
        n_hi[...], n_lo[...] = split2(-sin_ref[...])
        p_hi[...], p_lo[...] = split2(
            projection(lidar_ref[...], aod_ref[...], bins, aod_ref.shape[1] // bins, model_ref.shape[2]))

    def slab(row):
        return slabs_ref[pl.ds(row, z.slots, stride=z.rows), :]

    over_waves = ((0,), (0,))
    rest = z.width // 2 - half
    for u in range(z.unroll):
        i = pl.program_id(0) * z.unroll + u
        tail = slab(2 * z.pairs + i)
        real = jnp.concatenate([slab(i), tail], 1)
        imag = jnp.concatenate([slab(z.pairs + i), pltpu.roll(tail, half, 1)], 1)
        field = product(split2(real), (c_hi[...], c_lo[...]), over_waves) + product(
            split2(imag), (n_hi[...], n_lo[...]), over_waves)
        for which in range(2):
            tracer = jnp.concatenate(
                [field[which * half : (which + 1) * half],
                 field[LANES + which * (half // 2) : LANES + which * (half // 2) + rest]], 0)
            courant = courant_ref[which, u]
            row = lax.broadcasted_iota(jnp.int32, tracer.shape, 0)
            for repeat in range(STEPS):
                outflow = courant * tracer
                inflow = jnp.where(row >= bins, pltpu.roll(outflow, bins, 0), 0.0)
                tracer = tracer - outflow + inflow
            out_ref[which, u] = tracer
            model_ref[which, u] = product((p_hi[...], p_lo[...]), split2(tracer))


def paired(z, rows, cols):
    return pl.BlockSpec((2, z.unroll, rows, cols), lambda i: (0, i, 0, 0))


def synthesis_settle(z, slabs, cosine, sine, courant, lidar, aod):
    lats, channels, lons = courant.shape
    bins = lidar.shape[1]
    rows = -(-(channels // bins + 1) // 8) * 8
    tracer, model = pl.pallas_call(
        lambda *refs: synthesis_kernel(z, bins, *refs),
        grid=(z.pairs // z.unroll,),
        in_specs=[whole(z.slots * z.rows, LANES), whole(z.slots, lons), whole(z.slots, lons), paired(z, channels, lons),
                  whole(1, bins), whole(1, channels)],
        out_specs=[paired(z, channels, lons), paired(z, rows, lons)],
        out_shape=[
            jax.ShapeDtypeStruct((2, z.pairs, channels, lons), f32),
            jax.ShapeDtypeStruct((2, z.pairs, rows, lons), f32),
        ],
        scratch_shapes=[pltpu.VMEM((z.slots, lons), bf16)] * 4 + [pltpu.VMEM((rows, channels), bf16)] * 2,
        compiler_params=pltpu.CompilerParams(vmem_limit_bytes=VMEM_LIMIT),
        name="synthesis_settle",
    )(slabs.reshape(z.slots * z.rows, LANES), cosine, sine, courant.reshape(2, z.pairs, channels, lons), lidar, aod)
    return tracer.reshape(lats, channels, lons), model.reshape(lats, rows, lons)


OBS_ROWS = 4


def projection(lidar, aod, bins, levels, rows):
    channels = aod.shape[1]
    repeat = (lax.broadcasted_iota(jnp.int32, (bins, channels), 1) % bins
              == lax.broadcasted_iota(jnp.int32, (bins, channels), 0))
    repeat = jnp.where(repeat, 1.0, 0.0).astype(bf16)
    tiled = select_product(jnp.broadcast_to(lidar, (8, bins)), repeat)[:1]
    row = lax.broadcasted_iota(jnp.int32, (rows, channels), 0)
    level = lax.broadcasted_iota(jnp.int32, (rows, channels), 1) // bins
    return jnp.where((row < levels) & (level == row), tiled, jnp.where(row == levels, aod, 0.0))


def observe(z, levels, model_ref, seen_ref, resid, lidar_acc, aod_acc):
    lats, rows, lons = model_ref.shape
    cells = lats * levels
    devices = seen_ref.shape[0] // GROUP_ROWS
    slots = OBS_ROWS * seen_ref.shape[1]

    def halves(x):
        return jnp.concatenate(split2(x.T), 0)

    lidar_field = halves(model_ref[:, :levels, :].reshape(cells, lons))
    aod_field = halves(jnp.sum(model_ref[:, levels:, :], axis=1))
    lidar_acc[...] = jnp.zeros_like(lidar_acc)
    aod_acc[...] = jnp.zeros_like(aod_acc)
    over_slots = ((1,), (1,))

    def step(i, carry):
        def row(k):
            first = i * OBS_ROWS * GROUP_ROWS + k
            return jnp.concatenate([seen_ref[pl.ds(first + r * GROUP_ROWS, 1), :] for r in range(OBS_ROWS)], 1)

        column = row(0).astype(jnp.int32)
        lat = column // lons
        lon_hot = lax.broadcasted_iota(jnp.int32, (lons, slots), 0) == column - lat * lons
        cell = lat * levels + row(1).astype(jnp.int32)
        cell_hot = jnp.where(lax.broadcasted_iota(jnp.int32, (cells, slots), 0) == cell, 1.0, 0.0).astype(bf16)
        lat_hot = jnp.where(lax.broadcasted_iota(jnp.int32, (lats, slots), 0) == lat, 1.0, 0.0).astype(bf16)
        weight = row(4)

        def one(field, hot, observed, acc):
            picked = jnp.dot(field, hot, preferred_element_type=f32)
            picked = picked[:lons] + picked[lons:]
            left = weight * (jnp.sum(jnp.where(lon_hot, picked, 0.0), axis=0, keepdims=True) - observed)
            hi, lo = (jnp.where(lon_hot, part.astype(f32), 0.0).astype(bf16) for part in split2(left))
            acc[...] += lax.dot_general(hot, hi, (over_slots, ((), ())), preferred_element_type=f32) + lax.dot_general(
                hot, lo, (over_slots, ((), ())), preferred_element_type=f32)

        one(lidar_field, cell_hot, row(2), lidar_acc)
        one(aod_field, lat_hot, row(3), aod_acc)
        return carry

    lax.fori_loop(0, devices // OBS_ROWS, step, 0)
    resid[:, :levels, :] = lidar_acc[...].reshape(lats, levels, lons)
    spread = jnp.broadcast_to(aod_acc[...][:, None, :], (lats, rows - levels, lons))
    first = lax.broadcasted_iota(jnp.int32, spread.shape, 1) == 0
    resid[:, levels:, :] = jnp.where(first, spread, 0.0)


def second_kernel(z, bins, model_ref, seen_ref, lidar_ref, aod_ref, cos_ref, sin_ref, courant_ref, leg_ref, out_ref,
                  resid, lidar_acc, aod_acc, courant, q, c_hi, c_lo, n_hi, n_lo, p_hi, p_lo, r1, r2, v3, leg, z_all, send_u,
                  leg_sem, k_sem, c_send, c_recv, x_send, x_recv, a3_send, a3_recv, a4_send, a4_recv):
    at_me = Place(z)
    w, b = at_me.w, at_me.b
    half = LANES // 2
    quarter = LANES // 4
    channels = z.width // 2
    levels = channels // bins
    steps = z.pairs // z.unroll

    def courant_copy(k):
        at = pl.ds(k * z.unroll, z.unroll)
        return pltpu.make_async_copy(courant_ref.at[:, at], courant.at[:, at], k_sem.at[k])

    for k in range(steps):
        courant_copy(k).start()
    leg_copy = pltpu.make_async_copy(
        leg_ref.at[:, at_me.spot, pl.ds(at_me.half * z.half_lats, z.half_lats)], leg, leg_sem)
    leg_copy.start()
    barrier = at_me.greet()

    observe(z, levels, model_ref, seen_ref, resid, lidar_acc, aod_acc)

    c_hi[...], c_lo[...] = split2(cos_ref[...])
    n_hi[...], n_lo[...] = split2(-sin_ref[...])
    p_hi[...], p_lo[...] = split2(projection(lidar_ref[...], aod_ref[...], bins, levels, resid.shape[1]))
    for spare in range(3 * z.pairs, z.rows):
        q[pl.ds(spare, z.slots, stride=z.rows), :] = jnp.zeros((z.slots, LANES), f32)
    over_lons = ((1,), (1,))

    def analyse(k, carry):
        courant_copy(k).wait()
        for u in range(z.unroll):
            i = k * z.unroll + u
            fields = []
            for which in range(2):
                number = courant[which, i]
                adjoint = product((p_hi[...], p_lo[...]), split2(resid[which * z.pairs + i]), ((0,), (0,)))
                row = lax.broadcasted_iota(jnp.int32, adjoint.shape, 0)
                for repeat in range(STEPS):
                    below = jnp.where(row < channels - bins, pltpu.roll(adjoint, channels - bins, 0), 0.0)
                    adjoint = adjoint + number * (below - adjoint)
                fields.append(adjoint)
            gap = jnp.zeros((half // 2 - (channels - half), fields[0].shape[1]), f32)
            pieces = [field[:half] for field in fields]
            for field in fields:
                pieces.append(field[half:])
                if gap.shape[0]:
                    pieces.append(gap)
            pieces.append(jnp.zeros((half, fields[0].shape[1]), f32))
            both = split2(jnp.concatenate(pieces, 0))
            real = product((c_hi[...], c_lo[...]), both, over_lons)
            imag = product((n_hi[...], n_lo[...]), both, over_lons)
            q[pl.ds(i, z.slots, stride=z.rows), :] = real[:, :LANES]
            q[pl.ds(z.pairs + i, z.slots, stride=z.rows), :] = imag[:, :LANES]
            q[pl.ds(2 * z.pairs + i, z.slots, stride=z.rows), :] = real[:, LANES:] + pltpu.roll(imag[:, LANES:], half, 1)
        return carry

    lax.fori_loop(0, steps, analyse, 0)

    def block(wave, c):
        return pl.ds(pl.multiple_of((wave * z.own + c) * z.group * z.rows, 8), z.group * z.rows)

    def slab(c, spot):
        return pl.ds(pl.multiple_of(((w * z.own + c) * z.group + spot) * z.rows, 8), z.rows)

    def core_copy(c, which):
        wave = at_me.partner if which == 0 else at_me.relay
        return remote(q.at[block(wave, c)], r1.at[c, which], c_send.at[c, which], c_recv.at[c, which], at_me.partner, b)

    def across_copy(c):
        return remote(q.at[block(at_me.across, c)], r2.at[c], x_send.at[c], x_recv.at[c], at_me.across, b)

    def third_copy(c, e):
        return remote(q.at[slab(c, at_me.near_spot(e))], v3.at[at_me.spot, c], a3_send.at[c, e], a3_recv.at[c, e],
                      w, at_me.near(e))

    def third_own(c):
        return pltpu.make_async_copy(q.at[slab(c, at_me.spot)], v3.at[at_me.spot, c], a3_send.at[c, 0])

    def fourth_copy(c, d):
        return remote(send_u.at[c, at_me.peer(d)], out_ref.at[at_me.half, c, at_me.spot], a4_send.at[c, d],
                      a4_recv.at[c, d], w, at_me.peer(d))

    def fourth_own(c):
        return pltpu.make_async_copy(send_u.at[c, b], out_ref.at[at_me.half, c, at_me.spot], a4_send.at[c, 0])

    def transform(c):
        for s in range(z.group):
            at = s * z.lats
            real = v3[s, c, : z.pairs]
            imag = v3[s, c, z.pairs : 2 * z.pairs]
            tail = v3[s, c, 2 * z.pairs : 3 * z.pairs]
            lane = lane_of(real.shape)
            keep = lane % half < quarter
            z_all[at : at + z.pairs, :LANES] = jnp.where(lane < half, real, pltpu.roll(imag, half, 1))
            z_all[at + z.pairs : at + z.lats, :LANES] = jnp.where(lane < half, pltpu.roll(real, half, 1), imag)
            z_all[at : at + z.pairs, LANES:] = jnp.where(keep, tail, 0.0)
            z_all[at + z.pairs : at + z.lats, LANES:] = jnp.where(keep, pltpu.roll(tail, LANES - quarter, 1), 0.0)
        y = product(split2(leg[c]), split2(z_all[...]), ((0,), (0,)))
        low = z.modes // 2
        for s in range(z.bands):
            rows = y[s * z.modes : (s + 1) * z.modes]
            send_u[c, s, : z.modes] = rows[:, :LANES]
            send_u[c, s, z.modes :] = rows[:low, LANES:] + pltpu.roll(rows[low:, LANES:], quarter, 1)

    pl.semaphore_wait(barrier, z.bands + 1)

    def begin(c, carry):
        for which in (1, 0):
            core_copy(c, which).start()
        return carry

    lax.fori_loop(0, z.own, begin, 0)
    leg_copy.wait()

    def phase(p, carry):
        @pl.when(p < z.own)
        def _():
            core_copy(p, 1).wait_recv()
            at = block(at_me.across, p)
            q[at, :] = q[at, :] + r1[p, 1]
            across_copy(p).start()

        @pl.when((p >= LAG_ACROSS) & (p < z.own + LAG_ACROSS))
        def _():
            c = p - LAG_ACROSS
            core_copy(c, 0).wait_recv()
            across_copy(c).wait_recv()
            at = block(w, c)
            q[at, :] = q[at, :] + r1[c, 0] + r2[c]
            for e in range(1, z.group):
                third_copy(c, e).start()
            third_own(c).start()

        @pl.when(p >= LAG_ACROSS + LAG_SPREAD)
        def _():
            c = p - LAG_ACROSS - LAG_SPREAD
            third_own(c).wait()
            for e in range(1, z.group):
                third_copy(c, e).wait_recv()
            transform(c)
            for d in range(1, z.bands):
                fourth_copy(c, d).start()
            fourth_own(c).start()

        return carry

    lax.fori_loop(0, z.own + LAG_ACROSS + LAG_SPREAD, phase, 0)

    def drain(c, carry):
        across_copy(c).wait_send()
        for which in range(2):
            core_copy(c, which).wait_send()
        for e in range(1, z.group):
            third_copy(c, e).wait_send()
        for d in range(1, z.bands):
            fourth_copy(c, d).wait()
        fourth_own(c).wait()
        return carry

    lax.fori_loop(0, z.own, drain, 0)


def transform_backward(z, bins, model, seen, lidar, aod, cosine, sine, courant, legendre):
    anywhere = pl.BlockSpec(memory_space=pl.ANY)
    in_vmem = pl.BlockSpec(memory_space=pltpu.VMEM)
    dma = pltpu.SemaphoreType.DMA
    lats, channels, lons = courant.shape
    rows = model.shape[1]
    levels = channels // bins
    slab = (z.rows, LANES)
    chunk = (z.group * z.rows, LANES)
    table = pltpu.VMEM((z.slots, lons), bf16)
    return pl.pallas_call(
        lambda *refs: second_kernel(z, bins, *refs),
        in_specs=[in_vmem] * 6 + [anywhere, anywhere],
        out_specs=anywhere,
        out_shape=jax.ShapeDtypeStruct((2, z.own, z.group, z.in_rows, LANES), f32),
        scratch_shapes=[
            pltpu.VMEM(model.shape, f32),
            pltpu.VMEM((lats * levels, lons), f32),
            pltpu.VMEM((lats, lons), f32),
            pltpu.VMEM((2, z.pairs, channels, lons), f32),
            pltpu.VMEM((z.slots * z.rows, LANES), f32),
            table, table, table, table,
            pltpu.VMEM((rows, channels), bf16),
            pltpu.VMEM((rows, channels), bf16),
            pltpu.VMEM((z.own, 2) + chunk, f32),
            pltpu.VMEM((z.own,) + chunk, f32),
            pltpu.VMEM((z.group, z.own) + slab, f32),
            pltpu.VMEM((z.own, z.half_lats, z.modes * z.bands), f32),
            pltpu.VMEM((z.half_lats, 2 * LANES), f32),
            pltpu.VMEM((z.own, z.bands, z.in_rows, LANES), f32),
            dma(()), dma((z.pairs // z.unroll,)), dma((z.own, 2)), dma((z.own, 2)), dma((z.own,)), dma((z.own,)),
            dma((z.own, z.group)), dma((z.own, z.group)), dma((z.own, z.bands)), dma((z.own, z.bands)),
        ],
        compiler_params=pltpu.CompilerParams(collective_id=1, has_side_effects=True, vmem_limit_bytes=VMEM_LIMIT),
        name="transform_backward",
    )(model, seen, lidar, aod, cosine, sine, courant.reshape(2, z.pairs, channels, lons),
      legendre.reshape(z.own, z.group, *legendre.shape[1:]))


def last_kernel(z, slabs_ref, control_ref, scale_ref, root_ref, out_ref, s_a, s_b, r_hi, r_lo):
    half = LANES // 2
    quarter = LANES // 4

    @pl.when(pl.program_id(0) == 0)
    def _():
        r_hi[...], r_lo[...] = split2(interleaved(root_ref[...]))

    for m in range(GROUP_ROWS):
        slab = slabs_ref[0, m] + slabs_ref[1, m]
        tail = slab[z.modes :]
        keep = lane_of(tail.shape) % half < quarter
        both = jnp.concatenate(
            [jnp.where(keep, tail, 0.0), jnp.where(keep, pltpu.roll(tail, LANES - quarter, 1), 0.0)], 0)
        s_a[pl.ds(m, z.modes, stride=GROUP_ROWS), :] = slab[: z.modes]
        s_b[pl.ds(m, z.modes, stride=GROUP_ROWS), :] = both
    order = packed_order(z.width // 2, True)
    placed = jnp.concatenate([s_a[...], s_b[...]], 1)
    scale = scale_ref[...].reshape(z.modes * GROUP_ROWS, z.width)
    mixed = product(split2(scale * select_product(placed, order)), (r_hi[...], r_lo[...]), ((1,), (1,)))
    out_ref[...] = control_ref[...] + mixed.reshape(z.modes, GROUP_ROWS, z.width)


def finish(z, slabs, control, scale, root):
    by_waves = pl.BlockSpec((z.modes, GROUP_ROWS, z.width), lambda i: (0, i, 0))
    return pl.pallas_call(
        lambda *refs: last_kernel(z, *refs),
        grid=(z.waves // GROUP_ROWS,),
        in_specs=[
            pl.BlockSpec((2, GROUP_ROWS, z.in_rows, LANES), lambda i: (0, i, 0, 0)),
            by_waves, by_waves, whole(*root.shape),
        ],
        out_specs=by_waves,
        out_shape=jax.ShapeDtypeStruct(control.shape, f32),
        scratch_shapes=[pltpu.VMEM((z.modes * GROUP_ROWS, LANES), f32)] * 2 + [pltpu.VMEM((z.width, z.width), bf16)] * 2,
        compiler_params=pltpu.CompilerParams(vmem_limit_bytes=VMEM_LIMIT),
        name="finish",
    )(slabs.reshape(2, z.waves, z.in_rows, LANES), control, scale, root)


def fast_body(
    control,
    spectral_scale,
    vertical_root,
    legendre,
    zonal_number,
    courant,
    lidar_coef,
    aod_coef,
    obs_count,
    obs_column,
    obs_level,
    lidar_obs,
    aod_obs,
    obs_weight,
):
    modes_here, waves_here, width = control.shape
    wave_count = lax.axis_size("wave")
    lats_here, channels, lon_here = courant.shape
    z = Sizes(modes_here, waves_here, width, lats_here, lax.axis_size("band"), wave_count)
    bins = lidar_coef.shape[0]
    lidar, aod = lidar_coef.reshape(1, -1), aod_coef.reshape(1, -1)
    observed = (obs_count, obs_column, obs_level, lidar_obs, aod_obs, obs_weight)
    slabs, seen, cosine, sine = transform_forward(
        z, control, spectral_scale, vertical_root, legendre, zonal_number, lon_here, observed)
    tracer, model = synthesis_settle(z, slabs, cosine, sine, courant, lidar, aod)
    back = transform_backward(z, bins, model, seen, lidar, aod, cosine, sine, courant, legendre)
    return finish(z, back, control, spectral_scale, vertical_root), tracer


def fits(mesh, control, courant, columns, bins):
    bands, waves = mesh.shape["band"], mesh.shape["wave"]
    modes_here, waves_here = control[0] // bands, control[1] // waves
    lats_here, channels = courant[0] // bands, courant[1]
    return (
        waves == 4
        and bands % 2 == 0
        and waves_here % (bands // 2) == 0
        and waves_here % 8 == 0
        and modes_here % 16 == 0
        and lats_here % 8 == 0
        and LANES // 2 < channels <= LANES * 3 // 4
        and (channels - LANES // 2) % 8 == 0
        and courant[2] // waves % LANES == 0
        and GROUP_ROWS % (bands // 2) == 0
        and columns[1] == LANES
        and channels // bins == GROUP_ROWS
        and bands * waves % OBS_ROWS == 0
    )


SPECS = (
    P("band", "wave", None),
    P("band", "wave", None),
    P(),
    P("wave", None, None),
    P(),
    P("band", None, "wave"),
    P(),
    P(),
    P(("wave", "band"), None),
    P(("wave", "band"), None),
    P(("wave", "band"), None),
    P(("wave", "band"), None),
    P(("wave", "band"), None),
    P(("wave", "band"), None),
)


def solution(mesh):
    def program(*args):
        chosen = fast_body if fits(mesh, args[0].shape, args[5].shape, args[9].shape, args[6].shape[0]) else body
        return jax.shard_map(
            chosen,
            mesh=mesh,
            in_specs=SPECS,
            out_specs=(P("band", "wave", None), P("band", None, "wave")),
            check_vma=False,
        )(*args)

    return program
```

```python
import math

import jax
import jax.numpy as jnp
from jax import lax
from jax.experimental import pallas as pl
from jax.experimental.pallas import tpu as pltpu
from jax.sharding import PartitionSpec as P

MW = 224
LEV = 8
BINS = 12
STEPS = 4


highest = lax.Precision.HIGHEST
high = lax.Precision.HIGH


def trig_tables(numbers, lon_first, lon_count, lon_total, factor):
    longitudes = lon_first + jnp.arange(lon_count, dtype=jnp.int32)
    phases = numbers[:, None] * longitudes[None, :] % lon_total
    angles = phases.astype(jnp.float32) * (2.0 * math.pi / lon_total)
    return (jnp.cos(angles) * factor, jnp.sin(angles) * factor)


def settle_kernel(bins, tracer_ref, courant_ref, proj_ref, out_ref, model_ref):
    tracer = tracer_ref[0]
    courant = courant_ref[0]
    row = lax.broadcasted_iota(jnp.int32, tracer.shape, 0)
    for repeat in range(STEPS):
        outflow = courant * tracer
        inflow = jnp.where(row >= bins, pltpu.roll(outflow, bins, 0), 0.0)
        tracer = tracer - outflow + inflow
    out_ref[0] = tracer
    model_ref[0] = jnp.dot(proj_ref[...], tracer, precision=highest, preferred_element_type=jnp.float32)


def settle_adjoint_kernel(bins, resid_ref, courant_ref, proj_ref, out_ref):
    courant = courant_ref[0]
    adjoint = jnp.dot(proj_ref[...], resid_ref[0], precision=highest, preferred_element_type=jnp.float32)
    channels = adjoint.shape[0]
    row = lax.broadcasted_iota(jnp.int32, adjoint.shape, 0)
    for repeat in range(STEPS):
        below = jnp.where(row < channels - bins, pltpu.roll(adjoint, channels - bins, 0), 0.0)
        adjoint = adjoint + courant * (below - adjoint)
    out_ref[0] = adjoint


def per_lat(rows, cols):
    return pl.BlockSpec((1, rows, cols), lambda t: (t, 0, 0))


def whole(rows, cols):
    return pl.BlockSpec((rows, cols), lambda t: (0, 0))


def settle_forward(tracer, courant, proj, bins):
    lats, channels, lons = tracer.shape
    rows = proj.shape[0]
    return pl.pallas_call(
        lambda *refs: settle_kernel(bins, *refs),
        grid=(lats,),
        in_specs=[per_lat(channels, lons), per_lat(channels, lons), whole(rows, channels)],
        out_specs=[per_lat(channels, lons), per_lat(rows, lons)],
        out_shape=[
            jax.ShapeDtypeStruct((lats, channels, lons), jnp.float32),
            jax.ShapeDtypeStruct((lats, rows, lons), jnp.float32),
        ],
        name="settle_forward",
    )(tracer, courant, proj)


def settle_backward(resid, courant, proj_t, bins):
    lats, channels, lons = courant.shape
    rows = proj_t.shape[1]
    return pl.pallas_call(
        lambda *refs: settle_adjoint_kernel(bins, *refs),
        grid=(lats,),
        in_specs=[per_lat(rows, lons), per_lat(channels, lons), whole(channels, rows)],
        out_specs=per_lat(channels, lons),
        out_shape=jax.ShapeDtypeStruct((lats, channels, lons), jnp.float32),
        name="settle_backward",
    )(resid, courant, proj_t)


def synthesis_sum(cosine, sine_table, parts):
    return jnp.einsum("mo,mtc->tco", cosine, parts[..., 0], precision=high) - jnp.einsum(
        "mo,mtc->tco", sine_table, parts[..., 1], precision=high
    )


def analysis(cosine, sine_table, field):
    real_adj = jnp.einsum("mo,tco->mtc", cosine, field, precision=high)
    imag_adj = -jnp.einsum("mo,tco->mtc", sine_table, field, precision=high)
    stacked = jnp.stack([real_adj, imag_adj], axis=-1)
    return stacked.reshape(stacked.shape[0], stacked.shape[1], -1)


def body(
    control,
    spectral_scale,
    vertical_root,
    legendre,
    zonal_number,
    courant,
    lidar_coef,
    aod_coef,
    obs_count,
    obs_column,
    obs_level,
    lidar_obs,
    aod_obs,
    obs_weight,
):
    modes_here, waves_here, width = control.shape
    channels = width // 2
    wave_count = lax.axis_size("wave")
    band_count = lax.axis_size("band")
    lat_here = legendre.shape[1] // band_count
    lon_here = courant.shape[2]
    lon_total = lon_here * wave_count
    lon_first = lax.axis_index("wave") * lon_here
    factor = MW ** (-0.5)
    slot_count = obs_column.shape[1]
    live = jnp.arange(slot_count, dtype=jnp.int32)[None, :] < obs_count.reshape(-1, 1)
    packet = jnp.stack(
        [
            obs_column.astype(jnp.float32),
            obs_level.astype(jnp.float32),
            lidar_obs,
            aod_obs,
            jnp.where(live, obs_weight, 0.0),
        ],
        axis=1,
    )
    arrived = lax.all_to_all(packet, ("wave", "band"), split_axis=0, concat_axis=0, tiled=True)
    columns, levels, lidar_vals, aod_vals, weights = [arrived[:, i].reshape(-1) for i in range(5)]
    columns = columns.astype(jnp.int32)
    levels = levels.astype(jnp.int32)
    paired = control.reshape(modes_here, waves_here, channels, 2)
    mixed = jnp.einsum("nmcp,cd->nmdp", paired, vertical_root, precision=high).reshape(
        modes_here, waves_here, width
    )
    scaled = spectral_scale * mixed
    all_modes = lax.all_to_all(scaled, "band", split_axis=2, concat_axis=0, tiled=True)
    every_lat = jnp.einsum("mln,nmc->mlc", legendre, all_modes, precision=high)
    spectral = lax.all_to_all(every_lat, "band", split_axis=1, concat_axis=2, tiled=True)
    shard_piece = lax.all_gather(spectral, "wave", axis=0, tiled=True)
    numbers = zonal_number
    cosine, sine_table = trig_tables(numbers, lon_first, lon_here, lon_total, factor)
    parts = shard_piece.reshape(shard_piece.shape[0], lat_here, channels, 2)
    tracer = synthesis_sum(cosine, sine_table, parts)
    bins = lidar_coef.shape[0]
    levels_here = channels // bins
    proj_rows = -(-(levels_here + 1) // 8) * 8
    level_of = jnp.arange(channels, dtype=jnp.int32) // bins
    in_level = jnp.arange(levels_here, dtype=jnp.int32)[:, None] == level_of[None, :]
    proj = jnp.concatenate(
        [
            jnp.where(in_level, jnp.tile(lidar_coef, levels_here)[None, :], 0.0),
            aod_coef[None, :],
            jnp.zeros((proj_rows - levels_here - 1, channels), jnp.float32),
        ],
        axis=0,
    )
    tracer, model = settle_forward(tracer, courant, proj, bins)
    lat_index = columns // lon_here
    lon_hot = (columns % lon_here)[:, None] == jnp.arange(lon_here, dtype=jnp.int32)[None, :]
    lat_hot = (lat_index[:, None] == jnp.arange(lat_here, dtype=jnp.int32)[None, :]).astype(jnp.float32)
    cell = lat_index * levels_here + levels
    cell_hot = (
        cell[:, None] == jnp.arange(lat_here * levels_here, dtype=jnp.int32)[None, :]
    ).astype(jnp.float32)
    lidar_field = model[:, :levels_here].reshape(lat_here * levels_here, lon_here)
    aod_field = model[:, levels_here]
    lidar_rows = jnp.dot(cell_hot, lidar_field, precision=highest)
    aod_rows = jnp.dot(lat_hot, aod_field, precision=highest)
    lidar_model = jnp.sum(jnp.where(lon_hot, lidar_rows, 0.0), axis=1)
    aod_model = jnp.sum(jnp.where(lon_hot, aod_rows, 0.0), axis=1)
    lidar_resid = weights * (lidar_model - lidar_vals)
    aod_resid = weights * (aod_model - aod_vals)
    lidar_sum = lax.dot_general(
        cell_hot, jnp.where(lon_hot, lidar_resid[:, None], 0.0), (((0,), (0,)), ((), ())), precision=highest
    )
    aod_sum = lax.dot_general(
        lat_hot, jnp.where(lon_hot, aod_resid[:, None], 0.0), (((0,), (0,)), ((), ())), precision=highest
    )
    resid = jnp.concatenate(
        [
            lidar_sum.reshape(lat_here, levels_here, lon_here),
            aod_sum[:, None, :],
            jnp.zeros((lat_here, proj_rows - levels_here - 1, lon_here), jnp.float32),
        ],
        axis=1,
    )
    adjoint = settle_backward(resid, courant, proj.T, bins)
    numbers = zonal_number
    cosine, sine_table = trig_tables(numbers, lon_first, lon_here, lon_total, factor)
    spectral_adj = lax.psum_scatter(
        analysis(cosine, sine_table, adjoint), "wave", scatter_dimension=0, tiled=True
    )
    all_lats = lax.all_to_all(spectral_adj, "band", split_axis=2, concat_axis=1, tiled=True)
    mode_block = jnp.einsum("mtn,mtc->nmc", legendre, all_lats, precision=high)
    scaled_adj = lax.all_to_all(mode_block, "band", split_axis=0, concat_axis=2, tiled=True)
    mixed_adj = (spectral_scale * scaled_adj).reshape(modes_here, waves_here, channels, 2)
    control_adj = jnp.einsum("nmdp,cd->nmcp", mixed_adj, vertical_root, precision=high).reshape(
        modes_here, waves_here, width
    )
    return (control + control_adj, tracer)


LANES = 128
MESH_ID = pl.DeviceIdType.MESH
bf16 = jnp.bfloat16
f32 = jnp.float32
VMEM_LIMIT = 42 * 1024 * 1024
SMALL_LIMIT = 16 * 1024 * 1024


def split2(x):
    hi = x.astype(bf16)
    return hi, (x - hi.astype(f32)).astype(bf16)


def split3(x):
    hi, lo = split2(x)
    rest = x - hi.astype(f32)
    return hi, lo, (rest - lo.astype(f32)).astype(bf16)


def product(a, b, dims=((1,), (0,))):
    def one(x, y):
        return lax.dot_general(x, y, (dims, ((), ())), preferred_element_type=f32)

    return one(a[1], b[0]) + one(a[0], b[1]) + one(a[0], b[0])


def lane_of(shape):
    return lax.broadcasted_iota(jnp.int32, shape, len(shape) - 1)


def packed_order(channels, transposed):
    half = LANES // 2
    width = 2 * channels
    shape = (2 * LANES, width) if transposed else (width, 2 * LANES)
    source = lax.broadcasted_iota(jnp.int32, shape, 1 if transposed else 0)
    target = lax.broadcasted_iota(jnp.int32, shape, 0 if transposed else 1)
    channel = source // 2
    place = jnp.where(channel < half, channel, channel + half) + (source % 2) * half
    return jnp.where(place == target, 1.0, 0.0).astype(bf16)


def select_product(x, matrix):
    return sum(
        lax.dot_general(piece, matrix, (((1,), (0,)), ((), ())), preferred_element_type=f32)
        for piece in reversed(split3(x))
    )


def interleaved(root):
    channels = root.shape[0]
    wide = 2 * channels
    spread = (lax.broadcasted_iota(jnp.int32, (wide, channels), 0) // 2
              == lax.broadcasted_iota(jnp.int32, (wide, channels), 1))
    gather = (lax.broadcasted_iota(jnp.int32, (channels, wide), 1) // 2
              == lax.broadcasted_iota(jnp.int32, (channels, wide), 0))
    spread = jnp.where(spread, 1.0, 0.0).astype(bf16)
    gather = jnp.where(gather, 1.0, 0.0).astype(bf16)
    both = select_product(root, gather)
    both = sum(jnp.dot(spread, piece, preferred_element_type=f32) for piece in reversed(split3(both)))
    same = (lax.broadcasted_iota(jnp.int32, both.shape, 0) % 2) == (lax.broadcasted_iota(jnp.int32, both.shape, 1) % 2)
    return jnp.where(same, both, 0.0)


class Sizes:
    def __init__(self, modes, waves, width, lats, bands, wave_count):
        self.modes, self.waves, self.width, self.lats = modes, waves, width, lats
        self.bands, self.wave_count = bands, wave_count
        self.group = bands // 2
        self.own = waves // self.group
        self.half_lats = lats * self.group
        self.pairs = lats // 2
        self.rows = -(-(3 * self.pairs) // 8) * 8
        self.in_rows = modes + modes // 2
        self.slots = waves * wave_count
        self.unroll = max(u for u in range(1, UNROLL + 1) if self.pairs % u == 0)


class Place:
    def __init__(self, z):
        self.w, self.b = lax.axis_index("wave"), lax.axis_index("band")
        self.partner = self.w + 1 - 2 * (self.w % 2)
        self.across = (self.w + 2) % z.wave_count
        self.relay = (self.partner + 2) % z.wave_count
        self.half, self.spot = self.b // z.group, self.b % z.group
        self.z = z

    def peer(self, d):
        return (self.b + d) % self.z.bands

    def near_spot(self, e):
        return (self.spot + e) % self.z.group

    def near(self, e):
        return self.half * self.z.group + self.near_spot(e)

    def greet(self):
        barrier = pltpu.get_barrier_semaphore()
        others = [(self.w, self.peer(d)) for d in range(1, self.z.bands)]
        for wave, band in others + [(self.partner, self.b), (self.across, self.b)]:
            pl.semaphore_signal(barrier, inc=1, device_id={"wave": wave, "band": band}, device_id_type=MESH_ID)
        return barrier


def remote(src, dst, send, recv, wave, band):
    return pltpu.make_async_remote_copy(
        src, dst, send, recv, device_id={"wave": wave, "band": band}, device_id_type=MESH_ID)


AHEAD = 2
LAG_SPREAD = 2
LAG_ACROSS = 2
GROUP_ROWS = 8
UNROLL = 4


def first_kernel(z, control_ref, scale_ref, root_ref, leg_ref, count_ref, column_ref, level_ref, lidar_ref, aod_ref,
                 weight_ref, number_ref, out_ref, seen_ref, cos_ref, sin_ref, control, scale, s_a, s_b, send_u, recv_v, leg, y_a, y_b, send_y, packet,
                 leg_sem, in_sem, o_send, o_recv, a1_send, a1_recv, a2_send, a2_recv, x_send, x_recv, c_send, c_recv):
    at_me = Place(z)
    w, b = at_me.w, at_me.b
    half = LANES // 2
    quarter = LANES // 4
    phases = GROUP_ROWS // z.group
    groups = z.waves // GROUP_ROWS
    devices = z.wave_count * z.bands
    me = w * z.bands + b

    def input_copy(i, which):
        source, target = ((control_ref, control), (scale_ref, scale))[which]
        return pltpu.make_async_copy(
            source.at[:, pl.ds(i * GROUP_ROWS, GROUP_ROWS), :], target.at[i], in_sem.at[i, which])

    for i in range(groups):
        for which in range(2):
            input_copy(i, which).start()
    leg_copy = pltpu.make_async_copy(
        leg_ref.at[:, at_me.spot, pl.ds(at_me.half * z.half_lats, z.half_lats)], leg, leg_sem)
    leg_copy.start()
    barrier = pltpu.get_barrier_semaphore()

    def greet(e, carry):
        to = (me + e) % devices
        pl.semaphore_signal(barrier, inc=1, device_id={"wave": to // z.bands, "band": to % z.bands},
                            device_id_type=MESH_ID)
        return carry

    lax.fori_loop(1, devices, greet, 0)

    counts = jnp.broadcast_to(count_ref[...], (devices, devices))
    diagonal = lax.broadcasted_iota(jnp.int32, counts.shape, 0) == lax.broadcasted_iota(jnp.int32, counts.shape, 1)
    counts = jnp.sum(jnp.where(diagonal, counts, 0).astype(f32), axis=1, keepdims=True)
    weights = weight_ref[...]
    live = lax.broadcasted_iota(jnp.int32, weights.shape, 1).astype(f32) < counts
    fields = (column_ref[...].astype(f32), level_ref[...].astype(f32), lidar_ref[...], aod_ref[...],
              jnp.where(live, weights, 0.0))
    for k in range(GROUP_ROWS):
        value = fields[k] if k < len(fields) else jnp.zeros_like(weights)
        packet[pl.ds(k, devices, stride=GROUP_ROWS), :] = value

    def packet_copy(e):
        to = (me + e) % devices
        return remote(packet.at[pl.ds(to * GROUP_ROWS, GROUP_ROWS)], seen_ref.at[pl.ds(me * GROUP_ROWS, GROUP_ROWS)],
                      o_send.at[e], o_recv.at[e], to // z.bands, to % z.bands)

    packet_own = pltpu.make_async_copy(
        packet.at[pl.ds(me * GROUP_ROWS, GROUP_ROWS)], seen_ref.at[pl.ds(me * GROUP_ROWS, GROUP_ROWS)], o_send.at[0])

    root = split2(interleaved(root_ref[...]))
    order = packed_order(z.width // 2, False)

    def vertical(i):
        for which in range(2):
            input_copy(i, which).wait()
        x = control[i].reshape(z.modes * GROUP_ROWS, z.width)
        y = scale[i].reshape(z.modes * GROUP_ROWS, z.width)
        placed = select_product(y * product(split2(x), root), order)
        s_a[...] = placed[:, :LANES]
        s_b[...] = placed[:, LANES:]

    def first_copy(c, d):
        to = at_me.peer(d)
        return remote(send_u.at[c, to % z.group], recv_v.at[b, c], a1_send.at[c, d], a1_recv.at[c, d], w, to)

    def first_own(c):
        return pltpu.make_async_copy(send_u.at[c, at_me.spot], recv_v.at[b, c], a1_send.at[c, 0])

    def launch(c):
        @pl.when(c % phases == 0)
        def _():
            vertical(c // phases)

        low = z.modes // 2
        for spot in range(z.group):
            at = pl.ds(c % phases * z.group + spot, z.modes, stride=GROUP_ROWS)
            tall = s_b[at, :]
            send_u[c, spot, : z.modes] = s_a[at, :]
            send_u[c, spot, z.modes :] = tall[:low] + pltpu.roll(tall[low:], quarter, 1)
        for d in range(1, z.bands):
            first_copy(c, d).start()
        first_own(c).start()

    def second_copy(c, e):
        return remote(send_y.at[c, at_me.near_spot(e)], out_ref.at[w, c, at_me.spot], a2_send.at[c, e], a2_recv.at[c, e],
                      w, at_me.near(e))

    def second_own(c):
        return pltpu.make_async_copy(send_y.at[c, at_me.spot], out_ref.at[w, c, at_me.spot], a2_send.at[c, 0])

    def across_copy(c):
        return remote(out_ref.at[w, c], out_ref.at[w, c], x_send.at[c], x_recv.at[c], at_me.across, b)

    def core_copy(c, which):
        block = w if which == 0 else at_me.across
        return remote(out_ref.at[block, c], out_ref.at[block, c], c_send.at[c, which], c_recv.at[c, which],
                      at_me.partner, b)

    def transform(c):
        tops, tails = [], []
        for s in range(z.bands):
            tail = recv_v[s, c, z.modes :]
            keep = lane_of(tail.shape) % half < quarter
            tops.append(recv_v[s, c, : z.modes])
            tails.append(jnp.where(keep, tail, 0.0))
            tails.append(jnp.where(keep, pltpu.roll(tail, LANES - quarter, 1), 0.0))
        x = jnp.concatenate([jnp.concatenate(tops, 0), jnp.concatenate(tails, 0)], 1)
        y = product(split2(leg[c]), split2(x))
        y_a[...] = y[:, :LANES]
        y_b[...] = y[:, LANES:]
        for s in range(z.group):
            at = s * z.lats
            one = y_a[at : at + z.pairs]
            two = y_a[at + z.pairs : at + z.lats]
            left = lane_of(one.shape) < half
            send_y[c, s, z.rows - 8 :] = jnp.zeros((8, LANES), f32)
            send_y[c, s, : z.pairs] = jnp.where(left, one, pltpu.roll(two, half, 1))
            send_y[c, s, z.pairs : 2 * z.pairs] = jnp.where(left, pltpu.roll(one, half, 1), two)
            send_y[c, s, 2 * z.pairs : 3 * z.pairs] = y_b[at : at + z.pairs] + pltpu.roll(
                y_b[at + z.pairs : at + z.lats], quarter, 1)

    pl.semaphore_wait(barrier, devices - 1)
    for c in range(min(AHEAD, z.own)):
        launch(c)

    def send_packet(e, carry):
        packet_copy(e).start()
        return carry

    lax.fori_loop(1, devices, send_packet, 0)
    packet_own.start()
    lons = cos_ref.shape[1]
    lon_total = lons * z.wave_count
    longitude = lax.broadcasted_iota(jnp.int32, cos_ref.shape, 1) + w * lons
    angle = (number_ref[...] * longitude % lon_total).astype(f32) * (2.0 * math.pi / lon_total)
    factor = z.slots ** (-0.5)
    cos_ref[...] = jnp.cos(angle) * factor
    sin_ref[...] = jnp.sin(angle) * factor
    leg_copy.wait()

    def phase(p, carry):
        @pl.when(p + AHEAD < z.own)
        def _():
            launch(p + AHEAD)

        @pl.when(p < z.own)
        def _():
            first_own(p).wait()
            for d in range(1, z.bands):
                first_copy(p, d).wait_recv()
            transform(p)
            for e in range(1, z.group):
                second_copy(p, e).start()
            second_own(p).start()

        @pl.when((p >= LAG_SPREAD) & (p < z.own + LAG_SPREAD))
        def _():
            c = p - LAG_SPREAD
            for e in range(1, z.group):
                second_copy(c, e).wait_recv()
            second_own(c).wait()
            across_copy(c).start()
            core_copy(c, 0).start()

        @pl.when(p >= LAG_SPREAD + LAG_ACROSS)
        def _():
            c = p - LAG_SPREAD - LAG_ACROSS
            across_copy(c).wait_recv()
            core_copy(c, 1).start()

        return carry

    lax.fori_loop(0, z.own + LAG_SPREAD + LAG_ACROSS, phase, 0)

    def drain(c, carry):
        for d in range(1, z.bands):
            first_copy(c, d).wait_send()
        for e in range(1, z.group):
            second_copy(c, e).wait_send()
        across_copy(c).wait_send()
        for which in range(2):
            core_copy(c, which).wait()
        return carry

    lax.fori_loop(0, z.own, drain, 0)

    def drain_packet(e, carry):
        packet_copy(e).wait()
        return carry

    lax.fori_loop(1, devices, drain_packet, 0)
    packet_own.wait()


def transform_forward(z, control, scale, root, legendre, numbers, lons, observed):
    in_vmem = pl.BlockSpec(memory_space=pltpu.VMEM)
    anywhere = pl.BlockSpec(memory_space=pl.ANY)
    dma = pltpu.SemaphoreType.DMA
    devices = z.wave_count * z.bands
    groups = z.waves // GROUP_ROWS
    block = (groups, z.modes, GROUP_ROWS, z.width)
    return pl.pallas_call(
        lambda *refs: first_kernel(z, *refs),
        in_specs=[anywhere, anywhere, in_vmem, anywhere] + [in_vmem] * 7,
        out_specs=[in_vmem, anywhere, in_vmem, in_vmem],
        out_shape=[
            pltpu.VMEM((z.wave_count, z.own, z.group, z.rows, LANES), f32),
            jax.ShapeDtypeStruct((devices * GROUP_ROWS, LANES), f32),
            jax.ShapeDtypeStruct((z.slots, lons), f32),
            jax.ShapeDtypeStruct((z.slots, lons), f32),
        ],
        scratch_shapes=[
            pltpu.VMEM(block, f32),
            pltpu.VMEM(block, f32),
            pltpu.VMEM((z.modes * GROUP_ROWS, LANES), f32),
            pltpu.VMEM((z.modes * GROUP_ROWS, LANES), f32),
            pltpu.VMEM((z.own, z.group, z.in_rows, LANES), f32),
            pltpu.VMEM((z.bands, z.own, z.in_rows, LANES), f32),
            pltpu.VMEM((z.own, z.half_lats, z.modes * z.bands), f32),
            pltpu.VMEM((z.half_lats, LANES), f32),
            pltpu.VMEM((z.half_lats, LANES), f32),
            pltpu.VMEM((z.own, z.group, z.rows, LANES), f32),
            pltpu.VMEM((devices * GROUP_ROWS, LANES), f32),
            dma(()), dma((groups, 2)), dma((devices,)), dma((devices,)),
            dma((z.own, z.bands)), dma((z.own, z.bands)), dma((z.own, z.group)), dma((z.own, z.group)),
            dma((z.own,)), dma((z.own,)), dma((z.own, 2)), dma((z.own, 2)),
        ],
        compiler_params=pltpu.CompilerParams(collective_id=0, has_side_effects=True, vmem_limit_bytes=VMEM_LIMIT),
        name="transform_forward",
    )(control, scale, root, legendre.reshape(z.own, z.group, *legendre.shape[1:]), *observed,
      numbers.reshape(-1, 1))


def synthesis_kernel(z, bins, slabs_ref, cos_ref, sin_ref, courant_ref, lidar_ref, aod_ref, out_ref, model_ref,
                     c_hi, c_lo, n_hi, n_lo, p_hi, p_lo):
    half = LANES // 2

    @pl.when(pl.program_id(0) == 0)
    def _():
        c_hi[...], c_lo[...] = split2(cos_ref[...])
        n_hi[...], n_lo[...] = split2(-sin_ref[...])
        p_hi[...], p_lo[...] = split2(
            projection(lidar_ref[...], aod_ref[...], bins, aod_ref.shape[1] // bins, model_ref.shape[2]))

    def slab(row):
        return slabs_ref[pl.ds(row, z.slots, stride=z.rows), :]

    over_waves = ((0,), (0,))
    rest = z.width // 2 - half
    for u in range(z.unroll):
        i = pl.program_id(0) * z.unroll + u
        tail = slab(2 * z.pairs + i)
        real = jnp.concatenate([slab(i), tail], 1)
        imag = jnp.concatenate([slab(z.pairs + i), pltpu.roll(tail, half, 1)], 1)
        field = product(split2(real), (c_hi[...], c_lo[...]), over_waves) + product(
            split2(imag), (n_hi[...], n_lo[...]), over_waves)
        for which in range(2):
            tracer = jnp.concatenate(
                [field[which * half : (which + 1) * half],
                 field[LANES + which * (half // 2) : LANES + which * (half // 2) + rest]], 0)
            courant = courant_ref[which, u]
            row = lax.broadcasted_iota(jnp.int32, tracer.shape, 0)
            for repeat in range(STEPS):
                outflow = courant * tracer
                inflow = jnp.where(row >= bins, pltpu.roll(outflow, bins, 0), 0.0)
                tracer = tracer - outflow + inflow
            out_ref[which, u] = tracer
            model_ref[which, u] = product((p_hi[...], p_lo[...]), split2(tracer))


def paired(z, rows, cols):
    return pl.BlockSpec((2, z.unroll, rows, cols), lambda i: (0, i, 0, 0))


def synthesis_settle(z, slabs, cosine, sine, courant, lidar, aod):
    lats, channels, lons = courant.shape
    bins = lidar.shape[1]
    rows = -(-(channels // bins + 1) // 8) * 8
    tracer, model = pl.pallas_call(
        lambda *refs: synthesis_kernel(z, bins, *refs),
        grid=(z.pairs // z.unroll,),
        in_specs=[pl.BlockSpec(memory_space=pltpu.VMEM), whole(z.slots, lons), whole(z.slots, lons), paired(z, channels, lons),
                  whole(1, bins), whole(1, channels)],
        out_specs=[paired(z, channels, lons), paired(z, rows, lons)],
        out_shape=[
            jax.ShapeDtypeStruct((2, z.pairs, channels, lons), f32),
            jax.ShapeDtypeStruct((2, z.pairs, rows, lons), f32),
        ],
        scratch_shapes=[pltpu.VMEM((z.slots, lons), bf16)] * 4 + [pltpu.VMEM((rows, channels), bf16)] * 2,
        compiler_params=pltpu.CompilerParams(vmem_limit_bytes=SMALL_LIMIT),
        name="synthesis_settle",
    )(slabs.reshape(z.slots * z.rows, LANES), cosine, sine, courant.reshape(2, z.pairs, channels, lons), lidar, aod)
    return tracer.reshape(lats, channels, lons), model.reshape(lats, rows, lons)


OBS_ROWS = 4


def projection(lidar, aod, bins, levels, rows):
    channels = aod.shape[1]
    repeat = (lax.broadcasted_iota(jnp.int32, (bins, channels), 1) % bins
              == lax.broadcasted_iota(jnp.int32, (bins, channels), 0))
    repeat = jnp.where(repeat, 1.0, 0.0).astype(bf16)
    tiled = select_product(jnp.broadcast_to(lidar, (8, bins)), repeat)[:1]
    row = lax.broadcasted_iota(jnp.int32, (rows, channels), 0)
    level = lax.broadcasted_iota(jnp.int32, (rows, channels), 1) // bins
    return jnp.where((row < levels) & (level == row), tiled, jnp.where(row == levels, aod, 0.0))


def observe(z, levels, model_ref, seen_ref, resid, lidar_acc, aod_acc):
    lats, rows, lons = model_ref.shape
    cells = lats * levels
    devices = seen_ref.shape[0] // GROUP_ROWS
    slots = OBS_ROWS * seen_ref.shape[1]

    def halves(x):
        return jnp.concatenate(split2(x.T), 0)

    lidar_field = halves(model_ref[:, :levels, :].reshape(cells, lons))
    aod_field = halves(jnp.sum(model_ref[:, levels:, :], axis=1))
    lidar_acc[...] = jnp.zeros_like(lidar_acc)
    aod_acc[...] = jnp.zeros_like(aod_acc)
    over_slots = ((1,), (1,))

    def step(i, carry):
        def row(k):
            first = i * OBS_ROWS * GROUP_ROWS + k
            return jnp.concatenate([seen_ref[pl.ds(first + r * GROUP_ROWS, 1), :] for r in range(OBS_ROWS)], 1)

        column = row(0).astype(jnp.int32)
        lat = column // lons
        lon_hot = lax.broadcasted_iota(jnp.int32, (lons, slots), 0) == column - lat * lons
        cell = lat * levels + row(1).astype(jnp.int32)
        cell_hot = jnp.where(lax.broadcasted_iota(jnp.int32, (cells, slots), 0) == cell, 1.0, 0.0).astype(bf16)
        lat_hot = jnp.where(lax.broadcasted_iota(jnp.int32, (lats, slots), 0) == lat, 1.0, 0.0).astype(bf16)
        weight = row(4)

        def one(field, hot, observed, acc):
            picked = jnp.dot(field, hot, preferred_element_type=f32)
            picked = picked[:lons] + picked[lons:]
            left = weight * (jnp.sum(jnp.where(lon_hot, picked, 0.0), axis=0, keepdims=True) - observed)
            hi, lo = (jnp.where(lon_hot, part.astype(f32), 0.0).astype(bf16) for part in split2(left))
            acc[...] += lax.dot_general(hot, hi, (over_slots, ((), ())), preferred_element_type=f32) + lax.dot_general(
                hot, lo, (over_slots, ((), ())), preferred_element_type=f32)

        one(lidar_field, cell_hot, row(2), lidar_acc)
        one(aod_field, lat_hot, row(3), aod_acc)
        return carry

    lax.fori_loop(0, devices // OBS_ROWS, step, 0)
    resid[:, :levels, :] = lidar_acc[...].reshape(lats, levels, lons)
    spread = jnp.broadcast_to(aod_acc[...][:, None, :], (lats, rows - levels, lons))
    first = lax.broadcasted_iota(jnp.int32, spread.shape, 1) == 0
    resid[:, levels:, :] = jnp.where(first, spread, 0.0)


def second_kernel(z, bins, model_ref, seen_ref, lidar_ref, aod_ref, cos_ref, sin_ref, courant_ref, leg_ref, out_ref,
                  resid, lidar_acc, aod_acc, courant, q, c_hi, c_lo, n_hi, n_lo, p_hi, p_lo, r1, r2, v3, leg, z_all, send_u,
                  leg_sem, k_sem, c_send, c_recv, x_send, x_recv, a3_send, a3_recv, a4_send, a4_recv):
    at_me = Place(z)
    w, b = at_me.w, at_me.b
    half = LANES // 2
    quarter = LANES // 4
    channels = z.width // 2
    levels = channels // bins
    steps = z.pairs // z.unroll

    def courant_copy(k):
        at = pl.ds(k * z.unroll, z.unroll)
        return pltpu.make_async_copy(courant_ref.at[:, at], courant.at[:, at], k_sem.at[k])

    for k in range(steps):
        courant_copy(k).start()
    leg_copy = pltpu.make_async_copy(
        leg_ref.at[:, at_me.spot, pl.ds(at_me.half * z.half_lats, z.half_lats)], leg, leg_sem)
    leg_copy.start()
    barrier = at_me.greet()

    observe(z, levels, model_ref, seen_ref, resid, lidar_acc, aod_acc)

    c_hi[...], c_lo[...] = split2(cos_ref[...])
    n_hi[...], n_lo[...] = split2(-sin_ref[...])
    p_hi[...], p_lo[...] = split2(projection(lidar_ref[...], aod_ref[...], bins, levels, resid.shape[1]))
    for spare in range(3 * z.pairs, z.rows):
        q[pl.ds(spare, z.slots, stride=z.rows), :] = jnp.zeros((z.slots, LANES), f32)
    over_lons = ((1,), (1,))

    def analyse(k, carry):
        courant_copy(k).wait()
        for u in range(z.unroll):
            i = k * z.unroll + u
            fields = []
            for which in range(2):
                number = courant[which, i]
                adjoint = product((p_hi[...], p_lo[...]), split2(resid[which * z.pairs + i]), ((0,), (0,)))
                row = lax.broadcasted_iota(jnp.int32, adjoint.shape, 0)
                for repeat in range(STEPS):
                    below = jnp.where(row < channels - bins, pltpu.roll(adjoint, channels - bins, 0), 0.0)
                    adjoint = adjoint + number * (below - adjoint)
                fields.append(adjoint)
            gap = jnp.zeros((half // 2 - (channels - half), fields[0].shape[1]), f32)
            pieces = [field[:half] for field in fields]
            for field in fields:
                pieces.append(field[half:])
                if gap.shape[0]:
                    pieces.append(gap)
            pieces.append(jnp.zeros((half, fields[0].shape[1]), f32))
            both = split2(jnp.concatenate(pieces, 0))
            real = product((c_hi[...], c_lo[...]), both, over_lons)
            imag = product((n_hi[...], n_lo[...]), both, over_lons)
            q[pl.ds(i, z.slots, stride=z.rows), :] = real[:, :LANES]
            q[pl.ds(z.pairs + i, z.slots, stride=z.rows), :] = imag[:, :LANES]
            q[pl.ds(2 * z.pairs + i, z.slots, stride=z.rows), :] = real[:, LANES:] + pltpu.roll(imag[:, LANES:], half, 1)
        return carry

    lax.fori_loop(0, steps, analyse, 0)

    def block(wave, c):
        return pl.ds(pl.multiple_of((wave * z.own + c) * z.group * z.rows, 8), z.group * z.rows)

    def slab(c, spot):
        return pl.ds(pl.multiple_of(((w * z.own + c) * z.group + spot) * z.rows, 8), z.rows)

    def core_copy(c, which):
        wave = at_me.partner if which == 0 else at_me.relay
        return remote(q.at[block(wave, c)], r1.at[c, which], c_send.at[c, which], c_recv.at[c, which], at_me.partner, b)

    def across_copy(c):
        return remote(q.at[block(at_me.across, c)], r2.at[c], x_send.at[c], x_recv.at[c], at_me.across, b)

    def third_copy(c, e):
        return remote(q.at[slab(c, at_me.near_spot(e))], v3.at[at_me.spot, c], a3_send.at[c, e], a3_recv.at[c, e],
                      w, at_me.near(e))

    def third_own(c):
        return pltpu.make_async_copy(q.at[slab(c, at_me.spot)], v3.at[at_me.spot, c], a3_send.at[c, 0])

    def fourth_copy(c, d):
        return remote(send_u.at[c, at_me.peer(d)], out_ref.at[at_me.half, c, at_me.spot], a4_send.at[c, d],
                      a4_recv.at[c, d], w, at_me.peer(d))

    def fourth_own(c):
        return pltpu.make_async_copy(send_u.at[c, b], out_ref.at[at_me.half, c, at_me.spot], a4_send.at[c, 0])

    def transform(c):
        for s in range(z.group):
            at = s * z.lats
            real = v3[s, c, : z.pairs]
            imag = v3[s, c, z.pairs : 2 * z.pairs]
            tail = v3[s, c, 2 * z.pairs : 3 * z.pairs]
            lane = lane_of(real.shape)
            keep = lane % half < quarter
            z_all[at : at + z.pairs, :LANES] = jnp.where(lane < half, real, pltpu.roll(imag, half, 1))
            z_all[at + z.pairs : at + z.lats, :LANES] = jnp.where(lane < half, pltpu.roll(real, half, 1), imag)
            z_all[at : at + z.pairs, LANES:] = jnp.where(keep, tail, 0.0)
            z_all[at + z.pairs : at + z.lats, LANES:] = jnp.where(keep, pltpu.roll(tail, LANES - quarter, 1), 0.0)
        y = product(split2(leg[c]), split2(z_all[...]), ((0,), (0,)))
        low = z.modes // 2
        for s in range(z.bands):
            rows = y[s * z.modes : (s + 1) * z.modes]
            send_u[c, s, : z.modes] = rows[:, :LANES]
            send_u[c, s, z.modes :] = rows[:low, LANES:] + pltpu.roll(rows[low:, LANES:], quarter, 1)

    pl.semaphore_wait(barrier, z.bands + 1)

    def begin(c, carry):
        for which in (1, 0):
            core_copy(c, which).start()
        return carry

    lax.fori_loop(0, z.own, begin, 0)
    leg_copy.wait()

    def phase(p, carry):
        @pl.when(p < z.own)
        def _():
            core_copy(p, 1).wait_recv()
            at = block(at_me.across, p)
            q[at, :] = q[at, :] + r1[p, 1]
            across_copy(p).start()

        @pl.when((p >= LAG_ACROSS) & (p < z.own + LAG_ACROSS))
        def _():
            c = p - LAG_ACROSS
            core_copy(c, 0).wait_recv()
            across_copy(c).wait_recv()
            at = block(w, c)
            q[at, :] = q[at, :] + r1[c, 0] + r2[c]
            for e in range(1, z.group):
                third_copy(c, e).start()
            third_own(c).start()

        @pl.when(p >= LAG_ACROSS + LAG_SPREAD)
        def _():
            c = p - LAG_ACROSS - LAG_SPREAD
            third_own(c).wait()
            for e in range(1, z.group):
                third_copy(c, e).wait_recv()
            transform(c)
            for d in range(1, z.bands):
                fourth_copy(c, d).start()
            fourth_own(c).start()

        return carry

    lax.fori_loop(0, z.own + LAG_ACROSS + LAG_SPREAD, phase, 0)

    def drain(c, carry):
        across_copy(c).wait_send()
        for which in range(2):
            core_copy(c, which).wait_send()
        for e in range(1, z.group):
            third_copy(c, e).wait_send()
        for d in range(1, z.bands):
            fourth_copy(c, d).wait()
        fourth_own(c).wait()
        return carry

    lax.fori_loop(0, z.own, drain, 0)


def transform_backward(z, bins, model, seen, lidar, aod, cosine, sine, courant, legendre):
    anywhere = pl.BlockSpec(memory_space=pl.ANY)
    in_vmem = pl.BlockSpec(memory_space=pltpu.VMEM)
    dma = pltpu.SemaphoreType.DMA
    lats, channels, lons = courant.shape
    rows = model.shape[1]
    levels = channels // bins
    slab = (z.rows, LANES)
    chunk = (z.group * z.rows, LANES)
    table = pltpu.VMEM((z.slots, lons), bf16)
    return pl.pallas_call(
        lambda *refs: second_kernel(z, bins, *refs),
        in_specs=[in_vmem] * 6 + [anywhere, anywhere],
        out_specs=anywhere,
        out_shape=jax.ShapeDtypeStruct((2, z.own, z.group, z.in_rows, LANES), f32),
        scratch_shapes=[
            pltpu.VMEM(model.shape, f32),
            pltpu.VMEM((lats * levels, lons), f32),
            pltpu.VMEM((lats, lons), f32),
            pltpu.VMEM((2, z.pairs, channels, lons), f32),
            pltpu.VMEM((z.slots * z.rows, LANES), f32),
            table, table, table, table,
            pltpu.VMEM((rows, channels), bf16),
            pltpu.VMEM((rows, channels), bf16),
            pltpu.VMEM((z.own, 2) + chunk, f32),
            pltpu.VMEM((z.own,) + chunk, f32),
            pltpu.VMEM((z.group, z.own) + slab, f32),
            pltpu.VMEM((z.own, z.half_lats, z.modes * z.bands), f32),
            pltpu.VMEM((z.half_lats, 2 * LANES), f32),
            pltpu.VMEM((z.own, z.bands, z.in_rows, LANES), f32),
            dma(()), dma((z.pairs // z.unroll,)), dma((z.own, 2)), dma((z.own, 2)), dma((z.own,)), dma((z.own,)),
            dma((z.own, z.group)), dma((z.own, z.group)), dma((z.own, z.bands)), dma((z.own, z.bands)),
        ],
        compiler_params=pltpu.CompilerParams(collective_id=1, has_side_effects=True, vmem_limit_bytes=VMEM_LIMIT),
        name="transform_backward",
    )(model, seen, lidar, aod, cosine, sine, courant.reshape(2, z.pairs, channels, lons),
      legendre.reshape(z.own, z.group, *legendre.shape[1:]))


def last_kernel(z, slabs_ref, control_ref, scale_ref, root_ref, out_ref, s_a, s_b, r_hi, r_lo):
    half = LANES // 2
    quarter = LANES // 4

    @pl.when(pl.program_id(0) == 0)
    def _():
        r_hi[...], r_lo[...] = split2(interleaved(root_ref[...]))

    for m in range(GROUP_ROWS):
        slab = slabs_ref[0, m] + slabs_ref[1, m]
        tail = slab[z.modes :]
        keep = lane_of(tail.shape) % half < quarter
        both = jnp.concatenate(
            [jnp.where(keep, tail, 0.0), jnp.where(keep, pltpu.roll(tail, LANES - quarter, 1), 0.0)], 0)
        s_a[pl.ds(m, z.modes, stride=GROUP_ROWS), :] = slab[: z.modes]
        s_b[pl.ds(m, z.modes, stride=GROUP_ROWS), :] = both
    order = packed_order(z.width // 2, True)
    placed = jnp.concatenate([s_a[...], s_b[...]], 1)
    scale = scale_ref[...].reshape(z.modes * GROUP_ROWS, z.width)
    mixed = product(split2(scale * select_product(placed, order)), (r_hi[...], r_lo[...]), ((1,), (1,)))
    out_ref[...] = control_ref[...] + mixed.reshape(z.modes, GROUP_ROWS, z.width)


def finish(z, slabs, control, scale, root):
    by_waves = pl.BlockSpec((z.modes, GROUP_ROWS, z.width), lambda i: (0, i, 0))
    return pl.pallas_call(
        lambda *refs: last_kernel(z, *refs),
        grid=(z.waves // GROUP_ROWS,),
        in_specs=[
            pl.BlockSpec((2, GROUP_ROWS, z.in_rows, LANES), lambda i: (0, i, 0, 0)),
            by_waves, by_waves, whole(*root.shape),
        ],
        out_specs=by_waves,
        out_shape=jax.ShapeDtypeStruct(control.shape, f32),
        scratch_shapes=[pltpu.VMEM((z.modes * GROUP_ROWS, LANES), f32)] * 2 + [pltpu.VMEM((z.width, z.width), bf16)] * 2,
        compiler_params=pltpu.CompilerParams(vmem_limit_bytes=VMEM_LIMIT),
        name="finish",
    )(slabs.reshape(2, z.waves, z.in_rows, LANES), control, scale, root)


def fast_body(
    control,
    spectral_scale,
    vertical_root,
    legendre,
    zonal_number,
    courant,
    lidar_coef,
    aod_coef,
    obs_count,
    obs_column,
    obs_level,
    lidar_obs,
    aod_obs,
    obs_weight,
):
    modes_here, waves_here, width = control.shape
    wave_count = lax.axis_size("wave")
    lats_here, channels, lon_here = courant.shape
    z = Sizes(modes_here, waves_here, width, lats_here, lax.axis_size("band"), wave_count)
    bins = lidar_coef.shape[0]
    lidar, aod = lidar_coef.reshape(1, -1), aod_coef.reshape(1, -1)
    observed = (obs_count, obs_column, obs_level, lidar_obs, aod_obs, obs_weight)
    slabs, seen, cosine, sine = transform_forward(
        z, control, spectral_scale, vertical_root, legendre, zonal_number, lon_here, observed)
    tracer, model = synthesis_settle(z, slabs, cosine, sine, courant, lidar, aod)
    back = transform_backward(z, bins, model, seen, lidar, aod, cosine, sine, courant, legendre)
    return finish(z, back, control, spectral_scale, vertical_root), tracer


def fits(mesh, control, courant, columns, bins):
    bands, waves = mesh.shape["band"], mesh.shape["wave"]
    modes_here, waves_here = control[0] // bands, control[1] // waves
    lats_here, channels = courant[0] // bands, courant[1]
    return (
        waves == 4
        and bands % 2 == 0
        and waves_here % (bands // 2) == 0
        and waves_here % 8 == 0
        and modes_here % 16 == 0
        and lats_here % 8 == 0
        and LANES // 2 < channels <= LANES * 3 // 4
        and (channels - LANES // 2) % 8 == 0
        and courant[2] // waves % LANES == 0
        and GROUP_ROWS % (bands // 2) == 0
        and columns[1] == LANES
        and channels // bins == GROUP_ROWS
        and bands * waves % OBS_ROWS == 0
    )


SPECS = (
    P("band", "wave", None),
    P("band", "wave", None),
    P(),
    P("wave", None, None),
    P(),
    P("band", None, "wave"),
    P(),
    P(),
    P(("wave", "band"), None),
    P(("wave", "band"), None),
    P(("wave", "band"), None),
    P(("wave", "band"), None),
    P(("wave", "band"), None),
    P(("wave", "band"), None),
)


def solution(mesh):
    def program(*args):
        chosen = fast_body if fits(mesh, args[0].shape, args[5].shape, args[9].shape, args[6].shape[0]) else body
        return jax.shard_map(
            chosen,
            mesh=mesh,
            in_specs=SPECS,
            out_specs=(P("band", "wave", None), P("band", None, "wave")),
            check_vma=False,
        )(*args)

    return program
```

```python
import math

import jax
import jax.numpy as jnp
from jax import lax
from jax.experimental import pallas as pl
from jax.experimental.pallas import tpu as pltpu
from jax.sharding import PartitionSpec as P

MW = 224
LEV = 8
BINS = 12
STEPS = 4


highest = lax.Precision.HIGHEST
high = lax.Precision.HIGH


def trig_tables(numbers, lon_first, lon_count, lon_total, factor):
    longitudes = lon_first + jnp.arange(lon_count, dtype=jnp.int32)
    phases = numbers[:, None] * longitudes[None, :] % lon_total
    angles = phases.astype(jnp.float32) * (2.0 * math.pi / lon_total)
    return (jnp.cos(angles) * factor, jnp.sin(angles) * factor)


def settle_kernel(bins, tracer_ref, courant_ref, proj_ref, out_ref, model_ref):
    tracer = tracer_ref[0]
    courant = courant_ref[0]
    row = lax.broadcasted_iota(jnp.int32, tracer.shape, 0)
    for repeat in range(STEPS):
        outflow = courant * tracer
        inflow = jnp.where(row >= bins, pltpu.roll(outflow, bins, 0), 0.0)
        tracer = tracer - outflow + inflow
    out_ref[0] = tracer
    model_ref[0] = jnp.dot(proj_ref[...], tracer, precision=highest, preferred_element_type=jnp.float32)


def settle_adjoint_kernel(bins, resid_ref, courant_ref, proj_ref, out_ref):
    courant = courant_ref[0]
    adjoint = jnp.dot(proj_ref[...], resid_ref[0], precision=highest, preferred_element_type=jnp.float32)
    channels = adjoint.shape[0]
    row = lax.broadcasted_iota(jnp.int32, adjoint.shape, 0)
    for repeat in range(STEPS):
        below = jnp.where(row < channels - bins, pltpu.roll(adjoint, channels - bins, 0), 0.0)
        adjoint = adjoint + courant * (below - adjoint)
    out_ref[0] = adjoint


def per_lat(rows, cols):
    return pl.BlockSpec((1, rows, cols), lambda t: (t, 0, 0))


def whole(rows, cols):
    return pl.BlockSpec((rows, cols), lambda t: (0, 0))


def settle_forward(tracer, courant, proj, bins):
    lats, channels, lons = tracer.shape
    rows = proj.shape[0]
    return pl.pallas_call(
        lambda *refs: settle_kernel(bins, *refs),
        grid=(lats,),
        in_specs=[per_lat(channels, lons), per_lat(channels, lons), whole(rows, channels)],
        out_specs=[per_lat(channels, lons), per_lat(rows, lons)],
        out_shape=[
            jax.ShapeDtypeStruct((lats, channels, lons), jnp.float32),
            jax.ShapeDtypeStruct((lats, rows, lons), jnp.float32),
        ],
        name="settle_forward",
    )(tracer, courant, proj)


def settle_backward(resid, courant, proj_t, bins):
    lats, channels, lons = courant.shape
    rows = proj_t.shape[1]
    return pl.pallas_call(
        lambda *refs: settle_adjoint_kernel(bins, *refs),
        grid=(lats,),
        in_specs=[per_lat(rows, lons), per_lat(channels, lons), whole(channels, rows)],
        out_specs=per_lat(channels, lons),
        out_shape=jax.ShapeDtypeStruct((lats, channels, lons), jnp.float32),
        name="settle_backward",
    )(resid, courant, proj_t)


def synthesis_sum(cosine, sine_table, parts):
    return jnp.einsum("mo,mtc->tco", cosine, parts[..., 0], precision=high) - jnp.einsum(
        "mo,mtc->tco", sine_table, parts[..., 1], precision=high
    )


def analysis(cosine, sine_table, field):
    real_adj = jnp.einsum("mo,tco->mtc", cosine, field, precision=high)
    imag_adj = -jnp.einsum("mo,tco->mtc", sine_table, field, precision=high)
    stacked = jnp.stack([real_adj, imag_adj], axis=-1)
    return stacked.reshape(stacked.shape[0], stacked.shape[1], -1)


def body(
    control,
    spectral_scale,
    vertical_root,
    legendre,
    zonal_number,
    courant,
    lidar_coef,
    aod_coef,
    obs_count,
    obs_column,
    obs_level,
    lidar_obs,
    aod_obs,
    obs_weight,
):
    modes_here, waves_here, width = control.shape
    channels = width // 2
    wave_count = lax.axis_size("wave")
    band_count = lax.axis_size("band")
    lat_here = legendre.shape[1] // band_count
    lon_here = courant.shape[2]
    lon_total = lon_here * wave_count
    lon_first = lax.axis_index("wave") * lon_here
    factor = MW ** (-0.5)
    slot_count = obs_column.shape[1]
    live = jnp.arange(slot_count, dtype=jnp.int32)[None, :] < obs_count.reshape(-1, 1)
    packet = jnp.stack(
        [
            obs_column.astype(jnp.float32),
            obs_level.astype(jnp.float32),
            lidar_obs,
            aod_obs,
            jnp.where(live, obs_weight, 0.0),
        ],
        axis=1,
    )
    arrived = lax.all_to_all(packet, ("wave", "band"), split_axis=0, concat_axis=0, tiled=True)
    columns, levels, lidar_vals, aod_vals, weights = [arrived[:, i].reshape(-1) for i in range(5)]
    columns = columns.astype(jnp.int32)
    levels = levels.astype(jnp.int32)
    paired = control.reshape(modes_here, waves_here, channels, 2)
    mixed = jnp.einsum("nmcp,cd->nmdp", paired, vertical_root, precision=high).reshape(
        modes_here, waves_here, width
    )
    scaled = spectral_scale * mixed
    all_modes = lax.all_to_all(scaled, "band", split_axis=2, concat_axis=0, tiled=True)
    every_lat = jnp.einsum("mln,nmc->mlc", legendre, all_modes, precision=high)
    spectral = lax.all_to_all(every_lat, "band", split_axis=1, concat_axis=2, tiled=True)
    shard_piece = lax.all_gather(spectral, "wave", axis=0, tiled=True)
    numbers = zonal_number
    cosine, sine_table = trig_tables(numbers, lon_first, lon_here, lon_total, factor)
    parts = shard_piece.reshape(shard_piece.shape[0], lat_here, channels, 2)
    tracer = synthesis_sum(cosine, sine_table, parts)
    bins = lidar_coef.shape[0]
    levels_here = channels // bins
    proj_rows = -(-(levels_here + 1) // 8) * 8
    level_of = jnp.arange(channels, dtype=jnp.int32) // bins
    in_level = jnp.arange(levels_here, dtype=jnp.int32)[:, None] == level_of[None, :]
    proj = jnp.concatenate(
        [
            jnp.where(in_level, jnp.tile(lidar_coef, levels_here)[None, :], 0.0),
            aod_coef[None, :],
            jnp.zeros((proj_rows - levels_here - 1, channels), jnp.float32),
        ],
        axis=0,
    )
    tracer, model = settle_forward(tracer, courant, proj, bins)
    lat_index = columns // lon_here
    lon_hot = (columns % lon_here)[:, None] == jnp.arange(lon_here, dtype=jnp.int32)[None, :]
    lat_hot = (lat_index[:, None] == jnp.arange(lat_here, dtype=jnp.int32)[None, :]).astype(jnp.float32)
    cell = lat_index * levels_here + levels
    cell_hot = (
        cell[:, None] == jnp.arange(lat_here * levels_here, dtype=jnp.int32)[None, :]
    ).astype(jnp.float32)
    lidar_field = model[:, :levels_here].reshape(lat_here * levels_here, lon_here)
    aod_field = model[:, levels_here]
    lidar_rows = jnp.dot(cell_hot, lidar_field, precision=highest)
    aod_rows = jnp.dot(lat_hot, aod_field, precision=highest)
    lidar_model = jnp.sum(jnp.where(lon_hot, lidar_rows, 0.0), axis=1)
    aod_model = jnp.sum(jnp.where(lon_hot, aod_rows, 0.0), axis=1)
    lidar_resid = weights * (lidar_model - lidar_vals)
    aod_resid = weights * (aod_model - aod_vals)
    lidar_sum = lax.dot_general(
        cell_hot, jnp.where(lon_hot, lidar_resid[:, None], 0.0), (((0,), (0,)), ((), ())), precision=highest
    )
    aod_sum = lax.dot_general(
        lat_hot, jnp.where(lon_hot, aod_resid[:, None], 0.0), (((0,), (0,)), ((), ())), precision=highest
    )
    resid = jnp.concatenate(
        [
            lidar_sum.reshape(lat_here, levels_here, lon_here),
            aod_sum[:, None, :],
            jnp.zeros((lat_here, proj_rows - levels_here - 1, lon_here), jnp.float32),
        ],
        axis=1,
    )
    adjoint = settle_backward(resid, courant, proj.T, bins)
    numbers = zonal_number
    cosine, sine_table = trig_tables(numbers, lon_first, lon_here, lon_total, factor)
    spectral_adj = lax.psum_scatter(
        analysis(cosine, sine_table, adjoint), "wave", scatter_dimension=0, tiled=True
    )
    all_lats = lax.all_to_all(spectral_adj, "band", split_axis=2, concat_axis=1, tiled=True)
    mode_block = jnp.einsum("mtn,mtc->nmc", legendre, all_lats, precision=high)
    scaled_adj = lax.all_to_all(mode_block, "band", split_axis=0, concat_axis=2, tiled=True)
    mixed_adj = (spectral_scale * scaled_adj).reshape(modes_here, waves_here, channels, 2)
    control_adj = jnp.einsum("nmdp,cd->nmcp", mixed_adj, vertical_root, precision=high).reshape(
        modes_here, waves_here, width
    )
    return (control + control_adj, tracer)


LANES = 128
MESH_ID = pl.DeviceIdType.MESH
bf16 = jnp.bfloat16
f32 = jnp.float32
VMEM_LIMIT = 42 * 1024 * 1024
SMALL_LIMIT = 16 * 1024 * 1024


def split2(x):
    hi = x.astype(bf16)
    return hi, (x - hi.astype(f32)).astype(bf16)


def split3(x):
    hi, lo = split2(x)
    rest = x - hi.astype(f32)
    return hi, lo, (rest - lo.astype(f32)).astype(bf16)


def product(a, b, dims=((1,), (0,))):
    def one(x, y):
        return lax.dot_general(x, y, (dims, ((), ())), preferred_element_type=f32)

    return one(a[1], b[0]) + one(a[0], b[1]) + one(a[0], b[0])


def lane_of(shape):
    return lax.broadcasted_iota(jnp.int32, shape, len(shape) - 1)


def packed_order(channels, transposed):
    half = LANES // 2
    width = 2 * channels
    shape = (2 * LANES, width) if transposed else (width, 2 * LANES)
    source = lax.broadcasted_iota(jnp.int32, shape, 1 if transposed else 0)
    target = lax.broadcasted_iota(jnp.int32, shape, 0 if transposed else 1)
    channel = source // 2
    place = jnp.where(channel < half, channel, channel + half) + (source % 2) * half
    return jnp.where(place == target, 1.0, 0.0).astype(bf16)


def select_product(x, matrix):
    return sum(
        lax.dot_general(piece, matrix, (((1,), (0,)), ((), ())), preferred_element_type=f32)
        for piece in reversed(split3(x))
    )


def interleaved(root):
    channels = root.shape[0]
    wide = 2 * channels
    spread = (lax.broadcasted_iota(jnp.int32, (wide, channels), 0) // 2
              == lax.broadcasted_iota(jnp.int32, (wide, channels), 1))
    gather = (lax.broadcasted_iota(jnp.int32, (channels, wide), 1) // 2
              == lax.broadcasted_iota(jnp.int32, (channels, wide), 0))
    spread = jnp.where(spread, 1.0, 0.0).astype(bf16)
    gather = jnp.where(gather, 1.0, 0.0).astype(bf16)
    both = select_product(root, gather)
    both = sum(jnp.dot(spread, piece, preferred_element_type=f32) for piece in reversed(split3(both)))
    same = (lax.broadcasted_iota(jnp.int32, both.shape, 0) % 2) == (lax.broadcasted_iota(jnp.int32, both.shape, 1) % 2)
    return jnp.where(same, both, 0.0)


class Sizes:
    def __init__(self, modes, waves, width, lats, bands, wave_count):
        self.modes, self.waves, self.width, self.lats = modes, waves, width, lats
        self.bands, self.wave_count = bands, wave_count
        self.group = bands // 2
        self.own = waves // self.group
        self.half_lats = lats * self.group
        self.pairs = lats // 2
        self.rows = -(-(3 * self.pairs) // 8) * 8
        self.in_rows = modes + modes // 2
        self.slots = waves * wave_count
        self.unroll = max(u for u in range(1, UNROLL + 1) if self.pairs % u == 0)


class Place:
    def __init__(self, z):
        self.w, self.b = lax.axis_index("wave"), lax.axis_index("band")
        self.partner = self.w + 1 - 2 * (self.w % 2)
        self.across = (self.w + 2) % z.wave_count
        self.relay = (self.partner + 2) % z.wave_count
        self.half, self.spot = self.b // z.group, self.b % z.group
        self.z = z

    def peer(self, d):
        return (self.b + d) % self.z.bands

    def near_spot(self, e):
        return (self.spot + e) % self.z.group

    def near(self, e):
        return self.half * self.z.group + self.near_spot(e)

    def greet(self):
        barrier = pltpu.get_barrier_semaphore()
        others = [(self.w, self.peer(d)) for d in range(1, self.z.bands)]
        for wave, band in others + [(self.partner, self.b), (self.across, self.b)]:
            pl.semaphore_signal(barrier, inc=1, device_id={"wave": wave, "band": band}, device_id_type=MESH_ID)
        return barrier


def remote(src, dst, send, recv, wave, band):
    return pltpu.make_async_remote_copy(
        src, dst, send, recv, device_id={"wave": wave, "band": band}, device_id_type=MESH_ID)


AHEAD = 2
LAG_SPREAD = 2
LAG_ACROSS = 2
GROUP_ROWS = 8
UNROLL = 7


def first_kernel(z, control_hbm, scale_hbm, root_hbm, leg_ref, count_hbm, column_hbm, level_hbm, lidar_hbm, aod_hbm,
                 weight_hbm, number_hbm, out_ref, seen_ref, cos_ref, sin_ref,
                 root_ref, count_ref, column_ref, level_ref, lidar_ref, aod_ref, weight_ref, number_ref, s_sem, control, scale, s_a, s_b, send_u, recv_v, leg, y_a, y_b, send_y, packet,
                 leg_sem, in_sem, o_send, o_recv, a1_send, a1_recv, a2_send, a2_recv, x_send, x_recv, c_send, c_recv):
    at_me = Place(z)
    w, b = at_me.w, at_me.b
    half = LANES // 2
    quarter = LANES // 4
    phases = GROUP_ROWS // z.group
    groups = z.waves // GROUP_ROWS
    devices = z.wave_count * z.bands
    me = w * z.bands + b

    def input_copy(i, which):
        source, target = ((control_hbm, control), (scale_hbm, scale))[which]
        return pltpu.make_async_copy(
            source.at[:, pl.ds(i * GROUP_ROWS, GROUP_ROWS), :], target.at[i], in_sem.at[i, which])

    small = [
        pltpu.make_async_copy(source, target, s_sem.at[n])
        for n, (source, target) in enumerate((
            (root_hbm, root_ref), (count_hbm, count_ref), (column_hbm, column_ref), (level_hbm, level_ref),
            (lidar_hbm, lidar_ref), (aod_hbm, aod_ref), (weight_hbm, weight_ref), (number_hbm, number_ref)))
    ]
    for which in range(2):
        input_copy(0, which).start()
    for copy in small:
        copy.start()
    for i in range(1, groups):
        for which in range(2):
            input_copy(i, which).start()
    leg_copy = pltpu.make_async_copy(
        leg_ref.at[:, at_me.spot, pl.ds(at_me.half * z.half_lats, z.half_lats)], leg, leg_sem)
    leg_copy.start()
    barrier = pltpu.get_barrier_semaphore()

    def greet(e, carry):
        to = (me + e) % devices
        pl.semaphore_signal(barrier, inc=1, device_id={"wave": to // z.bands, "band": to % z.bands},
                            device_id_type=MESH_ID)
        return carry

    lax.fori_loop(1, devices, greet, 0)

    for copy in small:
        copy.wait()
    counts = jnp.broadcast_to(count_ref[...], (devices, devices))
    diagonal = lax.broadcasted_iota(jnp.int32, counts.shape, 0) == lax.broadcasted_iota(jnp.int32, counts.shape, 1)
    counts = jnp.sum(jnp.where(diagonal, counts, 0).astype(f32), axis=1, keepdims=True)
    weights = weight_ref[...]
    live = lax.broadcasted_iota(jnp.int32, weights.shape, 1).astype(f32) < counts
    fields = (column_ref[...].astype(f32), level_ref[...].astype(f32), lidar_ref[...], aod_ref[...],
              jnp.where(live, weights, 0.0))
    for k in range(GROUP_ROWS):
        value = fields[k] if k < len(fields) else jnp.zeros_like(weights)
        packet[pl.ds(k, devices, stride=GROUP_ROWS), :] = value

    def packet_copy(e):
        to = (me + e) % devices
        return remote(packet.at[pl.ds(to * GROUP_ROWS, GROUP_ROWS)], seen_ref.at[pl.ds(me * GROUP_ROWS, GROUP_ROWS)],
                      o_send.at[e], o_recv.at[e], to // z.bands, to % z.bands)

    packet_own = pltpu.make_async_copy(
        packet.at[pl.ds(me * GROUP_ROWS, GROUP_ROWS)], seen_ref.at[pl.ds(me * GROUP_ROWS, GROUP_ROWS)], o_send.at[0])

    root = split2(interleaved(root_ref[...]))
    order = packed_order(z.width // 2, False)

    def vertical(i):
        for which in range(2):
            input_copy(i, which).wait()
        x = control[i].reshape(z.modes * GROUP_ROWS, z.width)
        y = scale[i].reshape(z.modes * GROUP_ROWS, z.width)
        placed = select_product(y * product(split2(x), root), order)
        s_a[...] = placed[:, :LANES]
        s_b[...] = placed[:, LANES:]

    def first_copy(c, d):
        to = at_me.peer(d)
        return remote(send_u.at[c, to % z.group], recv_v.at[b, c], a1_send.at[c, d], a1_recv.at[c, d], w, to)

    def first_own(c):
        return pltpu.make_async_copy(send_u.at[c, at_me.spot], recv_v.at[b, c], a1_send.at[c, 0])

    def launch(c):
        @pl.when((c % phases == 0) & (c >= phases))
        def _():
            vertical(c // phases)

        low = z.modes // 2
        for spot in range(z.group):
            at = pl.ds(c % phases * z.group + spot, z.modes, stride=GROUP_ROWS)
            tall = s_b[at, :]
            send_u[c, spot, : z.modes] = s_a[at, :]
            send_u[c, spot, z.modes :] = tall[:low] + pltpu.roll(tall[low:], quarter, 1)
        for d in range(1, z.bands):
            first_copy(c, d).start()
        first_own(c).start()

    def second_copy(c, e):
        return remote(send_y.at[c, at_me.near_spot(e)], out_ref.at[w, c, at_me.spot], a2_send.at[c, e], a2_recv.at[c, e],
                      w, at_me.near(e))

    def second_own(c):
        return pltpu.make_async_copy(send_y.at[c, at_me.spot], out_ref.at[w, c, at_me.spot], a2_send.at[c, 0])

    def across_copy(c):
        return remote(out_ref.at[w, c], out_ref.at[w, c], x_send.at[c], x_recv.at[c], at_me.across, b)

    def core_copy(c, which):
        block = w if which == 0 else at_me.across
        return remote(out_ref.at[block, c], out_ref.at[block, c], c_send.at[c, which], c_recv.at[c, which],
                      at_me.partner, b)

    def transform(c):
        tops, tails = [], []
        for s in range(z.bands):
            tail = recv_v[s, c, z.modes :]
            keep = lane_of(tail.shape) % half < quarter
            tops.append(recv_v[s, c, : z.modes])
            tails.append(jnp.where(keep, tail, 0.0))
            tails.append(jnp.where(keep, pltpu.roll(tail, LANES - quarter, 1), 0.0))
        x = jnp.concatenate([jnp.concatenate(tops, 0), jnp.concatenate(tails, 0)], 1)
        y = product(split2(leg[c]), split2(x))
        y_a[...] = y[:, :LANES]
        y_b[...] = y[:, LANES:]
        for s in range(z.group):
            at = s * z.lats
            one = y_a[at : at + z.pairs]
            two = y_a[at + z.pairs : at + z.lats]
            left = lane_of(one.shape) < half
            send_y[c, s, z.rows - 8 :] = jnp.zeros((8, LANES), f32)
            send_y[c, s, : z.pairs] = jnp.where(left, one, pltpu.roll(two, half, 1))
            send_y[c, s, z.pairs : 2 * z.pairs] = jnp.where(left, pltpu.roll(one, half, 1), two)
            send_y[c, s, 2 * z.pairs : 3 * z.pairs] = y_b[at : at + z.pairs] + pltpu.roll(
                y_b[at + z.pairs : at + z.lats], quarter, 1)

    vertical(0)
    pl.semaphore_wait(barrier, devices - 1)
    for c in range(min(AHEAD, z.own)):
        launch(c)

    def send_packet(e, carry):
        packet_copy(e).start()
        return carry

    lax.fori_loop(1, devices, send_packet, 0)
    packet_own.start()
    lons = cos_ref.shape[1]
    lon_total = lons * z.wave_count
    longitude = lax.broadcasted_iota(jnp.int32, cos_ref.shape, 1) + w * lons
    across_lanes = jnp.broadcast_to(number_ref[...].astype(f32), (z.slots, z.slots))
    same = lax.broadcasted_iota(jnp.int32, across_lanes.shape, 0) == lane_of(across_lanes.shape)
    number = jnp.sum(jnp.where(same, across_lanes, 0.0), axis=1, keepdims=True).astype(jnp.int32)
    angle = (number * longitude % lon_total).astype(f32) * (2.0 * math.pi / lon_total)
    factor = z.slots ** (-0.5)
    cos_ref[...] = jnp.cos(angle) * factor
    sin_ref[...] = jnp.sin(angle) * factor
    leg_copy.wait()

    def phase(p, carry):
        @pl.when(p + AHEAD < z.own)
        def _():
            launch(p + AHEAD)

        @pl.when(p < z.own)
        def _():
            first_own(p).wait()
            for d in range(1, z.bands):
                first_copy(p, d).wait_recv()
            transform(p)
            for e in range(1, z.group):
                second_copy(p, e).start()
            second_own(p).start()

        @pl.when((p >= LAG_SPREAD) & (p < z.own + LAG_SPREAD))
        def _():
            c = p - LAG_SPREAD
            for e in range(1, z.group):
                second_copy(c, e).wait_recv()
            second_own(c).wait()
            across_copy(c).start()
            core_copy(c, 0).start()

        @pl.when(p >= LAG_SPREAD + LAG_ACROSS)
        def _():
            c = p - LAG_SPREAD - LAG_ACROSS
            across_copy(c).wait_recv()
            core_copy(c, 1).start()

        return carry

    lax.fori_loop(0, z.own + LAG_SPREAD + LAG_ACROSS, phase, 0)

    def drain(c, carry):
        for d in range(1, z.bands):
            first_copy(c, d).wait_send()
        for e in range(1, z.group):
            second_copy(c, e).wait_send()
        across_copy(c).wait_send()
        for which in range(2):
            core_copy(c, which).wait()
        return carry

    lax.fori_loop(0, z.own, drain, 0)

    def drain_packet(e, carry):
        packet_copy(e).wait()
        return carry

    lax.fori_loop(1, devices, drain_packet, 0)
    packet_own.wait()


def in_hbm(x):
    return pltpu.with_memory_space_constraint(x, pltpu.MemorySpace.HBM)


def transform_forward(z, control, scale, root, legendre, numbers, lons, observed):
    in_vmem = pl.BlockSpec(memory_space=pltpu.VMEM)
    anywhere = pl.BlockSpec(memory_space=pl.ANY)
    dma = pltpu.SemaphoreType.DMA
    devices = z.wave_count * z.bands
    groups = z.waves // GROUP_ROWS
    numbers = numbers.reshape(1, -1)
    control, scale, root, numbers = (in_hbm(x) for x in (control, scale, root, numbers))
    observed = [in_hbm(x) for x in observed]
    block = (groups, z.modes, GROUP_ROWS, z.width)
    return pl.pallas_call(
        lambda *refs: first_kernel(z, *refs),
        in_specs=[pl.BlockSpec(memory_space=pltpu.MemorySpace.HBM)] * 11,
        out_specs=[in_vmem, anywhere, in_vmem, in_vmem],
        out_shape=[
            pltpu.VMEM((z.wave_count, z.own, z.group, z.rows, LANES), f32),
            jax.ShapeDtypeStruct((devices * GROUP_ROWS, LANES), f32),
            jax.ShapeDtypeStruct((z.slots, lons), f32),
            jax.ShapeDtypeStruct((z.slots, lons), f32),
        ],
        scratch_shapes=[pltpu.VMEM(x.shape, x.dtype) for x in (root, *observed, numbers)] + [
            dma((8,)),
            pltpu.VMEM(block, f32),
            pltpu.VMEM(block, f32),
            pltpu.VMEM((z.modes * GROUP_ROWS, LANES), f32),
            pltpu.VMEM((z.modes * GROUP_ROWS, LANES), f32),
            pltpu.VMEM((z.own, z.group, z.in_rows, LANES), f32),
            pltpu.VMEM((z.bands, z.own, z.in_rows, LANES), f32),
            pltpu.VMEM((z.own, z.half_lats, z.modes * z.bands), f32),
            pltpu.VMEM((z.half_lats, LANES), f32),
            pltpu.VMEM((z.half_lats, LANES), f32),
            pltpu.VMEM((z.own, z.group, z.rows, LANES), f32),
            pltpu.VMEM((devices * GROUP_ROWS, LANES), f32),
            dma(()), dma((groups, 2)), dma((devices,)), dma((devices,)),
            dma((z.own, z.bands)), dma((z.own, z.bands)), dma((z.own, z.group)), dma((z.own, z.group)),
            dma((z.own,)), dma((z.own,)), dma((z.own, 2)), dma((z.own, 2)),
        ],
        compiler_params=pltpu.CompilerParams(collective_id=0, has_side_effects=True, vmem_limit_bytes=VMEM_LIMIT),
        name="transform_forward",
    )(control, scale, root, legendre.reshape(z.own, z.group, *legendre.shape[1:]), *observed, numbers)


def synthesis_kernel(z, bins, slabs_ref, cos_ref, sin_ref, courant_ref, lidar_ref, aod_ref, out_ref, model_ref,
                     c_hi, c_lo, n_hi, n_lo, p_hi, p_lo):
    half = LANES // 2

    @pl.when(pl.program_id(0) == 0)
    def _():
        c_hi[...], c_lo[...] = split2(cos_ref[...])
        n_hi[...], n_lo[...] = split2(-sin_ref[...])
        p_hi[...], p_lo[...] = split2(
            projection(lidar_ref[...], aod_ref[...], bins, aod_ref.shape[1] // bins, model_ref.shape[2]))

    def slab(row):
        return slabs_ref[pl.ds(row, z.slots, stride=z.rows), :]

    over_waves = ((0,), (0,))
    rest = z.width // 2 - half
    for u in range(z.unroll):
        i = pl.program_id(0) * z.unroll + u
        tail = slab(2 * z.pairs + i)
        real = jnp.concatenate([slab(i), tail], 1)
        imag = jnp.concatenate([slab(z.pairs + i), pltpu.roll(tail, half, 1)], 1)
        field = product(split2(real), (c_hi[...], c_lo[...]), over_waves) + product(
            split2(imag), (n_hi[...], n_lo[...]), over_waves)
        for which in range(2):
            tracer = jnp.concatenate(
                [field[which * half : (which + 1) * half],
                 field[LANES + which * (half // 2) : LANES + which * (half // 2) + rest]], 0)
            courant = courant_ref[which, u]
            row = lax.broadcasted_iota(jnp.int32, tracer.shape, 0)
            for repeat in range(STEPS):
                outflow = courant * tracer
                inflow = jnp.where(row >= bins, pltpu.roll(outflow, bins, 0), 0.0)
                tracer = tracer - outflow + inflow
            out_ref[which, u] = tracer
            model_ref[which, u] = product((p_hi[...], p_lo[...]), split2(tracer))


def paired(z, rows, cols):
    return pl.BlockSpec((2, z.unroll, rows, cols), lambda i: (0, i, 0, 0))


def synthesis_settle(z, slabs, cosine, sine, courant, lidar, aod):
    lats, channels, lons = courant.shape
    bins = lidar.shape[1]
    rows = -(-(channels // bins + 1) // 8) * 8
    tracer, model = pl.pallas_call(
        lambda *refs: synthesis_kernel(z, bins, *refs),
        grid=(z.pairs // z.unroll,),
        in_specs=[pl.BlockSpec(memory_space=pltpu.VMEM), whole(z.slots, lons), whole(z.slots, lons), paired(z, channels, lons),
                  whole(1, bins), whole(1, channels)],
        out_specs=[paired(z, channels, lons), paired(z, rows, lons)],
        out_shape=[
            jax.ShapeDtypeStruct((2, z.pairs, channels, lons), f32),
            jax.ShapeDtypeStruct((2, z.pairs, rows, lons), f32),
        ],
        scratch_shapes=[pltpu.VMEM((z.slots, lons), bf16)] * 4 + [pltpu.VMEM((rows, channels), bf16)] * 2,
        compiler_params=pltpu.CompilerParams(vmem_limit_bytes=SMALL_LIMIT),
        name="synthesis_settle",
    )(slabs.reshape(z.slots * z.rows, LANES), cosine, sine, courant.reshape(2, z.pairs, channels, lons), lidar, aod)
    return tracer.reshape(lats, channels, lons), model.reshape(lats, rows, lons)


OBS_ROWS = 4


def projection(lidar, aod, bins, levels, rows):
    channels = aod.shape[1]
    repeat = (lax.broadcasted_iota(jnp.int32, (bins, channels), 1) % bins
              == lax.broadcasted_iota(jnp.int32, (bins, channels), 0))
    repeat = jnp.where(repeat, 1.0, 0.0).astype(bf16)
    tiled = select_product(jnp.broadcast_to(lidar, (8, bins)), repeat)[:1]
    row = lax.broadcasted_iota(jnp.int32, (rows, channels), 0)
    level = lax.broadcasted_iota(jnp.int32, (rows, channels), 1) // bins
    return jnp.where((row < levels) & (level == row), tiled, jnp.where(row == levels, aod, 0.0))


def observe(z, levels, model_ref, seen_ref, resid, lidar_acc, aod_acc):
    lats, rows, lons = model_ref.shape
    cells = lats * levels
    devices = seen_ref.shape[0] // GROUP_ROWS
    slots = OBS_ROWS * seen_ref.shape[1]

    def halves(x):
        return jnp.concatenate(split2(x.T), 0)

    lidar_field = halves(model_ref[:, :levels, :].reshape(cells, lons))
    aod_field = halves(jnp.sum(model_ref[:, levels:, :], axis=1))
    lidar_acc[...] = jnp.zeros_like(lidar_acc)
    aod_acc[...] = jnp.zeros_like(aod_acc)
    over_slots = ((1,), (1,))

    def step(i, carry):
        def row(k):
            first = i * OBS_ROWS * GROUP_ROWS + k
            return jnp.concatenate([seen_ref[pl.ds(first + r * GROUP_ROWS, 1), :] for r in range(OBS_ROWS)], 1)

        column = row(0).astype(jnp.int32)
        lat = column // lons
        lon_hot = lax.broadcasted_iota(jnp.int32, (lons, slots), 0) == column - lat * lons
        cell = lat * levels + row(1).astype(jnp.int32)
        cell_hot = jnp.where(lax.broadcasted_iota(jnp.int32, (cells, slots), 0) == cell, 1.0, 0.0).astype(bf16)
        lat_hot = jnp.where(lax.broadcasted_iota(jnp.int32, (lats, slots), 0) == lat, 1.0, 0.0).astype(bf16)
        weight = row(4)

        def one(field, hot, observed, acc):
            picked = jnp.dot(field, hot, preferred_element_type=f32)
            picked = picked[:lons] + picked[lons:]
            left = weight * (jnp.sum(jnp.where(lon_hot, picked, 0.0), axis=0, keepdims=True) - observed)
            hi, lo = (jnp.where(lon_hot, part.astype(f32), 0.0).astype(bf16) for part in split2(left))
            acc[...] += lax.dot_general(hot, hi, (over_slots, ((), ())), preferred_element_type=f32) + lax.dot_general(
                hot, lo, (over_slots, ((), ())), preferred_element_type=f32)

        one(lidar_field, cell_hot, row(2), lidar_acc)
        one(aod_field, lat_hot, row(3), aod_acc)
        return carry

    lax.fori_loop(0, devices // OBS_ROWS, step, 0)
    resid[:, :levels, :] = lidar_acc[...].reshape(lats, levels, lons)
    spread = jnp.broadcast_to(aod_acc[...][:, None, :], (lats, rows - levels, lons))
    first = lax.broadcasted_iota(jnp.int32, spread.shape, 1) == 0
    resid[:, levels:, :] = jnp.where(first, spread, 0.0)


def second_kernel(z, bins, model_ref, seen_ref, lidar_ref, aod_ref, cos_ref, sin_ref, courant_ref, leg_ref, out_ref,
                  resid, lidar_acc, aod_acc, courant, q, c_hi, c_lo, n_hi, n_lo, p_hi, p_lo, r1, r2, v3, leg, z_all, send_u,
                  leg_sem, k_sem, c_send, c_recv, x_send, x_recv, a3_send, a3_recv, a4_send, a4_recv):
    at_me = Place(z)
    w, b = at_me.w, at_me.b
    half = LANES // 2
    quarter = LANES // 4
    channels = z.width // 2
    levels = channels // bins
    steps = z.pairs // z.unroll

    def courant_copy(k):
        at = pl.ds(k * z.unroll, z.unroll)
        return pltpu.make_async_copy(courant_ref.at[:, at], courant.at[:, at], k_sem.at[k])

    for k in range(steps):
        courant_copy(k).start()
    leg_copy = pltpu.make_async_copy(
        leg_ref.at[:, at_me.spot, pl.ds(at_me.half * z.half_lats, z.half_lats)], leg, leg_sem)
    leg_copy.start()
    barrier = at_me.greet()

    observe(z, levels, model_ref, seen_ref, resid, lidar_acc, aod_acc)

    c_hi[...], c_lo[...] = split2(cos_ref[...])
    n_hi[...], n_lo[...] = split2(-sin_ref[...])
    p_hi[...], p_lo[...] = split2(projection(lidar_ref[...], aod_ref[...], bins, levels, resid.shape[1]))
    for spare in range(3 * z.pairs, z.rows):
        q[pl.ds(spare, z.slots, stride=z.rows), :] = jnp.zeros((z.slots, LANES), f32)
    over_lons = ((1,), (1,))

    def analyse(k, carry):
        courant_copy(k).wait()
        for u in range(z.unroll):
            i = k * z.unroll + u
            fields = []
            for which in range(2):
                number = courant[which, i]
                adjoint = product((p_hi[...], p_lo[...]), split2(resid[which * z.pairs + i]), ((0,), (0,)))
                row = lax.broadcasted_iota(jnp.int32, adjoint.shape, 0)
                for repeat in range(STEPS):
                    below = jnp.where(row < channels - bins, pltpu.roll(adjoint, channels - bins, 0), 0.0)
                    adjoint = adjoint + number * (below - adjoint)
                fields.append(adjoint)
            gap = jnp.zeros((half // 2 - (channels - half), fields[0].shape[1]), f32)
            pieces = [field[:half] for field in fields]
            for field in fields:
                pieces.append(field[half:])
                if gap.shape[0]:
                    pieces.append(gap)
            pieces.append(jnp.zeros((half, fields[0].shape[1]), f32))
            both = split2(jnp.concatenate(pieces, 0))
            real = product((c_hi[...], c_lo[...]), both, over_lons)
            imag = product((n_hi[...], n_lo[...]), both, over_lons)
            q[pl.ds(i, z.slots, stride=z.rows), :] = real[:, :LANES]
            q[pl.ds(z.pairs + i, z.slots, stride=z.rows), :] = imag[:, :LANES]
            q[pl.ds(2 * z.pairs + i, z.slots, stride=z.rows), :] = real[:, LANES:] + pltpu.roll(imag[:, LANES:], half, 1)
        return carry

    lax.fori_loop(0, steps, analyse, 0)

    def block(wave, c):
        return pl.ds(pl.multiple_of((wave * z.own + c) * z.group * z.rows, 8), z.group * z.rows)

    def slab(c, spot):
        return pl.ds(pl.multiple_of(((w * z.own + c) * z.group + spot) * z.rows, 8), z.rows)

    def core_copy(c, which):
        wave = at_me.partner if which == 0 else at_me.relay
        return remote(q.at[block(wave, c)], r1.at[c, which], c_send.at[c, which], c_recv.at[c, which], at_me.partner, b)

    def across_copy(c):
        return remote(q.at[block(at_me.across, c)], r2.at[c], x_send.at[c], x_recv.at[c], at_me.across, b)

    def third_copy(c, e):
        return remote(q.at[slab(c, at_me.near_spot(e))], v3.at[at_me.spot, c], a3_send.at[c, e], a3_recv.at[c, e],
                      w, at_me.near(e))

    def third_own(c):
        return pltpu.make_async_copy(q.at[slab(c, at_me.spot)], v3.at[at_me.spot, c], a3_send.at[c, 0])

    def fourth_copy(c, d):
        return remote(send_u.at[c, at_me.peer(d)], out_ref.at[at_me.half, c, at_me.spot], a4_send.at[c, d],
                      a4_recv.at[c, d], w, at_me.peer(d))

    def fourth_own(c):
        return pltpu.make_async_copy(send_u.at[c, b], out_ref.at[at_me.half, c, at_me.spot], a4_send.at[c, 0])

    def transform(c):
        for s in range(z.group):
            at = s * z.lats
            real = v3[s, c, : z.pairs]
            imag = v3[s, c, z.pairs : 2 * z.pairs]
            tail = v3[s, c, 2 * z.pairs : 3 * z.pairs]
            lane = lane_of(real.shape)
            keep = lane % half < quarter
            z_all[at : at + z.pairs, :LANES] = jnp.where(lane < half, real, pltpu.roll(imag, half, 1))
            z_all[at + z.pairs : at + z.lats, :LANES] = jnp.where(lane < half, pltpu.roll(real, half, 1), imag)
            z_all[at : at + z.pairs, LANES:] = jnp.where(keep, tail, 0.0)
            z_all[at + z.pairs : at + z.lats, LANES:] = jnp.where(keep, pltpu.roll(tail, LANES - quarter, 1), 0.0)
        y = product(split2(leg[c]), split2(z_all[...]), ((0,), (0,)))
        low = z.modes // 2
        for s in range(z.bands):
            rows = y[s * z.modes : (s + 1) * z.modes]
            send_u[c, s, : z.modes] = rows[:, :LANES]
            send_u[c, s, z.modes :] = rows[:low, LANES:] + pltpu.roll(rows[low:, LANES:], quarter, 1)

    pl.semaphore_wait(barrier, z.bands + 1)

    def begin(c, carry):
        for which in (1, 0):
            core_copy(c, which).start()
        return carry

    lax.fori_loop(0, z.own, begin, 0)
    leg_copy.wait()

    def phase(p, carry):
        @pl.when(p < z.own)
        def _():
            core_copy(p, 1).wait_recv()
            at = block(at_me.across, p)
            q[at, :] = q[at, :] + r1[p, 1]
            across_copy(p).start()

        @pl.when((p >= LAG_ACROSS) & (p < z.own + LAG_ACROSS))
        def _():
            c = p - LAG_ACROSS
            core_copy(c, 0).wait_recv()
            across_copy(c).wait_recv()
            at = block(w, c)
            q[at, :] = q[at, :] + r1[c, 0] + r2[c]
            for e in range(1, z.group):
                third_copy(c, e).start()
            third_own(c).start()

        @pl.when(p >= LAG_ACROSS + LAG_SPREAD)
        def _():
            c = p - LAG_ACROSS - LAG_SPREAD
            third_own(c).wait()
            for e in range(1, z.group):
                third_copy(c, e).wait_recv()
            transform(c)
            for d in range(1, z.bands):
                fourth_copy(c, d).start()
            fourth_own(c).start()

        return carry

    lax.fori_loop(0, z.own + LAG_ACROSS + LAG_SPREAD, phase, 0)

    def drain(c, carry):
        across_copy(c).wait_send()
        for which in range(2):
            core_copy(c, which).wait_send()
        for e in range(1, z.group):
            third_copy(c, e).wait_send()
        for d in range(1, z.bands):
            fourth_copy(c, d).wait()
        fourth_own(c).wait()
        return carry

    lax.fori_loop(0, z.own, drain, 0)


def transform_backward(z, bins, model, seen, lidar, aod, cosine, sine, courant, legendre):
    anywhere = pl.BlockSpec(memory_space=pl.ANY)
    in_vmem = pl.BlockSpec(memory_space=pltpu.VMEM)
    dma = pltpu.SemaphoreType.DMA
    lats, channels, lons = courant.shape
    rows = model.shape[1]
    levels = channels // bins
    slab = (z.rows, LANES)
    chunk = (z.group * z.rows, LANES)
    table = pltpu.VMEM((z.slots, lons), bf16)
    return pl.pallas_call(
        lambda *refs: second_kernel(z, bins, *refs),
        in_specs=[in_vmem] * 6 + [anywhere, anywhere],
        out_specs=anywhere,
        out_shape=jax.ShapeDtypeStruct((2, z.own, z.group, z.in_rows, LANES), f32),
        scratch_shapes=[
            pltpu.VMEM(model.shape, f32),
            pltpu.VMEM((lats * levels, lons), f32),
            pltpu.VMEM((lats, lons), f32),
            pltpu.VMEM((2, z.pairs, channels, lons), f32),
            pltpu.VMEM((z.slots * z.rows, LANES), f32),
            table, table, table, table,
            pltpu.VMEM((rows, channels), bf16),
            pltpu.VMEM((rows, channels), bf16),
            pltpu.VMEM((z.own, 2) + chunk, f32),
            pltpu.VMEM((z.own,) + chunk, f32),
            pltpu.VMEM((z.group, z.own) + slab, f32),
            pltpu.VMEM((z.own, z.half_lats, z.modes * z.bands), f32),
            pltpu.VMEM((z.half_lats, 2 * LANES), f32),
            pltpu.VMEM((z.own, z.bands, z.in_rows, LANES), f32),
            dma(()), dma((z.pairs // z.unroll,)), dma((z.own, 2)), dma((z.own, 2)), dma((z.own,)), dma((z.own,)),
            dma((z.own, z.group)), dma((z.own, z.group)), dma((z.own, z.bands)), dma((z.own, z.bands)),
        ],
        compiler_params=pltpu.CompilerParams(collective_id=1, has_side_effects=True, vmem_limit_bytes=VMEM_LIMIT),
        name="transform_backward",
    )(model, seen, lidar, aod, cosine, sine, courant.reshape(2, z.pairs, channels, lons),
      legendre.reshape(z.own, z.group, *legendre.shape[1:]))


def last_kernel(z, slabs_ref, control_ref, scale_ref, root_ref, out_ref, s_a, s_b, r_hi, r_lo):
    half = LANES // 2
    quarter = LANES // 4

    @pl.when(pl.program_id(0) == 0)
    def _():
        r_hi[...], r_lo[...] = split2(interleaved(root_ref[...]))

    for m in range(GROUP_ROWS):
        slab = slabs_ref[0, m] + slabs_ref[1, m]
        tail = slab[z.modes :]
        keep = lane_of(tail.shape) % half < quarter
        both = jnp.concatenate(
            [jnp.where(keep, tail, 0.0), jnp.where(keep, pltpu.roll(tail, LANES - quarter, 1), 0.0)], 0)
        s_a[pl.ds(m, z.modes, stride=GROUP_ROWS), :] = slab[: z.modes]
        s_b[pl.ds(m, z.modes, stride=GROUP_ROWS), :] = both
    order = packed_order(z.width // 2, True)
    placed = jnp.concatenate([s_a[...], s_b[...]], 1)
    scale = scale_ref[...].reshape(z.modes * GROUP_ROWS, z.width)
    mixed = product(split2(scale * select_product(placed, order)), (r_hi[...], r_lo[...]), ((1,), (1,)))
    out_ref[...] = control_ref[...] + mixed.reshape(z.modes, GROUP_ROWS, z.width)


def finish(z, slabs, control, scale, root):
    by_waves = pl.BlockSpec((z.modes, GROUP_ROWS, z.width), lambda i: (0, i, 0))
    return pl.pallas_call(
        lambda *refs: last_kernel(z, *refs),
        grid=(z.waves // GROUP_ROWS,),
        in_specs=[
            pl.BlockSpec((2, GROUP_ROWS, z.in_rows, LANES), lambda i: (0, i, 0, 0)),
            by_waves, by_waves, whole(*root.shape),
        ],
        out_specs=by_waves,
        out_shape=jax.ShapeDtypeStruct(control.shape, f32),
        scratch_shapes=[pltpu.VMEM((z.modes * GROUP_ROWS, LANES), f32)] * 2 + [pltpu.VMEM((z.width, z.width), bf16)] * 2,
        compiler_params=pltpu.CompilerParams(vmem_limit_bytes=VMEM_LIMIT),
        name="finish",
    )(slabs.reshape(2, z.waves, z.in_rows, LANES), control, scale, root)


def fast_body(
    control,
    spectral_scale,
    vertical_root,
    legendre,
    zonal_number,
    courant,
    lidar_coef,
    aod_coef,
    obs_count,
    obs_column,
    obs_level,
    lidar_obs,
    aod_obs,
    obs_weight,
):
    modes_here, waves_here, width = control.shape
    wave_count = lax.axis_size("wave")
    lats_here, channels, lon_here = courant.shape
    z = Sizes(modes_here, waves_here, width, lats_here, lax.axis_size("band"), wave_count)
    bins = lidar_coef.shape[0]
    lidar, aod = lidar_coef.reshape(1, -1), aod_coef.reshape(1, -1)
    observed = (obs_count, obs_column, obs_level, lidar_obs, aod_obs, obs_weight)
    slabs, seen, cosine, sine = transform_forward(
        z, control, spectral_scale, vertical_root, legendre, zonal_number, lon_here, observed)
    tracer, model = synthesis_settle(z, slabs, cosine, sine, courant, lidar, aod)
    back = transform_backward(z, bins, model, seen, lidar, aod, cosine, sine, courant, legendre)
    return finish(z, back, control, spectral_scale, vertical_root), tracer


def fits(mesh, control, courant, columns, bins):
    bands, waves = mesh.shape["band"], mesh.shape["wave"]
    modes_here, waves_here = control[0] // bands, control[1] // waves
    lats_here, channels = courant[0] // bands, courant[1]
    return (
        waves == 4
        and bands % 2 == 0
        and waves_here % (bands // 2) == 0
        and waves_here % 8 == 0
        and modes_here % 16 == 0
        and lats_here % 8 == 0
        and LANES // 2 < channels <= LANES * 3 // 4
        and (channels - LANES // 2) % 8 == 0
        and courant[2] // waves % LANES == 0
        and GROUP_ROWS % (bands // 2) == 0
        and columns[1] == LANES
        and channels // bins == GROUP_ROWS
        and bands * waves % OBS_ROWS == 0
    )


SPECS = (
    P("band", "wave", None),
    P("band", "wave", None),
    P(),
    P("wave", None, None),
    P(),
    P("band", None, "wave"),
    P(),
    P(),
    P(("wave", "band"), None),
    P(("wave", "band"), None),
    P(("wave", "band"), None),
    P(("wave", "band"), None),
    P(("wave", "band"), None),
    P(("wave", "band"), None),
)


def solution(mesh):
    def program(*args):
        chosen = fast_body if fits(mesh, args[0].shape, args[5].shape, args[9].shape, args[6].shape[0]) else body
        return jax.shard_map(
            chosen,
            mesh=mesh,
            in_specs=SPECS,
            out_specs=(P("band", "wave", None), P("band", None, "wave")),
            check_vma=False,
        )(*args)

    return program
```
